32 devices in a mesh: dp: 16 (over z, y, x), tensor: 2 (over core).
Axes of the slice: x: 2, y: 2, z: 4, core: 2. Of those that a mesh axis runs over, the one named last changes fastest.
Arguments:
- stream_in: bfloat16 [16384, 1024], P(('dp', 'tensor'))
- grad_out: bfloat16 [16384, 1024], P(('dp', 'tensor')), may hold values from -6 to 6
- clip_lengths: int32 [16], P('dp'), may hold values from 512 to 1024, as said below
- first_up: bfloat16 [1024, 4096], P('dp', 'tensor'), may hold values from -0.1875 to 0.1875
- first_down: bfloat16 [4096, 1024], P('tensor', 'dp'), may hold values from -0.1875 to 0.1875
- attn_proj: bfloat16 [3, 1024, 1024], P(None, 'dp', 'tensor'), may hold values from -0.1875 to 0.1875
- attn_out: bfloat16 [1024, 1024], P('tensor', 'dp'), may hold values from -1.5 to 1.5
- rel_table: bfloat16 [73, 64], replicated, may hold values from -6 to 6
- glu_weight: bfloat16 [2, 1024, 1024], P(None, 'dp', 'tensor'), may hold values from -0.1875 to 0.1875
- conv_taps: float32 [31, 1024], replicated, may hold values from -1.8 to 1.8
- conv_out: bfloat16 [1024, 1024], P('tensor', 'dp'), may hold values from -0.375 to 0.375
- second_up: bfloat16 [1024, 4096], P('dp', 'tensor'), may hold values from -0.1875 to 0.1875
- second_down: bfloat16 [4096, 1024], P('tensor', 'dp'), may hold values from -0.1875 to 0.1875
- norm_gains: float32 [6, 1024], replicated, may hold values from 0.1 to 1.9
- norm_shifts: float32 [6, 1024], replicated, may hold values from -1.8 to 1.8
Outputs:
- output: bfloat16 [16384, 1024], P(('dp', 'tensor'))
- grad_in: float32 [16384, 1024], P(('dp', 'tensor'))
- grad_first_up: float32 [1024, 4096], P('dp', 'tensor')
- grad_first_down: float32 [4096, 1024], P('tensor', 'dp')
- grad_attn_proj: float32 [3, 1024, 1024], P(None, 'dp', 'tensor')
- grad_attn_out: float32 [1024, 1024], P('tensor', 'dp')
- grad_rel_table: float32 [73, 64], replicated
- grad_glu_weight: float32 [2, 1024, 1024], P(None, 'dp', 'tensor')
- grad_conv_taps: float32 [31, 1024], replicated
- grad_conv_out: float32 [1024, 1024], P('tensor', 'dp')
- grad_second_up: float32 [1024, 4096], P('dp', 'tensor')
- grad_second_down: float32 [4096, 1024], P('tensor', 'dp')
- grad_norm_gains: float32 [6, 1024], replicated
- grad_norm_shifts: float32 [6, 1024], replicated
- rms_values: float32 [5], replicated
The draws below stay inside these ranges and needn't reach their ends.
Inputs may be any that keep to these rules, and one draw needn't show every extreme that they name: `clip_lengths`: keys at or past a clip's length are excluded; some clip is full in every draw.
All inputs are finite; a program needn't handle non-finite values.
Results may differ from the reference program's by a relative error of at most 0.025.
Values may be sent and summed in bfloat16 or wider, within the bound.
A program may use at most 256 MiB of HBM per device.

```python
import jax
import jax.numpy as jnp
from jax import lax

D = 1024
HEADS = 16
HEAD = 64
FF = 4096
KERNEL = 31
LEFT = 64
RIGHT = 8
L = 1024
CLIPS = 1
BUCKETS = 73
CLIPS_ALL = 16
TOKENS = 16384
N_DP = 16


def draw_stream_in(key, part):
    row_pos = jnp.arange(TOKENS, dtype=jnp.float32) / max(TOKENS - 1, 1)
    noise_raw = jax.random.truncated_normal(key, -4.0, 4.0, (TOKENS, D), jnp.float32)
    row_scale = 0.6 * 3.0 ** row_pos
    return (noise_raw * row_scale[:, None]).astype(jnp.bfloat16)


def draw_clip_lengths(key, part):
    key_draw = jax.random.fold_in(key, 11)
    key_pick = jax.random.fold_in(key, 12)
    drawn_len = jax.random.randint(key_draw, (CLIPS_ALL,), L // 2, L + 1)
    chosen = jax.random.randint(key_pick, (), 0, CLIPS_ALL)
    return jnp.where(jnp.arange(CLIPS_ALL) == chosen, L, drawn_len).astype(jnp.int32)


def spiked(entries, rng, source, target, parts, factor):
    def block_of(axis_at):
        return (jnp.arange(entries.shape[axis_at]) // (entries.shape[axis_at] // parts)).reshape((-1,) + (1,) * (entries.ndim - 1 - axis_at))

    near = jax.random.permutation(rng, parts)[block_of(target)]
    second = (block_of(target) + parts // 2) % parts
    return jnp.where((block_of(source) == near) | (block_of(source) == second), factor * entries, entries)


def steps_of(own_key, shape, cuts, smallest, top_value):
    def one(dim, blocks):
        heights = jax.random.uniform(jax.random.fold_in(jax.random.fold_in(own_key, 6), dim), (blocks,), jnp.float32, smallest / len(cuts), top_value / len(cuts))
        return jnp.repeat(jnp.exp(heights), shape[dim] // blocks).reshape((-1,) + (1,) * (len(shape) - dim - 1))

    factor_of = one(*cuts[0])
    for cut in cuts[1:]:
        factor_of = factor_of * one(*cut)
    return factor_of


def normal_values(key, extent, spread, limit, pieces=(), kind=jnp.bfloat16):
    values = spread * jax.random.normal(key, extent, jnp.float32)
    if pieces:
        values = values * steps_of(key, extent, pieces, -0.22, 0.18)
    return jnp.clip(values, -limit, limit).astype(kind)


def bell_draw_with(rng, shape, spread, reach, split, heavy, kind=jnp.bfloat16):
    values = spread * jax.random.normal(rng, shape, jnp.float32)
    if split:
        values = values * steps_of(rng, shape, split, -0.22, 0.18)
    return jnp.clip(spiked(values, jax.random.fold_in(rng, 3), *heavy), -reach, reach).astype(kind)


def setup_inputs(seed: int = 0) -> dict:
    streams_of = jax.random.split(jax.random.key(seed), 16)
    stream_in = draw_stream_in(jax.random.fold_in(streams_of[15], 71), 0)
    grad_out = bell_draw_with(streams_of[1], (TOKENS, D), 1.0, 6.0, ((0, 32),), (0, 1, 32, 2.75))
    clip_lengths = draw_clip_lengths(jax.random.fold_in(streams_of[15], 71), 0)
    first_up = normal_values(streams_of[3], (D, FF), D ** -0.5, 0.1875, ((0, 16), (1, 2)))
    first_down = normal_values(streams_of[4], (FF, D), (FF // 4) ** -0.5, 0.1875, ((0, 2), (1, 16)))
    attn_proj = normal_values(streams_of[5], (3, D, D), D ** -0.5, 0.1875, ((1, 16), (2, 2)))
    attn_out = normal_values(streams_of[6], (D, D), 16 ** -0.5, 1.5, ((0, 2), (1, 16)))
    rel_table = normal_values(streams_of[7], (BUCKETS, HEAD), 1.0, 6.0)
    glu_weight = normal_values(streams_of[8], (2, D, D), D ** -0.5, 0.1875, ((1, 16), (2, 2)))
    conv_taps = normal_values(streams_of[9], (KERNEL, D), 0.3, 1.8, (), jnp.float32)
    conv_out = normal_values(streams_of[10], (D, D), (D // 4) ** -0.5, 0.375, ((0, 2), (1, 16)))
    second_up = normal_values(streams_of[11], (D, FF), D ** -0.5, 0.1875, ((0, 16), (1, 2)))
    second_down = normal_values(streams_of[12], (FF, D), (FF // 4) ** -0.5, 0.1875, ((0, 2), (1, 16)))
    norm_gains = jnp.clip(1.0 + 0.18 * jax.random.normal(streams_of[13], (6, D), jnp.float32), 0.1, 1.9)
    norm_shifts = normal_values(streams_of[14], (6, D), 0.3, 1.8, (), jnp.float32)
    return dict(stream_in=stream_in, grad_out=grad_out, clip_lengths=clip_lengths, first_up=first_up, first_down=first_down, attn_proj=attn_proj, attn_out=attn_out, rel_table=rel_table, glu_weight=glu_weight, conv_taps=conv_taps, conv_out=conv_out, second_up=second_up, second_down=second_down, norm_gains=norm_gains, norm_shifts=norm_shifts)


EPSILON = 1e-05
MASKED = -1e+30
HIGHEST = lax.Precision.HIGHEST

@jax.custom_vjp
def low(v):
    return lax.optimization_barrier(v.astype(jnp.bfloat16)).astype(jnp.float32)

@jax.custom_vjp
def low_back(v):
    return v

def low_keep(v):
    return (low(v), None)

def low_pass(kept, grad):
    return (grad,)

def back_keep(v):
    return (v, None)

def back_low(kept, grad):
    return (low(grad),)
low.defvjp(low_keep, low_pass)
low_back.defvjp(back_keep, back_low)

def matmul(first_op, second_op):
    return jnp.dot(first_op, second_op, precision=HIGHEST, preferred_element_type=jnp.float32)

def layer_norm(stream, gain_row, shift_row):
    centered = stream - lax.optimization_barrier(jnp.mean(stream, axis=-1, keepdims=True))
    inv_std = lax.rsqrt(lax.optimization_barrier(jnp.mean(centered * centered, axis=-1, keepdims=True)) + EPSILON)
    return centered * inv_std * gain_row + shift_row

def feed_forward(entered, weight_in, weight_out):
    before = low_back(matmul(entered, weight_in))
    return low_back(matmul(low(jax.nn.silu(before)), weight_out))

def attend_block(query_blk, key_clip, value_clip, rel_table, first_row, length):
    direct = jnp.einsum('bhd,khd->hbk', query_blk, key_clip, precision=HIGHEST)
    toward = jnp.einsum('bhd,nd->hbn', query_blk, rel_table, precision=HIGHEST)
    row_ids = first_row + jnp.arange(query_blk.shape[0], dtype=jnp.int32)
    col_ids = jnp.arange(key_clip.shape[0], dtype=jnp.int32)
    bucket = jnp.clip(col_ids[None, :] - row_ids[:, None], -LEFT, RIGHT) + LEFT
    relative = jnp.take_along_axis(toward, jnp.broadcast_to(bucket[None], direct.shape), axis=2)
    scores = low_back((direct + relative) * HEAD ** (-0.5))
    scores = jnp.where((col_ids < length)[None, None, :], scores, MASKED)
    row_peak = lax.optimization_barrier(jnp.max(scores, axis=-1, keepdims=True))
    exponent = jnp.exp(scores - row_peak)
    attn_probs = low(exponent / lax.optimization_barrier(jnp.sum(exponent, axis=-1, keepdims=True)))
    return jnp.einsum('hbk,khd->bhd', attn_probs, value_clip, precision=HIGHEST)

def attention(entered, attn_proj, attn_out, rel_table, lengths):

    def project(proj_index):
        return low(low_back(matmul(entered, attn_proj[proj_index]))).reshape(CLIPS, L, HEADS, HEAD)
    queries = project(0)
    key_rows = project(1)
    value_rows = project(2)
    block_rows = min(512, L)
    block_count = L // block_rows

    def one_clip(clip_item):
        query_clip, key_clip, value_clip, length = clip_item

        def one_block(blk_index):
            query_blk = lax.dynamic_slice_in_dim(query_clip, blk_index * block_rows, block_rows, 0)
            return attend_block(query_blk, key_clip, value_clip, rel_table, blk_index * block_rows, length)
        return lax.map(jax.checkpoint(one_block), jnp.arange(block_count, dtype=jnp.int32))
    attended = lax.map(one_clip, (queries, key_rows, value_rows, lengths))
    attended = low(low_back(attended.reshape(CLIPS * L, D)))
    return low_back(matmul(attended, attn_out))

def convolve(entered, glu_weight, conv_taps, gain_row, shift_row, conv_out):
    glu_first = low_back(matmul(entered, glu_weight[0]))
    glu_second = low_back(matmul(entered, glu_weight[1]))
    gated = (glu_first * jax.nn.sigmoid(glu_second)).reshape(CLIPS, L, D)
    padded = jnp.pad(gated, ((0, 0), (KERNEL - 1, 0), (0, 0)))
    mixed_conv = jnp.zeros_like(gated)
    for tap_index in range(KERNEL):
        mixed_conv = mixed_conv + conv_taps[tap_index] * padded[:, tap_index:tap_index + L]
    shaped = layer_norm(mixed_conv.reshape(CLIPS * L, D), gain_row, shift_row)
    return low_back(matmul(low(jax.nn.silu(shaped)), conv_out))

def layer(stream, lengths, weights):
    first_up, first_down, attn_proj, attn_out, rel_table, glu_weight, conv_taps, conv_out, second_up, second_down, norm_gains, norm_shifts = weights

    def enter_norm(norm_row, value):
        return low(layer_norm(value, norm_gains[norm_row], norm_shifts[norm_row]))
    branch_one = feed_forward(enter_norm(0, stream), first_up, first_down)
    stream_one = stream + 0.5 * branch_one
    branch_two = attention(enter_norm(1, stream_one), attn_proj, attn_out, rel_table, lengths)
    stream_two = stream_one + branch_two
    branch_three = convolve(enter_norm(2, stream_two), glu_weight, conv_taps, norm_gains[3], norm_shifts[3], conv_out)
    stream_three = stream_two + branch_three
    branch_four = feed_forward(enter_norm(4, stream_three), second_up, second_down)
    stream_four = stream_three + 0.5 * branch_four
    squares = jnp.stack([jnp.sum(branch_one * branch_one), jnp.sum(branch_two * branch_two), jnp.sum(branch_three * branch_three), jnp.sum(branch_four * branch_four), jnp.sum(stream_four * stream_four)])
    return (layer_norm(stream_four, norm_gains[5], norm_shifts[5]), squares)

def reference(stream_in, grad_out, clip_lengths, first_up, first_down, attn_proj, attn_out, rel_table, glu_weight, conv_taps, conv_out, second_up, second_down, norm_gains, norm_shifts):
    weights = tuple((array.astype(jnp.float32) for array in (first_up, first_down, attn_proj, attn_out, rel_table, glu_weight, conv_taps, conv_out, second_up, second_down, norm_gains, norm_shifts)))
    group_rows = CLIPS * L
    streams = stream_in.astype(jnp.float32).reshape(N_DP, group_rows, D)
    cotangents = grad_out.astype(jnp.float32).reshape(N_DP, group_rows, D)
    lengths = clip_lengths.reshape(N_DP, CLIPS).astype(jnp.int32)

    def one_group(carried, group_item):
        weight_sums, square_sums = carried
        stream, grad_rows, length_row = group_item

        def forward(stream_value, weight_value):
            return layer(stream_value, length_row, weight_value)
        result, pullback, squares = jax.vjp(forward, stream, weights, has_aux=True)
        grad_stream, grad_weights = pullback(grad_rows)
        weight_sums = jax.tree.map(lambda running, added: running + added, weight_sums, grad_weights)
        return ((weight_sums, square_sums + squares), (result, grad_stream))
    initial = (jax.tree.map(jnp.zeros_like, weights), jnp.zeros((5,), jnp.float32))
    (weight_sums, square_sums), (results, grad_streams) = lax.scan(one_group, initial, (streams, cotangents, lengths))
    rms_values = jnp.sqrt(square_sums / (TOKENS * D))
    return (results.reshape(TOKENS, D).astype(jnp.bfloat16), grad_streams.reshape(TOKENS, D), weight_sums[0], weight_sums[1], weight_sums[2], weight_sums[3], weight_sums[4], weight_sums[5], weight_sums[6], weight_sums[7], weight_sums[8], weight_sums[9], weight_sums[10], weight_sums[11], rms_values)
```

```python
import functools

import jax
import jax.numpy as jnp
from jax import lax
from jax.experimental import pallas as pl
from jax.experimental.pallas import tpu as pltpu
from jax.sharding import PartitionSpec as P

HEAD = 64
KERNEL = 31
LEFT = 64
RIGHT = 8
EPSILON = 1e-05
MASKED = -1e30
BLK = 128
SPAN = 512
NT = (((1,), (1,)), ((), ()))
TN = (((0,), (0,)), ((), ()))


def dot_nt(a, b):
    return lax.dot_general(a, b, NT, preferred_element_type=jnp.float32)


def dot_tn(a, b):
    return lax.dot_general(a, b, TN, preferred_element_type=jnp.float32)


def dot_nn(a, b):
    return jnp.dot(a, b, preferred_element_type=jnp.float32)


def rel_blocks(tin, b, own_blocks, key_blocks, rank):
    t_left, t_right = tin[:, 0:1], tin[:, SPAN - 1 : SPAN]
    band = pltpu.roll(tin, SPAN - BLK, 1, stride=1, stride_axis=0)
    out = []
    for kb in range(key_blocks):
        wraps = rank * own_blocks + kb >= key_blocks
        if kb in (b - 1, b) or (kb == b + 1 and kb < own_blocks):
            out.append(band[:, (kb - b + 1) * BLK : (kb - b + 2) * BLK])
        elif kb == b + 1:
            out.append(jnp.where(wraps, t_left, band[:, 2 * BLK : 3 * BLK]))
        elif b == 0 and kb == key_blocks - 1:
            out.append(jnp.where(wraps, band[:, :BLK], t_right))
        elif kb < b - 1:
            out.append(t_left)
        elif kb < own_blocks:
            out.append(t_right)
        else:
            out.append(jnp.where(wraps, t_left, t_right))
    return out


def halves(x):
    low = lax.broadcasted_iota(jnp.int32, x.shape, 1) < HEAD
    zero = jnp.zeros_like(x)
    return jnp.where(low, x, zero), jnp.where(low, zero, x)


def flip_rows(x):
    tiles = []
    back = 7 - lax.broadcasted_iota(jnp.int32, (8, BLK), 0)
    for first in range(x.shape[0] - 8, -1, -8):
        cols = [
            jnp.take_along_axis(x[first : first + 8, c : c + BLK], back, axis=0, mode="promise_in_bounds")
            for c in range(0, x.shape[1], BLK)
        ]
        tiles.append(jnp.concatenate(cols, axis=1) if len(cols) > 1 else cols[0])
    return jnp.concatenate(tiles, axis=0)


def attn_fwd_kernel(rank_ref, q_ref, k_ref, v_ref, tab_ref, mask_ref, o_ref, lse_ref):
    rank = rank_ref[0]
    rows, keys = q_ref.shape[0], k_ref.shape[0]
    own_blocks, key_blocks = rows // BLK, keys // BLK
    low = lax.broadcasted_iota(jnp.int32, (BLK, 2 * HEAD), 1) < HEAD
    for b in range(own_blocks):
        q_blk = q_ref[b * BLK : (b + 1) * BLK, :] * jnp.asarray(HEAD**-0.5, jnp.bfloat16)
        results = []
        for hh, q_one in enumerate(halves(q_blk)):
            tin = dot_nt(q_one, tab_ref[...])
            rel = rel_blocks(tin, b, own_blocks, key_blocks, rank)
            raw = dot_nt(q_one, k_ref[...])
            s = [
                raw[:, kb * BLK : (kb + 1) * BLK] + rel[kb] + mask_ref[:, kb * BLK : (kb + 1) * BLK]
                for kb in range(key_blocks)
            ]
            s = jnp.concatenate(s, axis=1)
            peak = jnp.max(s, axis=-1, keepdims=True)
            e = jnp.exp(s - peak)
            total = jnp.sum(e, axis=-1, keepdims=True)
            o = dot_nn(e.astype(jnp.bfloat16), v_ref[...])
            results.append(o / total)
            first = (hh * own_blocks + b) * BLK
            lse_ref[0, first : first + BLK, :] = peak + jnp.log(total)
        o_ref[b * BLK : (b + 1) * BLK, :] = jnp.where(low, results[0], results[1]).astype(jnp.bfloat16)


def attn_fwd(rank, q, k, v, tab2, mask):
    rows, width = q.shape
    keys = k.shape[0]
    pairs = width // (2 * HEAD)
    col = lambda n: pl.BlockSpec((n, 2 * HEAD), lambda p, r: (0, p))
    return pl.pallas_call(
        attn_fwd_kernel,
        grid_spec=pltpu.PrefetchScalarGridSpec(
            num_scalar_prefetch=1,
            grid=(pairs,),
            in_specs=[
                col(rows),
                col(keys),
                col(keys),
                pl.BlockSpec((SPAN, 2 * HEAD), lambda p, r: (0, 0)),
                pl.BlockSpec((1, keys), lambda p, r: (0, 0)),
            ],
            out_specs=[col(rows), pl.BlockSpec((1, 2 * rows, 1), lambda p, r: (p, 0, 0))],
        ),
        out_shape=[
            jax.ShapeDtypeStruct((rows, width), jnp.bfloat16),
            jax.ShapeDtypeStruct((pairs, 2 * rows, 1), jnp.float32),
        ],
        name="attn_fwd",
    )(rank, q, k, v, tab2, mask)


def attn_bwd_kernel(
    rank_ref, q_ref, k_ref, v_ref, do_ref, o_ref, lse_ref, tab_ref, mask_ref,
    dq_ref, dk_ref, dv_ref, dtab_ref, p_sc, ds_sc, q_sc, do_sc,
):
    rank = rank_ref[0]
    rows, keys = q_ref.shape[0], k_ref.shape[0]
    own_blocks, key_blocks = rows // BLK, keys // BLK
    low = lax.broadcasted_iota(jnp.int32, (BLK, 2 * HEAD), 1) < HEAD
    lane = lax.broadcasted_iota(jnp.int32, (BLK, BLK), 1)
    scale = jnp.asarray(HEAD**-0.5, jnp.bfloat16)

    @pl.when(pl.program_id(0) == 0)
    def _():
        dtab_ref[...] = jnp.zeros_like(dtab_ref)

    for b in range(own_blocks):
        at = slice(b * BLK, (b + 1) * BLK)
        q_blk = q_ref[at, :] * scale
        do_blk = do_ref[at, :]
        prod = do_blk.astype(jnp.float32) * o_ref[at, :].astype(jnp.float32)
        q_back = halves(flip_rows(q_blk.astype(jnp.float32)).astype(jnp.bfloat16))
        results = []
        for hh, (q_one, do_one, pr_one) in enumerate(zip(halves(q_blk), halves(do_blk), halves(prod))):
            first = (hh * own_blocks + b) * BLK
            here = slice(first, first + BLK)
            inner = jnp.sum(pr_one, axis=-1, keepdims=True)
            lse = lse_ref[0, here, :]
            tin = dot_nt(q_one, tab_ref[...])
            rel = rel_blocks(tin - lse, b, own_blocks, key_blocks, rank)
            raw = dot_nt(q_one, k_ref[...])
            dp = dot_nt(do_one, v_ref[...])
            left = jnp.zeros((BLK, BLK), jnp.float32)
            right = jnp.zeros((BLK, BLK), jnp.float32)
            window = [None, None, None]
            for kb in range(key_blocks):
                ks = slice(kb * BLK, (kb + 1) * BLK)
                p = jnp.exp(raw[:, ks] + rel[kb] + mask_ref[:, ks])
                ds = (p * (dp[:, ks] - inner)).astype(jnp.bfloat16)
                p_sc[here, ks] = p.astype(jnp.bfloat16)
                ds_sc[here, ks] = ds
                ds = ds.astype(jnp.float32)
                wraps = rank * own_blocks + kb >= key_blocks
                zero = jnp.zeros_like(ds)
                if kb in (b - 1, b) or (kb == b + 1 and kb < own_blocks):
                    window[kb - b + 1] = ds
                elif kb == b + 1:
                    window[2] = jnp.where(wraps, zero, ds)
                    left = left + jnp.where(wraps, ds, zero)
                elif b == 0 and kb == key_blocks - 1:
                    window[0] = jnp.where(wraps, ds, zero)
                    right = right + jnp.where(wraps, zero, ds)
                elif kb < b - 1:
                    left = left + ds
                elif kb < own_blocks:
                    right = right + ds
                else:
                    left = left + jnp.where(wraps, ds, zero)
                    right = right + jnp.where(wraps, zero, ds)
            none = jnp.zeros((BLK, BLK), jnp.float32)
            window = jnp.concatenate([none if w is None else flip_rows(w) for w in window] + [none], axis=1)
            back = pltpu.roll(window, 1, 1, stride=1, stride_axis=0)
            s_left = flip_rows(jnp.broadcast_to(jnp.sum(left, axis=-1, keepdims=True), (BLK, BLK)))
            s_right = flip_rows(jnp.broadcast_to(jnp.sum(right, axis=-1, keepdims=True), (BLK, BLK)))
            u = jnp.concatenate(
                [
                    back[:, :BLK] + jnp.where(lane == 0, s_left, 0.0),
                    back[:, BLK : 3 * BLK],
                    back[:, 3 * BLK :] + jnp.where(lane == BLK - 1, s_right, 0.0),
                ],
                axis=1,
            ).astype(jnp.bfloat16)
            q_sc[here, :] = q_one
            do_sc[here, :] = do_one
            dtab_ref[...] += dot_tn(u, q_back[hh])
            results.append(dot_nn(ds_sc[here, :], k_ref[...]) + flip_rows(dot_nn(u, tab_ref[...])))
        dq_ref[at, :] = (jnp.where(low, results[0], results[1]) * HEAD**-0.5).astype(jnp.bfloat16)
    dk_ref[...] = dot_tn(ds_sc[...], q_sc[...]).astype(dk_ref.dtype)
    dv_ref[...] = dot_tn(p_sc[...], do_sc[...]).astype(dv_ref.dtype)


def attn_bwd(rank, q, k, v, do, o, lse, tab2, mask):
    rows, width = q.shape
    keys = k.shape[0]
    pairs = width // (2 * HEAD)
    col = lambda n: pl.BlockSpec((n, 2 * HEAD), lambda p, r: (0, p))
    return pl.pallas_call(
        attn_bwd_kernel,
        grid_spec=pltpu.PrefetchScalarGridSpec(
            num_scalar_prefetch=1,
            grid=(pairs,),
            in_specs=[
                col(rows),
                col(keys),
                col(keys),
                col(rows),
                col(rows),
                pl.BlockSpec((1, 2 * rows, 1), lambda p, r: (p, 0, 0)),
                pl.BlockSpec((SPAN, 2 * HEAD), lambda p, r: (0, 0)),
                pl.BlockSpec((1, keys), lambda p, r: (0, 0)),
            ],
            out_specs=[col(rows), col(keys), col(keys), pl.BlockSpec((SPAN, 2 * HEAD), lambda p, r: (0, 0))],
            scratch_shapes=[
                pltpu.VMEM((2 * rows, keys), jnp.bfloat16),
                pltpu.VMEM((2 * rows, keys), jnp.bfloat16),
                pltpu.VMEM((2 * rows, 2 * HEAD), jnp.bfloat16),
                pltpu.VMEM((2 * rows, 2 * HEAD), jnp.bfloat16),
            ],
        ),
        out_shape=[
            jax.ShapeDtypeStruct((rows, width), jnp.bfloat16),
            jax.ShapeDtypeStruct((keys, width), jnp.bfloat16),
            jax.ShapeDtypeStruct((keys, width), jnp.bfloat16),
            jax.ShapeDtypeStruct((SPAN, 2 * HEAD), jnp.float32),
        ],
        name="attn_bwd",
    )(rank, q, k, v, do, o, lse, tab2, mask)


def span_table(rel_table):
    rows = jnp.clip(jnp.arange(SPAN) - SPAN // 2, -LEFT, RIGHT) + LEFT
    table = jnp.take(rel_table, rows, axis=0)
    return jnp.concatenate([table, table], axis=1)


def fold_table(dtab):
    one = dtab[:, :HEAD] + dtab[:, HEAD:]
    rows = jnp.clip(jnp.arange(SPAN) - SPAN // 2, -LEFT, RIGHT) + LEFT
    pick = (rows[None, :] == jnp.arange(LEFT + RIGHT + 1)[:, None]).astype(jnp.float32)
    return jnp.dot(pick, one, precision=lax.Precision.HIGHEST)


MESH = pl.DeviceIdType.MESH
ANY = pl.BlockSpec(memory_space=pl.ANY)
VMEM = pl.BlockSpec(memory_space=pltpu.VMEM)
FACTORS = {16: (4, 2, 2), 32: (4, 2, 4)}


class Place:
    def __init__(self, dims, n_tensor):
        self.dims, self.n_tensor = dims, n_tensor
        n_a, n_b, n_c = dims
        d = lax.axis_index("dp")
        self.t = lax.axis_index("tensor")
        self.at = (lax.div(d, n_b * n_c), lax.rem(lax.div(d, n_c), n_b), lax.rem(d, n_c))

    def peer(self, axis, step):
        at, t = list(self.at), self.t
        if axis == 3:
            t = lax.rem(t + step, self.n_tensor)
            index = t
        else:
            at[axis] = index = lax.rem(at[axis] + step, self.dims[axis])
        n_a, n_b, n_c = self.dims
        return ((at[0] * n_b + at[1]) * n_c + at[2], t), index

    def size(self, axis):
        return self.n_tensor if axis == 3 else self.dims[axis]

    def barrier(self, axes=(0, 1, 2, 3)):
        sem = pltpu.get_barrier_semaphore()
        count = 0
        for axis in axes:
            for step in range(1, self.size(axis)):
                pl.semaphore_signal(sem, inc=1, device_id=self.peer(axis, step)[0], device_id_type=MESH)
                count += 1
        pl.semaphore_wait(sem, count)


def remote(src, dst, send_sem, recv_sem, device):
    return pltpu.make_async_remote_copy(
        src_ref=src, dst_ref=dst, send_sem=send_sem, recv_sem=recv_sem, device_id=device, device_id_type=MESH
    )


class Gather:
    ORDERS = ((0, 1, 2), (0, 2, 1))

    def __init__(self, place, shard, whole, send, recv, local):
        self.place, self.shard, self.whole = place, shard, whole
        self.send, self.recv, self.local = send, recv, local
        self.half = shard.shape[1] // 2
        self.width = shard.shape[2]

    @staticmethod
    def slots(dims, n_tensor):
        return sum(d - 1 for d in dims) + 2 * (n_tensor - 1)

    def slot(self, color, stage, step):
        dims = self.place.dims
        base = [0]
        for axis in self.ORDERS[color]:
            base.append(base[-1] + dims[axis] - 1)
        base.append(base[-1] + self.place.n_tensor - 1)
        return (color, base[stage] + step - 1)

    def region(self, color, index, t):
        cols = pl.ds(pl.multiple_of(t * self.width, 128), self.width)
        return self.whole.at[(slice(None),) + tuple(index) + (pl.ds(color * self.half, self.half), cols)]

    def index(self, color, stage, moved=None):
        order, out = self.ORDERS[color], list(self.place.at)
        for axis in order[:stage]:
            out[axis] = slice(None)
        if moved is not None:
            out[order[stage]] = moved
        return out

    def own(self):
        cols = pl.ds(pl.multiple_of(self.place.t * self.width, 128), self.width)
        there = self.whole.at[(slice(None),) + self.place.at + (slice(None), cols)]
        return pltpu.make_async_copy(self.shard, there, self.local)

    def copies(self, stage, arriving=False):
        place = self.place
        for color in (0, 1):
            order = self.ORDERS[color]
            axis = order[stage] if stage < 3 else 3
            for step in range(1, place.size(axis)):
                device, peer = place.peer(axis, step)
                _, source = place.peer(axis, place.size(axis) - step)
                slot = self.slot(color, stage, step)
                sems = (self.send.at[slot], self.recv.at[slot])
                t = place.t
                if stage < 3:
                    mine = self.region(color, self.index(color, stage), t)
                    theirs = self.region(color, self.index(color, stage, source), t)
                elif stage == 3:
                    mine = self.region(color, self.index(color, 2), t)
                    theirs = self.region(color, self.index(color, 2), source)
                elif self.skip(3):
                    mine = self.region(color, self.index(color, 3), t)
                    theirs = self.region(color, self.index(color, 3), source)
                else:
                    index = self.index(color, 2, place.peer(order[2], 1)[1])
                    mine = self.region(color, index, t)
                    theirs = self.region(color, index, source)
                if stage == 0:
                    mine_src = self.shard.at[:, pl.ds(color * self.half, self.half), :]
                else:
                    mine_src = mine
                if arriving:
                    yield remote(theirs, theirs, *sems, device)
                else:
                    yield remote(mine_src, mine, *sems, device)

    def start(self, stage):
        if self.skip(stage):
            return
        for copy in self.copies(stage):
            copy.start()

    def skip(self, stage):
        return stage == 3 and max(self.place.dims[1:]) > 2

    def arrived(self, stage):
        if self.skip(stage):
            return
        for copy in self.copies(stage, arriving=True):
            copy.wait_recv()

    def sent(self, stage):
        if self.skip(stage):
            return
        for copy in self.copies(stage):
            copy.wait_send()


def gather_kernel(dims, n_tensor, n, *refs):
    shards, wholes = refs[:n], refs[n : 2 * n]
    send, recv, local = refs[2 * n :]
    place = Place(dims, n_tensor)
    gathers = [
        Gather(place, s, w, send.at[i], recv.at[i], local.at[i]) for i, (s, w) in enumerate(zip(shards, wholes))
    ]
    for g in gathers:
        g.own().start()
    place.barrier()
    for g in gathers:
        g.start(0)
    for g in gathers:
        g.own().wait()
    for step in range(n + 2):
        if step < n:
            gathers[step].arrived(0)
            gathers[step].start(1)
        if 0 <= step - 1 < n:
            gathers[step - 1].arrived(1)
            gathers[step - 1].start(2)
            gathers[step - 1].start(3)
        if 0 <= step - 2 < n:
            gathers[step - 2].arrived(2)
            gathers[step - 2].start(4)
    for g in gathers:
        for stage in (3, 4):
            g.arrived(stage)
        for stage in range(5):
            g.sent(stage)


def gather_weights(shards, dims, n_tensor, collective_id):
    n = len(shards)
    n_a, n_b, n_c = dims
    slots = Gather.slots(dims, n_tensor)
    outs = pl.pallas_call(
        functools.partial(gather_kernel, dims, n_tensor, n),
        out_shape=[
            jax.ShapeDtypeStruct((s.shape[0], n_a, n_b, n_c, s.shape[1], n_tensor * s.shape[2]), s.dtype) for s in shards
        ],
        in_specs=[VMEM] * n,
        out_specs=[ANY] * n,
        scratch_shapes=[
            pltpu.SemaphoreType.DMA((n, 2, slots)),
            pltpu.SemaphoreType.DMA((n, 2, slots)),
            pltpu.SemaphoreType.DMA((n,)),
        ],
        compiler_params=pltpu.CompilerParams(collective_id=collective_id, has_side_effects=True),
        name="gather_weights",
    )(*shards)
    return [o.reshape(o.shape[0], -1, o.shape[-1]) for o in outs]


class Piece:
    def __init__(self, source, lead, first, width):
        self.source, self.lead, self.first, self.width = source, lead, first, width


def pieces_of(shapes, n_tensor, chunk):
    chunks, room = [], 0
    for source, (n, _, cols) in enumerate(shapes):
        cols //= n_tensor
        for lead in range(n):
            first = 0
            while first < cols:
                width = min(cols - first, chunk if room == 0 else room)
                if room == 0:
                    chunks.append([])
                    room = chunk
                chunks[-1].append(Piece(source, lead, first, width))
                room -= width
                first += width
    return chunks


class Scatter:
    ORDERS = ((2, 1, 0), (1, 2, 0))

    def __init__(self, place, pieces, grads, outs, bufs, sems):
        self.place, self.pieces, self.grads, self.outs = place, pieces, grads, outs
        self.held, self.far, self.near, self.first, self.second, self.third = bufs
        self.send, self.recv, self.local = sems
        self.width = sum(p.width for p in pieces)
        self.half = self.held.shape[3] // 2

    def rows(self, color):
        return pl.ds(color * self.half, self.half)

    def slab(self, piece, t):
        cols = pl.ds(pl.multiple_of(t * (self.grads[piece.source].shape[-1] // self.place.n_tensor) + piece.first, 128), piece.width)
        return self.grads[piece.source].at[piece.lead, :, :, :, :, cols]

    def columns(self):
        at = 0
        for number, piece in enumerate(self.pieces):
            yield number, piece, pl.ds(at, piece.width)
            at += piece.width

    def loads(self):
        for number, piece, cols in self.columns():
            yield pltpu.make_async_copy(self.slab(piece, self.place.t), self.held.at[:, :, :, :, cols], self.local.at[number])

    def tensor_copies(self):
        for step in range(1, self.place.n_tensor):
            device, peer = self.place.peer(3, step)
            for number, piece, cols in self.columns():
                slot = (step - 1) * 2 + number
                yield remote(
                    self.slab(piece, peer), self.far.at[step - 1, :, :, :, :, cols], self.send.at[slot], self.recv.at[slot], device
                )

    def near_loads(self, slot):
        for step in range(1, self.place.n_tensor):
            yield pltpu.make_async_copy(
                self.far.at[step - 1, :, :, :, :, pl.ds(0, self.width)],
                self.near.at[slot, step - 1, :, :, :, :, pl.ds(0, self.width)],
                self.local.at[1 + step],
            )

    def copies(self, stage):
        place = self.place
        base = 2 * (place.n_tensor - 1)
        cols = pl.ds(0, self.width)
        for color in (0, 1):
            order = self.ORDERS[color]
            axis = order[stage - 1]
            for step in range(1, place.size(axis)):
                device, there = place.peer(axis, step)
                index = [slice(None)] * 3
                for done in order[: stage - 1]:
                    index[done] = place.at[done]
                index[axis] = there
                buf = (self.first, self.second, self.third)[stage - 1][color]
                slot = base + sum(place.size(x) - 1 for x in order[: stage - 1]) + step - 1 + color * sum(d - 1 for d in place.dims)
                whole = (slice(None),) * (len(buf.shape) - 2)
                yield remote(
                    self.held.at[tuple(index) + (self.rows(color), cols)],
                    buf.at[(step - 1,) + whole[1:] + (slice(None), cols)],
                    self.send.at[slot],
                    self.recv.at[slot],
                    device,
                )

    @staticmethod
    def slots(dims, n_tensor):
        return 2 * (n_tensor - 1) + 2 * sum(d - 1 for d in dims)

    def add_tensor(self, slot):
        n_a, n_b, n_c = self.place.dims
        cols = slice(0, self.width)

        def body(i, _):
            at = (lax.div(i, n_b * n_c), lax.rem(lax.div(i, n_c), n_b), lax.rem(i, n_c))
            total = self.held[at + (slice(None), cols)].astype(jnp.float32)
            for step in range(1, self.place.n_tensor):
                total = total + self.near[(slot, step - 1) + at + (slice(None), cols)].astype(jnp.float32)
            self.held[at + (slice(None), cols)] = total.astype(jnp.bfloat16)
            return 0

        lax.fori_loop(0, n_a * n_b * n_c, body, 0)

    def add(self, stage):
        place = self.place
        cols = slice(0, self.width)
        for color in (0, 1):
            order = self.ORDERS[color]
            rows = slice(color * self.half, (color + 1) * self.half)
            left = [x for x in (0, 1, 2) if x not in order[:stage]]
            buf = (self.first, self.second)[stage - 1][color]
            count = 1
            for x in left:
                count *= place.dims[x]

            def body(i, _):
                at = list(place.at)
                if len(left) == 2:
                    where = (lax.div(i, place.dims[left[1]]), lax.rem(i, place.dims[left[1]]))
                else:
                    where = (i,)
                for x, w in zip(left, where):
                    at[x] = w
                at = tuple(at) + (rows, cols)
                total = self.held[at].astype(jnp.float32)
                for step in range(1, place.size(order[stage - 1])):
                    total = total + buf[(step - 1,) + where + (slice(None), cols)].astype(jnp.float32)
                self.held[at] = total.astype(jnp.bfloat16)
                return 0

            lax.fori_loop(0, count, body, 0)

    def finish(self):
        for _, piece, cols in self.columns():
            cols = slice(cols.start, cols.start + cols.size)
            for color in (0, 1):
                rows = slice(color * self.half, (color + 1) * self.half)
                total = self.held[self.place.at + (rows, cols)].astype(jnp.float32)
                for step in range(1, self.place.dims[0]):
                    total = total + self.third[color][step - 1, :, cols].astype(jnp.float32)
                self.outs[piece.source][piece.lead, rows, piece.first : piece.first + piece.width] = total


class Total:
    AXES = (3, 2, 1, 0)

    def __init__(self, place, value, out, boxes, send, recv):
        self.place, self.value, self.out, self.boxes, self.send, self.recv = place, value, out, boxes, send, recv

    @staticmethod
    def slots(dims, n_tensor):
        return sum(dims) + n_tensor - 4

    def copies(self, stage):
        place, axis = self.place, self.AXES[stage]
        base = sum(place.size(x) - 1 for x in self.AXES[:stage])
        for step in range(1, place.size(axis)):
            device, _ = place.peer(axis, step)
            slot = base + step - 1
            yield remote(self.value.at[stage], self.boxes[stage].at[step - 1], self.send.at[slot], self.recv.at[slot], device)

    def add(self, stage):
        place, axis = self.place, self.AXES[stage]
        size = place.size(axis)
        mine = place.t if axis == 3 else place.at[axis]
        own = self.value[stage]
        if size == 2:
            total = own + self.boxes[stage][0]
        else:
            total = jnp.zeros_like(own)
            for index in range(size):
                step = lax.rem(mine - index + size, size)
                term = self.boxes[stage][jnp.maximum(step - 1, 0)]
                total = total + jnp.where(step == 0, own, term)
        if stage == 3:
            self.out[...] = total
        else:
            self.value[stage + 1] = total


def scatter_kernel(dims, n_tensor, plan, n, has_total, *refs):
    count = len(plan)
    refs = list(refs)
    take = lambda k: [refs.pop(0) for _ in range(k)]
    grads = take(n)
    vec = take(1)[0] if has_total else None
    outs = take(n)
    vec_out = take(1)[0] if has_total else None
    (far,) = take(1)
    held, near, x0, x1, y0, y1, z0, z1, send, recv, local = take(11)
    place = Place(dims, n_tensor)
    chunks = [
        Scatter(
            place, pieces, grads, outs,
            (held.at[i], far.at[i], near, (x0.at[i], x1.at[i]), (y0.at[i], y1.at[i]), (z0.at[i], z1.at[i])),
            (send.at[i], recv.at[i], local.at[i]),
        )
        for i, pieces in enumerate(plan)
    ]
    for c in chunks:
        for copy in c.loads():
            copy.start()
    total = None
    if has_total:
        value, *rest = take(7)
        total = Total(place, value, vec_out, rest[:4], rest[4], rest[5])
        value[0] = vec[...]
    place.barrier()
    if total is not None:
        for copy in total.copies(0):
            copy.start()
    for c in chunks:
        for copy in c.tensor_copies():
            copy.start()

    def fetch(i):
        for copy in chunks[i].tensor_copies():
            copy.wait_recv()
        for copy in chunks[i].near_loads(i % 2):
            copy.start()

    fetch(0)
    for step in range(max(count + 3, 4 if has_total else 0)):
        if step < count:
            c = chunks[step]
            for copy in c.loads():
                copy.wait()
            for copy in c.near_loads(step % 2):
                copy.wait()
            if step + 1 < count:
                fetch(step + 1)
            c.add_tensor(step % 2)
            for copy in c.copies(1):
                copy.start()
        for stage in (1, 2):
            at = step - stage
            if 0 <= at < count:
                for copy in chunks[at].copies(stage):
                    copy.wait_recv()
                chunks[at].add(stage)
                for copy in chunks[at].copies(stage + 1):
                    copy.start()
        if 0 <= step - 3 < count:
            for copy in chunks[step - 3].copies(3):
                copy.wait_recv()
            chunks[step - 3].finish()
        if total is not None and step < 4:
            for copy in total.copies(step):
                copy.wait_recv()
            total.add(step)
            if step < 3:
                for copy in total.copies(step + 1):
                    copy.start()
    for c in chunks:
        for copy in c.tensor_copies():
            copy.wait_send()
        for stage in (1, 2, 3):
            for copy in c.copies(stage):
                copy.wait_send()
    if total is not None:
        for stage in range(4):
            for copy in total.copies(stage):
                copy.wait_send()


def scatter_grads(grads, vec, dims, n_tensor, collective_id, chunk=1024):
    n_a, n_b, n_c = dims
    places = n_a * n_b * n_c
    rows = grads[0].shape[1] // places
    plan = pieces_of([g.shape for g in grads], n_tensor, chunk)
    count = len(plan)
    chunk = max(sum(p.width for p in pieces) for pieces in plan)
    views = [g.reshape(g.shape[0], n_a, n_b, n_c, rows, g.shape[2]) for g in grads]
    n = len(grads)
    half = rows // 2
    bf = jnp.bfloat16
    slots = Scatter.slots(dims, n_tensor)
    out_shape = [jax.ShapeDtypeStruct((g.shape[0], rows, g.shape[2] // n_tensor), jnp.float32) for g in grads]
    out_specs = [VMEM] * n
    scratch = [
        pltpu.VMEM((count, n_a, n_b, n_c, rows, chunk), bf),
        pltpu.VMEM((2, n_tensor - 1, n_a, n_b, n_c, rows, chunk), bf),
        pltpu.VMEM((count, n_c - 1, n_a, n_b, half, chunk), bf),
        pltpu.VMEM((count, n_b - 1, n_a, n_c, half, chunk), bf),
        pltpu.VMEM((count, n_b - 1, n_a, half, chunk), bf),
        pltpu.VMEM((count, n_c - 1, n_a, half, chunk), bf),
        pltpu.VMEM((count, n_a - 1, half, chunk), bf),
        pltpu.VMEM((count, n_a - 1, half, chunk), bf),
        pltpu.SemaphoreType.DMA((count, slots)),
        pltpu.SemaphoreType.DMA((count, slots)),
        pltpu.SemaphoreType.DMA((count, 1 + n_tensor)),
    ]
    args, in_specs = list(views), [ANY] * n
    has_total = vec is not None
    if has_total:
        args.append(vec)
        in_specs.append(VMEM)
        out_shape.append(jax.ShapeDtypeStruct(vec.shape, vec.dtype))
        out_specs.append(VMEM)
        box = lambda k: pltpu.VMEM((k - 1,) + vec.shape, vec.dtype)
        t_slots = Total.slots(dims, n_tensor)
        scratch += [pltpu.VMEM((4,) + vec.shape, vec.dtype), box(n_tensor), box(n_c), box(n_b), box(n_a)]
        scratch += [pltpu.SemaphoreType.DMA((t_slots,)), pltpu.SemaphoreType.DMA((t_slots,))]
    out_shape.append(jax.ShapeDtypeStruct((count, n_tensor - 1, n_a, n_b, n_c, rows, chunk), bf))
    out_specs.append(ANY)
    outs = pl.pallas_call(
        functools.partial(scatter_kernel, dims, n_tensor, plan, n, has_total),
        out_shape=out_shape,
        in_specs=in_specs,
        out_specs=out_specs,
        scratch_shapes=scratch,
        compiler_params=pltpu.CompilerParams(
            collective_id=collective_id, has_side_effects=True, vmem_limit_bytes=66_000_000
        ),
        name="scatter_grads",
    )(*args)
    return outs[:n], (outs[n] if has_total else None)


def exchange_kernel(dims, n_tensor, n, *refs):
    ins, outs = refs[:n], refs[n : 2 * n]
    send, recv, local = refs[2 * n :]
    place = Place(dims, n_tensor)

    def copies(i):
        for step in range(1, n_tensor):
            device, _ = place.peer(3, step)
            sems = (send.at[i, step - 1], recv.at[i, step - 1])
            yield remote(ins[i], outs[i].at[n_tensor - step], *sems, device)

    own = [pltpu.make_async_copy(ins[i], outs[i].at[0], local.at[i]) for i in range(n)]
    for copy in own:
        copy.start()
    place.barrier((3,))
    for i in range(n):
        for copy in copies(i):
            copy.start()
    for i in range(n):
        own[i].wait()
        for copy in copies(i):
            copy.wait()


def exchange_rows(arrays, dims, n_tensor, collective_id):
    n = len(arrays)
    outs = pl.pallas_call(
        functools.partial(exchange_kernel, dims, n_tensor, n),
        out_shape=[jax.ShapeDtypeStruct((n_tensor,) + a.shape, a.dtype) for a in arrays],
        in_specs=[VMEM] * n,
        out_specs=[ANY] * n,
        scratch_shapes=[
            pltpu.SemaphoreType.DMA((n, n_tensor - 1)),
            pltpu.SemaphoreType.DMA((n, n_tensor - 1)),
            pltpu.SemaphoreType.DMA((n,)),
        ],
        compiler_params=pltpu.CompilerParams(collective_id=collective_id, has_side_effects=True),
        name="exchange_rows",
    )(*arrays)
    return [o.reshape(-1, o.shape[-1]) for o in outs]


def return_kernel(dims, n_tensor, n, *refs):
    ins, outs, bufs = refs[:n], refs[n : 2 * n], refs[2 * n : 3 * n]
    send, recv = refs[3 * n :]
    place = Place(dims, n_tensor)
    rows = outs[0].shape[0]

    def copies(i):
        for step in range(1, n_tensor):
            device, _ = place.peer(3, step)
            sems = (send.at[i, step - 1], recv.at[i, step - 1])
            yield remote(ins[i].at[pl.ds(step * rows, rows), :], bufs[i].at[step - 1], *sems, device)

    place.barrier((3,))
    for i in range(n):
        for copy in copies(i):
            copy.start()
    for i in range(n):
        for copy in copies(i):
            copy.wait()
        for first in range(0, rows, 64):
            total = ins[i][first : first + 64, :].astype(jnp.float32)
            for step in range(1, n_tensor):
                total = total + bufs[i][step - 1, first : first + 64, :].astype(jnp.float32)
            outs[i][first : first + 64, :] = total.astype(outs[i].dtype)


def return_rows(arrays, dims, n_tensor, collective_id):
    n = len(arrays)
    rows, width = arrays[0].shape[0] // n_tensor, arrays[0].shape[1]
    return pl.pallas_call(
        functools.partial(return_kernel, dims, n_tensor, n),
        out_shape=[jax.ShapeDtypeStruct((rows, width), a.dtype) for a in arrays],
        in_specs=[VMEM] * n,
        out_specs=[VMEM] * n,
        scratch_shapes=[pltpu.VMEM((n_tensor - 1, rows, width), a.dtype) for a in arrays]
        + [pltpu.SemaphoreType.DMA((n, n_tensor - 1)), pltpu.SemaphoreType.DMA((n, n_tensor - 1))],
        compiler_params=pltpu.CompilerParams(collective_id=collective_id, has_side_effects=True),
        name="return_rows",
    )(*arrays)


def norm_forward(stream, gain_row, shift_row):
    centered = stream - jnp.mean(stream, axis=-1, keepdims=True)
    inv_std = lax.rsqrt(jnp.mean(centered * centered, axis=-1, keepdims=True) + EPSILON)
    normed = centered * inv_std
    return (normed * gain_row + shift_row, normed, inv_std)


def norm_backward(grad_result, normed, inv_std, gain_row):
    grad_normed = grad_result * gain_row
    return inv_std * (
        grad_normed
        - jnp.mean(grad_normed, axis=-1, keepdims=True)
        - normed * jnp.mean(grad_normed * normed, axis=-1, keepdims=True)
    )


def low(value):
    return value.astype(jnp.bfloat16)


def ffn_forward(entered, weight_in, weight_out_t):
    before = dot_nn(entered, weight_in)
    active = low(jax.nn.silu(before))
    return dot_nt(active, weight_out_t), (before, active)


def ffn_backward(entered, saved, grad_low, weight_in, weight_out_t):
    before, active = saved
    sigma = jax.nn.sigmoid(before)
    grad_active = dot_nn(grad_low, weight_out_t)
    grad_before = low(grad_active * sigma * (1.0 + before * (1.0 - sigma)))
    grad_in = low(dot_tn(entered, grad_before))
    grad_out_t = low(dot_tn(grad_low, active))
    return dot_nt(grad_before, weight_in), grad_in, grad_out_t


def taps_forward(signal, before, conv_taps):
    rows = signal.shape[0]
    padded = jnp.concatenate([before, signal], axis=0)
    skip = before.shape[0] - (KERNEL - 1)
    result = jnp.zeros_like(signal)
    for tap in range(KERNEL):
        result = result + conv_taps[tap] * padded[skip + tap : skip + tap + rows]
    return result


def taps_backward(grad, after, signal, before, conv_taps):
    rows = signal.shape[0]
    padded_signal = jnp.concatenate([before, signal], axis=0)
    padded_grad = jnp.concatenate([grad, after], axis=0)
    skip = before.shape[0] - (KERNEL - 1)
    grad_signal = jnp.zeros_like(signal)
    taps = []
    for tap in range(KERNEL):
        back = KERNEL - 1 - tap
        grad_signal = grad_signal + conv_taps[tap] * padded_grad[back : back + rows]
        taps.append(jnp.sum(grad * padded_signal[skip + tap : skip + tap + rows], axis=0))
    return grad_signal, jnp.stack(taps)


HALO = 32


def on_device(
    dims,
    n_tensor,
    stream_in,
    grad_out,
    clip_lengths,
    first_up,
    first_down,
    attn_proj,
    attn_out,
    rel_table,
    glu_weight,
    conv_taps,
    conv_out,
    second_up,
    second_down,
    norm_gains,
    norm_shifts,
):
    rank = lax.axis_index("tensor")
    rows, width = stream_in.shape
    keys = rows * n_tensor
    shards = [
        first_up[None], first_down.T[None], attn_proj, attn_out.T[None],
        glu_weight, conv_out.T[None], second_up[None], second_down.T[None],
    ]
    gathered = gather_weights(shards, dims, n_tensor, 0)
    (up_one,), (down_one,), proj, (out_attn,), glu, (out_conv,), (up_two,), (down_two,) = gathered

    def enter(stream, row):
        result, normed, inv_std = norm_forward(stream, norm_gains[row], norm_shifts[row])
        return low(result), (normed, inv_std)

    def norm_back(grad_result, saved, row):
        normed, inv_std = saved
        grad_input = norm_backward(grad_result, normed, inv_std, norm_gains[row])
        return grad_input, jnp.sum(grad_result * normed, axis=0), jnp.sum(grad_result, axis=0)

    def shift_rank(value, step):
        pairs = [(i, i + step) for i in range(n_tensor) if 0 <= i + step < n_tensor]
        return lax.ppermute(value, "tensor", pairs)

    stream = stream_in.astype(jnp.float32)
    squares = []

    entered_a, norm_a = enter(stream, 0)
    branch, ffn_a = ffn_forward(entered_a, up_one, down_one)
    squares.append(jnp.sum(branch * branch))
    stream = stream + 0.5 * branch

    entered_b, norm_b = enter(stream, 1)
    query, own_keys, own_vals = (low(dot_nn(entered_b, proj[i])) for i in range(3))
    key_rows, val_rows = exchange_rows([own_keys, own_vals], dims, n_tensor, 2)
    place = lax.rem(jnp.arange(keys, dtype=jnp.int32) + rank * rows, keys)
    mask = jnp.where(place < clip_lengths[0], 0.0, MASKED).astype(jnp.float32)[None]
    table = span_table(rel_table)
    rank_list = rank.astype(jnp.int32)[None]
    attended, log_totals = attn_fwd(rank_list, query, key_rows, val_rows, table, mask)
    branch = dot_nt(attended, out_attn)
    squares.append(jnp.sum(branch * branch))
    stream = stream + branch

    entered_c, norm_c = enter(stream, 2)
    glu_first = dot_nn(entered_c, glu[0])
    glu_second = dot_nn(entered_c, glu[1])
    sig_second = jax.nn.sigmoid(glu_second)
    gated = glu_first * sig_second
    gated_before = shift_rank(gated[rows - HALO :], 1)
    mixed = taps_forward(gated, gated_before, conv_taps)
    shaped, normed_mid, scale_mid = norm_forward(mixed, norm_gains[3], norm_shifts[3])
    conv_act = low(jax.nn.silu(shaped))
    branch = dot_nt(conv_act, out_conv)
    squares.append(jnp.sum(branch * branch))
    stream = stream + branch

    entered_d, norm_d = enter(stream, 4)
    branch, ffn_d = ffn_forward(entered_d, up_two, down_two)
    squares.append(jnp.sum(branch * branch))
    stream = stream + 0.5 * branch
    squares.append(jnp.sum(stream * stream))
    result, normed_e, scale_e = norm_forward(stream, norm_gains[5], norm_shifts[5])
    output = low(result)

    grad_stream, gain_e, shift_e = norm_back(grad_out.astype(jnp.float32), (normed_e, scale_e), 5)
    grad_low = low(0.5 * grad_stream)
    grad_entered, grad_up_two, grad_down_two = ffn_backward(entered_d, ffn_d, grad_low, up_two, down_two)
    grad_extra, gain_d, shift_d = norm_back(grad_entered, norm_d, 4)
    grad_stream = grad_stream + grad_extra

    grad_low = low(grad_stream)
    grad_conv_out = low(dot_tn(grad_low, conv_act))
    sigma = jax.nn.sigmoid(shaped)
    grad_shaped = dot_nn(grad_low, out_conv) * sigma * (1.0 + shaped * (1.0 - sigma))
    grad_mixed, gain_mid, shift_mid = norm_back(grad_shaped, (normed_mid, scale_mid), 3)
    grad_after = shift_rank(grad_mixed[:HALO], -1)
    grad_gated, taps_grad = taps_backward(grad_mixed, grad_after, gated, gated_before, conv_taps)
    grad_first = low(grad_gated * sig_second)
    grad_second = low(grad_gated * glu_first * sig_second * (1.0 - sig_second))
    grad_glu = [low(dot_tn(entered_c, g)) for g in (grad_first, grad_second)]
    grad_entered = dot_nt(grad_first, glu[0]) + dot_nt(grad_second, glu[1])
    grad_extra, gain_c, shift_c = norm_back(grad_entered, norm_c, 2)
    grad_stream = grad_stream + grad_extra

    grad_low = low(grad_stream)
    grad_attn_out = low(dot_tn(grad_low, attended))
    grad_attended = low(dot_nn(grad_low, out_attn))
    grad_query, grad_keys, grad_vals, grad_span = attn_bwd(
        rank_list, query, key_rows, val_rows, grad_attended, attended, log_totals, table, mask
    )
    grad_keys, grad_vals = return_rows([grad_keys, grad_vals], dims, n_tensor, 3)
    grad_parts = (grad_query, grad_keys, grad_vals)
    grad_proj = [low(dot_tn(entered_b, g)) for g in grad_parts]
    grad_entered = sum(dot_nt(g, proj[i]) for i, g in enumerate(grad_parts))
    grad_extra, gain_b, shift_b = norm_back(grad_entered, norm_b, 1)
    grad_stream = grad_stream + grad_extra

    grad_low = low(0.5 * grad_stream)
    grad_entered, grad_up_one, grad_down_one = ffn_backward(entered_a, ffn_a, grad_low, up_one, down_one)
    grad_extra, gain_a, shift_a = norm_back(grad_entered, norm_a, 0)
    grad_stream = grad_stream + grad_extra

    span_grad = fold_table(grad_span)
    span_rows = -(-span_grad.size // width)
    table_rows = jnp.pad(span_grad.reshape(-1), (0, span_rows * width - span_grad.size)).reshape(span_rows, width)
    square_row = jnp.pad(jnp.stack(squares), (0, width - len(squares)))[None]
    parts = [
        jnp.stack([gain_a, gain_b, gain_c, gain_mid, gain_d, gain_e]),
        jnp.stack([shift_a, shift_b, shift_c, shift_mid, shift_d, shift_e]),
        taps_grad,
        table_rows,
        square_row,
    ]
    vec = jnp.concatenate(parts, axis=0)
    vec = jnp.pad(vec, ((0, -vec.shape[0] % 8), (0, 0)))
    grads = [
        grad_down_two, grad_up_two, grad_conv_out, *grad_glu, grad_attn_out, *grad_proj, grad_down_one, grad_up_one,
    ]
    summed, vec = scatter_grads([g[None] for g in grads], vec, dims, n_tensor, 1)
    s_down_two, s_up_two, s_conv, s_glu0, s_glu1, s_attn, s_q, s_k, s_v, s_down_one, s_up_one = (s[0] for s in summed)
    at = 0
    pieces = []
    for part in parts:
        pieces.append(vec[at : at + part.shape[0]])
        at += part.shape[0]
    gains_sum, shifts_sum, taps_sum, table_sum, square_sum = pieces
    table_sum = table_sum.reshape(-1)[: span_grad.size].reshape(span_grad.shape)
    count_all = float(lax.axis_size("dp") * keys * width)
    rms_values = jnp.sqrt(square_sum[0, : len(squares)] / count_all)
    return (
        output,
        grad_stream,
        s_up_one,
        s_down_one.T,
        jnp.stack([s_q, s_k, s_v]),
        s_attn.T,
        table_sum,
        jnp.stack([s_glu0, s_glu1]),
        taps_sum,
        s_conv.T,
        s_up_two,
        s_down_two.T,
        gains_sum,
        shifts_sum,
        rms_values,
    )


def solution(mesh):
    n_dp, n_tensor = mesh.shape["dp"], mesh.shape["tensor"]
    dims = FACTORS.get(n_dp, (n_dp, 1, 1))
    return jax.shard_map(
        functools.partial(on_device, dims, n_tensor),
        mesh=mesh,
        in_specs=(
            P(("dp", "tensor"), None),
            P(("dp", "tensor"), None),
            P("dp"),
            P("dp", "tensor"),
            P("tensor", "dp"),
            P(None, "dp", "tensor"),
            P("tensor", "dp"),
            P(),
            P(None, "dp", "tensor"),
            P(),
            P("tensor", "dp"),
            P("dp", "tensor"),
            P("tensor", "dp"),
            P(),
            P(),
        ),
        out_specs=(
            P(("dp", "tensor"), None),
            P(("dp", "tensor"), None),
            P("dp", "tensor"),
            P("tensor", "dp"),
            P(None, "dp", "tensor"),
            P("tensor", "dp"),
            P(),
            P(None, "dp", "tensor"),
            P(),
            P("tensor", "dp"),
            P("dp", "tensor"),
            P("tensor", "dp"),
            P(),
            P(),
            P(),
        ),
        check_vma=False,
    )
```

```python
import functools

import jax
import jax.numpy as jnp
from jax import lax
from jax.experimental import pallas as pl
from jax.experimental.pallas import tpu as pltpu
from jax.sharding import PartitionSpec as P

HEAD = 64
KERNEL = 31
LEFT = 64
RIGHT = 8
EPSILON = 1e-05
MASKED = -1e30
VMEM_LIMIT = 66_000_000
HOST_G = (512, 6, 5)
HOST_S = (256, 8, 6)
BLK = 128
SPAN = 512
NT = (((1,), (1,)), ((), ()))
TN = (((0,), (0,)), ((), ()))


def dot_nt(a, b):
    return lax.dot_general(a, b, NT, preferred_element_type=jnp.float32)


def dot_tn(a, b):
    return lax.dot_general(a, b, TN, preferred_element_type=jnp.float32)


def dot_nn(a, b):
    return jnp.dot(a, b, preferred_element_type=jnp.float32)


def rel_blocks(tin, b, own_blocks, key_blocks, rank):
    t_left, t_right = tin[:, 0:1], tin[:, SPAN - 1 : SPAN]
    band = pltpu.roll(tin, SPAN - BLK, 1, stride=1, stride_axis=0)
    out = []
    for kb in range(key_blocks):
        wraps = rank * own_blocks + kb >= key_blocks
        if kb in (b - 1, b) or (kb == b + 1 and kb < own_blocks):
            out.append(band[:, (kb - b + 1) * BLK : (kb - b + 2) * BLK])
        elif kb == b + 1:
            out.append(jnp.where(wraps, t_left, band[:, 2 * BLK : 3 * BLK]))
        elif b == 0 and kb == key_blocks - 1:
            out.append(jnp.where(wraps, band[:, :BLK], t_right))
        elif kb < b - 1:
            out.append(t_left)
        elif kb < own_blocks:
            out.append(t_right)
        else:
            out.append(jnp.where(wraps, t_left, t_right))
    return out


def halves(x):
    low = lax.broadcasted_iota(jnp.int32, x.shape, 1) < HEAD
    zero = jnp.zeros_like(x)
    return jnp.where(low, x, zero), jnp.where(low, zero, x)


def flip_rows(x):
    tiles = []
    back = 7 - lax.broadcasted_iota(jnp.int32, (8, BLK), 0)
    for first in range(x.shape[0] - 8, -1, -8):
        cols = [
            jnp.take_along_axis(x[first : first + 8, c : c + BLK], back, axis=0, mode="promise_in_bounds")
            for c in range(0, x.shape[1], BLK)
        ]
        tiles.append(jnp.concatenate(cols, axis=1) if len(cols) > 1 else cols[0])
    return jnp.concatenate(tiles, axis=0)


def split_refs(refs, sizes):
    out, at = [], 0
    for size in sizes:
        out.append(refs[at : at + size])
        at += size
    return out


def ticker(plan, ins, outs, scratch, ticks):
    if plan is None:
        return lambda block, blocks: None
    steps = plan.steps(ins, outs, scratch)

    def tick(block, blocks):
        for number, step in enumerate(steps):
            at = min(number * ticks // (len(steps) - 1), ticks - 1) if number < len(steps) - 1 else ticks
            if at < ticks and at % blocks == block:
                pl.when(pl.program_id(0) == at // blocks)(step)
            if at == ticks and block == blocks:
                pl.when(pl.program_id(0) == ticks // blocks - 1)(step)

    return tick


def attn_fwd_kernel(plan, *refs):
    n_in, n_out = (len(plan.in_specs), len(plan.out_specs)) if plan else (0, 0)
    own, plan_in, (o_ref, lse_ref), plan_out, plan_scratch = split_refs(refs, (5, n_in, 2, n_out, len(refs)))
    q_ref, k_ref, v_ref, tab_ref, mask_ref = own
    rank = lax.axis_index("tensor")
    rows, keys = q_ref.shape[0], k_ref.shape[0]
    own_blocks, key_blocks = rows // BLK, keys // BLK
    low = lax.broadcasted_iota(jnp.int32, (BLK, 2 * HEAD), 1) < HEAD
    tick = ticker(plan, plan_in, plan_out, plan_scratch, own_blocks * pl.num_programs(0))
    for b in range(own_blocks):
        tick(b, own_blocks)
        q_blk = q_ref[b * BLK : (b + 1) * BLK, :] * jnp.asarray(HEAD**-0.5, jnp.bfloat16)
        results = []
        for hh, q_one in enumerate(halves(q_blk)):
            tin = dot_nt(q_one, tab_ref[...])
            rel = rel_blocks(tin, b, own_blocks, key_blocks, rank)
            raw = dot_nt(q_one, k_ref[...])
            s = [
                raw[:, kb * BLK : (kb + 1) * BLK] + rel[kb] + mask_ref[:, kb * BLK : (kb + 1) * BLK]
                for kb in range(key_blocks)
            ]
            s = jnp.concatenate(s, axis=1)
            peak = jnp.max(s, axis=-1, keepdims=True)
            e = jnp.exp(s - peak)
            total = jnp.sum(e, axis=-1, keepdims=True)
            o = dot_nn(e.astype(jnp.bfloat16), v_ref[...])
            results.append(o / total)
            first = (hh * own_blocks + b) * BLK
            lse_ref[0, first : first + BLK, :] = peak + jnp.log(total)
        o_ref[b * BLK : (b + 1) * BLK, :] = jnp.where(low, results[0], results[1]).astype(jnp.bfloat16)
    tick(own_blocks, own_blocks)


def attn_fwd(q, k, v, tab2, mask, plan=None, collective_id=None):
    rows, width = q.shape
    keys = k.shape[0]
    pairs = width // (2 * HEAD)
    col = lambda n: pl.BlockSpec((n, 2 * HEAD), lambda p: (0, p))
    out_specs = [col(rows), pl.BlockSpec((1, 2 * rows, 1), lambda p: (p, 0, 0))]
    out_shape = [
        jax.ShapeDtypeStruct((rows, width), jnp.bfloat16),
        jax.ShapeDtypeStruct((pairs, 2 * rows, 1), jnp.float32),
    ]
    outs = pl.pallas_call(
        functools.partial(attn_fwd_kernel, plan),
        grid=(pairs,),
        in_specs=[
            col(rows),
            col(keys),
            col(keys),
            pl.BlockSpec((SPAN, 2 * HEAD), lambda p: (0, 0)),
            pl.BlockSpec((1, keys), lambda p: (0, 0)),
        ]
        + (plan.in_specs if plan else []),
        out_specs=out_specs + (plan.out_specs if plan else []),
        out_shape=out_shape + (plan.out_shape if plan else []),
        scratch_shapes=plan.scratch if plan else [],
        compiler_params=pltpu.CompilerParams(
            collective_id=collective_id, has_side_effects=plan is not None, vmem_limit_bytes=VMEM_LIMIT
        ),
        name="attn_fwd",
    )(q, k, v, tab2, mask, *(plan.args if plan else []))
    return outs[0], outs[1], plan.results(outs[2:]) if plan else []


def attn_bwd_kernel(plan, *refs):
    n_in, n_out = (len(plan.in_specs), len(plan.out_specs)) if plan else (0, 0)
    own, plan_in, own_out, plan_out, own_scratch, plan_scratch = split_refs(refs, (8, n_in, 4, n_out, 4, len(refs)))
    q_ref, k_ref, v_ref, do_ref, o_ref, lse_ref, tab_ref, mask_ref = own
    dq_ref, dk_ref, dv_ref, dtab_ref = own_out
    p_sc, ds_sc, q_sc, do_sc = own_scratch
    rank = lax.axis_index("tensor")
    rows, keys = q_ref.shape[0], k_ref.shape[0]
    own_blocks, key_blocks = rows // BLK, keys // BLK
    low = lax.broadcasted_iota(jnp.int32, (BLK, 2 * HEAD), 1) < HEAD
    lane = lax.broadcasted_iota(jnp.int32, (BLK, BLK), 1)
    scale = jnp.asarray(HEAD**-0.5, jnp.bfloat16)

    @pl.when(pl.program_id(0) == 0)
    def _():
        dtab_ref[...] = jnp.zeros_like(dtab_ref)

    tick = ticker(plan, plan_in, plan_out, plan_scratch, own_blocks * pl.num_programs(0))
    for b in range(own_blocks):
        tick(b, own_blocks)
        at = slice(b * BLK, (b + 1) * BLK)
        q_blk = q_ref[at, :] * scale
        do_blk = do_ref[at, :]
        prod = do_blk.astype(jnp.float32) * o_ref[at, :].astype(jnp.float32)
        q_back = halves(flip_rows(q_blk.astype(jnp.float32)).astype(jnp.bfloat16))
        results = []
        for hh, (q_one, do_one, pr_one) in enumerate(zip(halves(q_blk), halves(do_blk), halves(prod))):
            first = (hh * own_blocks + b) * BLK
            here = slice(first, first + BLK)
            inner = jnp.sum(pr_one, axis=-1, keepdims=True)
            lse = lse_ref[0, here, :]
            tin = dot_nt(q_one, tab_ref[...])
            rel = rel_blocks(tin - lse, b, own_blocks, key_blocks, rank)
            raw = dot_nt(q_one, k_ref[...])
            dp = dot_nt(do_one, v_ref[...])
            left = jnp.zeros((BLK, BLK), jnp.float32)
            right = jnp.zeros((BLK, BLK), jnp.float32)
            window = [None, None, None]
            for kb in range(key_blocks):
                ks = slice(kb * BLK, (kb + 1) * BLK)
                p = jnp.exp(raw[:, ks] + rel[kb] + mask_ref[:, ks])
                ds = (p * (dp[:, ks] - inner)).astype(jnp.bfloat16)
                p_sc[here, ks] = p.astype(jnp.bfloat16)
                ds_sc[here, ks] = ds
                ds = ds.astype(jnp.float32)
                wraps = rank * own_blocks + kb >= key_blocks
                zero = jnp.zeros_like(ds)
                if kb in (b - 1, b) or (kb == b + 1 and kb < own_blocks):
                    window[kb - b + 1] = ds
                elif kb == b + 1:
                    window[2] = jnp.where(wraps, zero, ds)
                    left = left + jnp.where(wraps, ds, zero)
                elif b == 0 and kb == key_blocks - 1:
                    window[0] = jnp.where(wraps, ds, zero)
                    right = right + jnp.where(wraps, zero, ds)
                elif kb < b - 1:
                    left = left + ds
                elif kb < own_blocks:
                    right = right + ds
                else:
                    left = left + jnp.where(wraps, ds, zero)
                    right = right + jnp.where(wraps, zero, ds)
            none = jnp.zeros((BLK, BLK), jnp.float32)
            window = jnp.concatenate([none if w is None else flip_rows(w) for w in window] + [none], axis=1)
            back = pltpu.roll(window, 1, 1, stride=1, stride_axis=0)
            s_left = flip_rows(jnp.broadcast_to(jnp.sum(left, axis=-1, keepdims=True), (BLK, BLK)))
            s_right = flip_rows(jnp.broadcast_to(jnp.sum(right, axis=-1, keepdims=True), (BLK, BLK)))
            u = jnp.concatenate(
                [
                    back[:, :BLK] + jnp.where(lane == 0, s_left, 0.0),
                    back[:, BLK : 3 * BLK],
                    back[:, 3 * BLK :] + jnp.where(lane == BLK - 1, s_right, 0.0),
                ],
                axis=1,
            ).astype(jnp.bfloat16)
            q_sc[here, :] = q_one
            do_sc[here, :] = do_one
            dtab_ref[...] += dot_tn(u, q_back[hh])
            results.append(dot_nn(ds_sc[here, :], k_ref[...]) + flip_rows(dot_nn(u, tab_ref[...])))
        dq_ref[at, :] = (jnp.where(low, results[0], results[1]) * HEAD**-0.5).astype(jnp.bfloat16)
    dk_ref[...] = dot_tn(ds_sc[...], q_sc[...]).astype(dk_ref.dtype)
    dv_ref[...] = dot_tn(p_sc[...], do_sc[...]).astype(dv_ref.dtype)
    tick(own_blocks, own_blocks)


def attn_bwd(q, k, v, do, o, lse, tab2, mask, plan=None, collective_id=None):
    rows, width = q.shape
    keys = k.shape[0]
    pairs = width // (2 * HEAD)
    col = lambda n: pl.BlockSpec((n, 2 * HEAD), lambda p: (0, p))
    table = pl.BlockSpec((SPAN, 2 * HEAD), lambda p: (0, 0))
    out_shape = [
        jax.ShapeDtypeStruct((rows, width), jnp.bfloat16),
        jax.ShapeDtypeStruct((keys, width), jnp.bfloat16),
        jax.ShapeDtypeStruct((keys, width), jnp.bfloat16),
        jax.ShapeDtypeStruct((SPAN, 2 * HEAD), jnp.float32),
    ]
    outs = pl.pallas_call(
        functools.partial(attn_bwd_kernel, plan),
        grid=(pairs,),
        in_specs=[
            col(rows),
            col(keys),
            col(keys),
            col(rows),
            col(rows),
            pl.BlockSpec((1, 2 * rows, 1), lambda p: (p, 0, 0)),
            table,
            pl.BlockSpec((1, keys), lambda p: (0, 0)),
        ]
        + (plan.in_specs if plan else []),
        out_specs=[col(rows), col(keys), col(keys), table] + (plan.out_specs if plan else []),
        out_shape=out_shape + (plan.out_shape if plan else []),
        scratch_shapes=[
            pltpu.VMEM((2 * rows, keys), jnp.bfloat16),
            pltpu.VMEM((2 * rows, keys), jnp.bfloat16),
            pltpu.VMEM((2 * rows, 2 * HEAD), jnp.bfloat16),
            pltpu.VMEM((2 * rows, 2 * HEAD), jnp.bfloat16),
        ]
        + (plan.scratch if plan else []),
        compiler_params=pltpu.CompilerParams(
            collective_id=collective_id, has_side_effects=plan is not None, vmem_limit_bytes=VMEM_LIMIT
        ),
        name="attn_bwd",
    )(q, k, v, do, o, lse, tab2, mask, *(plan.args if plan else []))
    return (*outs[:4], plan.results(outs[4:]) if plan else [])


def span_table(rel_table):
    rows = jnp.clip(jnp.arange(SPAN) - SPAN // 2, -LEFT, RIGHT) + LEFT
    table = jnp.take(rel_table, rows, axis=0)
    return jnp.concatenate([table, table], axis=1)


def fold_table(dtab):
    one = dtab[:, :HEAD] + dtab[:, HEAD:]
    rows = jnp.clip(jnp.arange(SPAN) - SPAN // 2, -LEFT, RIGHT) + LEFT
    pick = (rows[None, :] == jnp.arange(LEFT + RIGHT + 1)[:, None]).astype(jnp.float32)
    return jnp.dot(pick, one, precision=lax.Precision.HIGHEST)


MESH = pl.DeviceIdType.MESH
ANY = pl.BlockSpec(memory_space=pl.ANY)
VMEM = pl.BlockSpec(memory_space=pltpu.VMEM)
FACTORS = {16: (4, 2, 2), 32: (4, 2, 4)}


class Place:
    def __init__(self, dims, n_tensor):
        self.dims, self.n_tensor = dims, n_tensor
        n_a, n_b, n_c = dims
        d = lax.axis_index("dp")
        self.t = lax.axis_index("tensor")
        self.at = (lax.div(d, n_b * n_c), lax.rem(lax.div(d, n_c), n_b), lax.rem(d, n_c))

    def peer(self, axis, step):
        at, t = list(self.at), self.t
        if axis == 3:
            t = lax.rem(t + step, self.n_tensor)
            index = t
        else:
            at[axis] = index = lax.rem(at[axis] + step, self.dims[axis])
        n_a, n_b, n_c = self.dims
        return ((at[0] * n_b + at[1]) * n_c + at[2], t), index

    def size(self, axis):
        return self.n_tensor if axis == 3 else self.dims[axis]

    def barrier(self, axes=(0, 1, 2, 3)):
        sem = pltpu.get_barrier_semaphore()
        count = 0
        for axis in axes:
            for step in range(1, self.size(axis)):
                pl.semaphore_signal(sem, inc=1, device_id=self.peer(axis, step)[0], device_id_type=MESH)
                count += 1
        pl.semaphore_wait(sem, count)


def remote(src, dst, send_sem, recv_sem, device):
    return pltpu.make_async_remote_copy(
        src_ref=src, dst_ref=dst, send_sem=send_sem, recv_sem=recv_sem, device_id=device, device_id_type=MESH
    )


class Piece:
    def __init__(self, source, lead, first, width):
        self.source, self.lead, self.first, self.width = source, lead, first, width


def pieces_of(parts, chunk):
    return [
        Piece(source, lead, first, min(chunk, cols - first))
        for source, (n, cols) in enumerate(parts)
        for lead in range(n)
        for first in range(0, cols, chunk)
    ]


def run_all(copies, action):
    for copy in copies:
        getattr(copy, action)()


class Gather:
    NORMAL = ((0, 1, 2), (0, 2, 1))
    EARLY = ((2, 1, 0), (1, 2, 0))

    def __init__(self, place, piece, orders, shard, whole, send, recv, local):
        self.place, self.piece, self.orders = place, piece, orders
        self.shard, self.whole = shard, whole
        self.send, self.recv, self.local = send, recv, local
        self.half = shard.shape[1] // 2

    @staticmethod
    def slots(dims, n_tensor):
        return 2 * (sum(d - 1 for d in dims) + 2 * (n_tensor - 1))

    def slot(self, color, stage, step):
        place, order = self.place, self.orders[color]
        sizes = [place.dims[x] - 1 for x in order] + [place.n_tensor - 1] * 2
        return color * sum(sizes) + sum(sizes[:stage]) + step - 1

    def columns(self, t):
        piece = self.piece
        return pl.ds(pl.multiple_of(t * self.shard.shape[2] + piece.first, 128), piece.width)

    def region(self, color, index, t):
        rows = pl.ds(color * self.half, self.half)
        return self.whole.at[(self.piece.lead,) + tuple(index) + (rows, self.columns(t))]

    def source(self, rows):
        piece = self.piece
        return self.shard.at[piece.lead, rows, pl.ds(piece.first, piece.width)]

    def index(self, color, stage, moved=None):
        order, out = self.orders[color], list(self.place.at)
        for axis in order[:stage]:
            out[axis] = slice(None)
        if moved is not None:
            out[order[stage]] = moved
        return out

    def own(self):
        there = self.whole.at[(self.piece.lead,) + self.place.at + (slice(None), self.columns(self.place.t))]
        return pltpu.make_async_copy(self.source(slice(None)), there, self.local)

    def copies(self, stage, arriving=False):
        place, t = self.place, self.place.t
        for color, order in enumerate(self.orders):
            in_one = place.dims[order[2]] > 2
            if stage == 3 and in_one:
                continue
            axis = order[stage] if stage < 3 else 3
            for step in range(1, place.size(axis)):
                device, _ = place.peer(axis, step)
                _, origin = place.peer(axis, place.size(axis) - step)
                slot = self.slot(color, stage, step)
                if stage < 3:
                    index, there, then = self.index(color, stage), self.index(color, stage, origin), t
                else:
                    if in_one:
                        index = self.index(color, 3)
                    elif stage == 3:
                        index = self.index(color, 2)
                    else:
                        index = self.index(color, 2, place.peer(order[2], 1)[1])
                    there, then = index, origin
                mine, theirs = self.region(color, index, t), self.region(color, there, then)
                origin_ref = self.source(pl.ds(color * self.half, self.half)) if stage == 0 else mine
                sems = (self.send.at[slot], self.recv.at[slot], device)
                yield remote(theirs, theirs, *sems) if arriving else remote(origin_ref, mine, *sems)

    def start(self, stage):
        run_all(self.copies(stage), "start")

    def arrived(self, stage):
        run_all(self.copies(stage, arriving=True), "wait_recv")

    def sent(self, stage):
        run_all(self.copies(stage), "wait_send")


class GatherPlan:
    def __init__(self, shards, dims, n_tensor, chunk=1024, every=6, depth=3):
        self.dims, self.n_tensor, self.depth = dims, n_tensor, depth
        self.args = list(shards)
        self.pieces = pieces_of([(s.shape[0], s.shape[2]) for s in shards], chunk)
        self.orders = [Gather.EARLY if i % every == 0 else Gather.NORMAL for i in range(len(self.pieces))]
        count, slots = len(self.pieces), Gather.slots(dims, n_tensor)
        self.in_specs = [VMEM] * len(shards)
        self.out_specs = [ANY] * len(shards)
        self.out_shape = [
            jax.ShapeDtypeStruct((s.shape[0], *dims, s.shape[1], n_tensor * s.shape[2]), s.dtype) for s in shards
        ]
        self.scratch = [
            pltpu.SemaphoreType.DMA((count, slots)),
            pltpu.SemaphoreType.DMA((count, slots)),
            pltpu.SemaphoreType.DMA((count,)),
        ]

    def results(self, outs):
        return [o.reshape(o.shape[0], -1, o.shape[-1]) for o in outs]

    def steps(self, shards, wholes, scratch):
        send, recv, local = scratch
        place = Place(self.dims, self.n_tensor)
        gathers = [
            Gather(place, p, orders, shards[p.source], wholes[p.source], send.at[i], recv.at[i], local.at[i])
            for i, (p, orders) in enumerate(zip(self.pieces, self.orders))
        ]
        count, depth = len(gathers), self.depth

        def begin():
            for g in gathers:
                g.own().start()
            place.barrier()
            for g in gathers:
                g.start(0)
            for g in gathers:
                g.own().wait()

        def step(i):
            if i < count:
                gathers[i].arrived(0)
                gathers[i].start(1)
            at = i - depth
            if 0 <= at < count:
                gathers[at].arrived(1)
                gathers[at].start(2)
                gathers[at].start(3)
            at = i - 2 * depth
            if 0 <= at < count:
                gathers[at].arrived(2)
                gathers[at].start(4)

        def end():
            for g in gathers:
                g.arrived(3)
                g.arrived(4)
                for stage in range(5):
                    g.sent(stage)

        return [begin] + [functools.partial(step, i) for i in range(count + 2 * depth)] + [end]


class Scatter:
    NORMAL = ((2, 1, 0), (1, 2, 0))
    EARLY = ((0, 1, 2), (0, 2, 1))

    def __init__(self, place, piece, orders, grad, out, held, far, near, bufs, sems):
        self.place, self.piece, self.orders = place, piece, orders
        self.grad, self.out = grad, out
        self.held, self.far, self.near, self.bufs = held, far, near, bufs
        self.send, self.recv, self.local = sems
        self.half = held.shape[3] // 2

    @staticmethod
    def slots(dims, n_tensor):
        return n_tensor - 1 + 2 * sum(d - 1 for d in dims)

    @staticmethod
    def left(order, stage):
        return [x for x in (0, 1, 2) if x not in order[:stage]]

    def slab(self, t):
        piece = self.piece
        first = t * (self.grad.shape[-1] // self.place.n_tensor) + piece.first
        return self.grad.at[piece.lead, :, :, :, :, pl.ds(pl.multiple_of(first, 128), piece.width)]

    def load(self):
        return pltpu.make_async_copy(self.slab(self.place.t), self.held, self.local.at[0])

    def near_loads(self):
        for step in range(1, self.place.n_tensor):
            yield pltpu.make_async_copy(self.far.at[step - 1], self.near.at[step - 1], self.local.at[step])

    def copies(self, stage):
        place = self.place
        if stage == 0:
            for step in range(1, place.n_tensor):
                device, peer = place.peer(3, step)
                sems = (self.send.at[step - 1], self.recv.at[step - 1], device)
                yield remote(self.slab(peer), self.far.at[step - 1], *sems)
            return
        base = place.n_tensor - 1
        for color, order in enumerate(self.orders):
            axis = order[stage - 1]
            for step in range(1, place.size(axis)):
                device, there = place.peer(axis, step)
                index = [slice(None)] * 3
                for done in order[: stage - 1]:
                    index[done] = place.at[done]
                index[axis] = there
                slot = base + color * sum(d - 1 for d in place.dims)
                slot += sum(place.size(x) - 1 for x in order[: stage - 1]) + step - 1
                origin = self.held.at[tuple(index) + (pl.ds(color * self.half, self.half),)]
                sems = (self.send.at[slot], self.recv.at[slot], device)
                yield remote(origin, self.bufs[stage - 1][color].at[step - 1], *sems)

    def add_tensor(self):
        n_a, n_b, n_c = self.place.dims

        def body(i, _):
            at = (lax.div(i, n_b * n_c), lax.rem(lax.div(i, n_c), n_b), lax.rem(i, n_c))
            total = self.held[at].astype(jnp.float32)
            for step in range(1, self.place.n_tensor):
                total = total + self.near[(step - 1,) + at].astype(jnp.float32)
            self.held[at] = total.astype(jnp.bfloat16)
            return 0

        lax.fori_loop(0, n_a * n_b * n_c, body, 0)

    def add(self, stage):
        place, piece = self.place, self.piece
        for color, order in enumerate(self.orders):
            rows = slice(color * self.half, (color + 1) * self.half)
            left = self.left(order, stage)
            buf = self.bufs[stage - 1][color]

            def total_at(where):
                at = list(place.at)
                for x, w in zip(left, where):
                    at[x] = w
                at = tuple(at) + (rows,)
                total = self.held[at].astype(jnp.float32)
                for step in range(1, place.size(order[stage - 1])):
                    total = total + buf[(step - 1,) + where].astype(jnp.float32)
                return at, total

            def body(i, _):
                if len(left) == 2:
                    size = place.dims[left[1]]
                    at, total = total_at((lax.div(i, size), lax.rem(i, size)))
                else:
                    at, total = total_at((i,))
                self.held[at] = total.astype(jnp.bfloat16)
                return 0

            if left:
                count = 1
                for x in left:
                    count *= place.dims[x]
                lax.fori_loop(0, count, body, 0)
            else:
                cols = slice(piece.first, piece.first + piece.width)
                self.out[piece.lead, rows, cols] = total_at(())[1]


class Total:
    AXES = (3, 2, 1, 0)

    def __init__(self, place, value, out, boxes, send, recv):
        self.place, self.value, self.out, self.boxes, self.send, self.recv = place, value, out, boxes, send, recv

    @staticmethod
    def slots(dims, n_tensor):
        return sum(dims) + n_tensor - 4

    def copies(self, stage):
        place, axis = self.place, self.AXES[stage]
        base = sum(place.size(x) - 1 for x in self.AXES[:stage])
        for step in range(1, place.size(axis)):
            device, _ = place.peer(axis, step)
            sems = (self.send.at[base + step - 1], self.recv.at[base + step - 1], device)
            yield remote(self.value.at[stage], self.boxes[stage].at[step - 1], *sems)

    def add(self, stage):
        place, axis = self.place, self.AXES[stage]
        size = place.size(axis)
        mine = place.t if axis == 3 else place.at[axis]
        own = self.value[stage]
        if size == 2:
            total = own + self.boxes[stage][0]
        else:
            total = jnp.zeros_like(own)
            for index in range(size):
                step = lax.rem(mine - index + size, size)
                term = self.boxes[stage][jnp.maximum(step - 1, 0)]
                total = total + jnp.where(step == 0, own, term)
        if stage == 3:
            self.out[...] = total
        else:
            self.value[stage + 1] = total


class ScatterPlan:
    def __init__(self, grads, vec, dims, n_tensor, chunk=512, every=6, depth=2):
        self.dims, self.n_tensor, self.has_total = dims, n_tensor, vec is not None
        self.depth = depth
        n_a, n_b, n_c = dims
        rows = grads[0].shape[1] // (n_a * n_b * n_c)
        parts = [(g.shape[0], g.shape[2] // n_tensor) for g in grads]
        chunk = min(chunk, *(cols for _, cols in parts))
        self.pieces = pieces_of(parts, chunk)
        count, slots = len(self.pieces), Scatter.slots(dims, n_tensor)
        kinds = [0 if i % every else 1 for i in range(count)]
        self.places = [(k, kinds[:i].count(k)) for i, k in enumerate(kinds)]
        self.args = [g.reshape(g.shape[0], n_a, n_b, n_c, rows, g.shape[2]) for g in grads]
        self.in_specs = [ANY] * len(grads)
        self.out_shape = [jax.ShapeDtypeStruct((g.shape[0], rows, g.shape[2] // n_tensor), jnp.float32) for g in grads]
        self.out_specs = [VMEM] * len(grads)
        bf, half = jnp.bfloat16, rows // 2
        self.scratch = [
            pltpu.VMEM((count, n_a, n_b, n_c, rows, chunk), bf),
            pltpu.VMEM((2, n_tensor - 1, n_a, n_b, n_c, rows, chunk), bf),
            pltpu.SemaphoreType.DMA((count, slots)),
            pltpu.SemaphoreType.DMA((count, slots)),
            pltpu.SemaphoreType.DMA((count, n_tensor)),
        ]
        for kind, orders in enumerate((Scatter.NORMAL, Scatter.EARLY)):
            for stage in (1, 2, 3):
                for order in orders:
                    left = [dims[x] for x in Scatter.left(order, stage)]
                    shape = (max(kinds.count(kind), 1), dims[order[stage - 1]] - 1, *left, half, chunk)
                    self.scratch.append(pltpu.VMEM(shape, bf))
        if self.has_total:
            self.args.append(vec)
            self.in_specs.append(VMEM)
            self.out_shape.append(jax.ShapeDtypeStruct(vec.shape, vec.dtype))
            self.out_specs.append(VMEM)
            self.scratch.append(pltpu.VMEM((4,) + vec.shape, vec.dtype))
            self.scratch += [pltpu.VMEM((k - 1,) + vec.shape, vec.dtype) for k in (n_tensor, n_c, n_b, n_a)]
            self.scratch += [pltpu.SemaphoreType.DMA((Total.slots(dims, n_tensor),))] * 2
        self.out_shape.append(jax.ShapeDtypeStruct((count, n_tensor - 1, n_a, n_b, n_c, rows, chunk), bf))
        self.out_specs.append(ANY)

    def results(self, outs):
        return list(outs[:-1])

    def steps(self, ins, outs, scratch):
        place = Place(self.dims, self.n_tensor)
        far = outs[-1]
        held, near, send, recv, local = scratch[:5]
        chunks = []
        for i, (piece, (kind, at)) in enumerate(zip(self.pieces, self.places)):
            orders = (Scatter.NORMAL, Scatter.EARLY)[kind]
            boxes = scratch[5 + 6 * kind : 11 + 6 * kind]
            bufs = [[boxes[2 * stage + color].at[at] for color in (0, 1)] for stage in range(3)]
            chunks.append(
                Scatter(
                    place, piece, orders, ins[piece.source], outs[piece.source], held.at[i], far.at[i],
                    near.at[i % 2], bufs, (send.at[i], recv.at[i], local.at[i]),
                )
            )
        count, depth = len(chunks), self.depth
        total = None
        if self.has_total:
            value, *rest = scratch[17:]
            total = Total(place, value, outs[-2], rest[:4], rest[4], rest[5])

        def fetch(i):
            run_all(chunks[i].copies(0), "wait_recv")
            run_all(chunks[i].near_loads(), "start")

        def begin():
            for c in chunks:
                c.load().start()
            if total is not None:
                value[0] = ins[-1][...]
            place.barrier()
            if total is not None:
                run_all(total.copies(0), "start")
            for c in chunks:
                run_all(c.copies(0), "start")

        def step(i):
            if i == 0:
                fetch(0)
            if i < count:
                chunks[i].load().wait()
                run_all(chunks[i].near_loads(), "wait")
                if i + 1 < count:
                    fetch(i + 1)
                chunks[i].add_tensor()
                run_all(chunks[i].copies(1), "start")
            for stage in (1, 2, 3):
                if 0 <= i - depth * stage < count:
                    c = chunks[i - depth * stage]
                    run_all(c.copies(stage), "wait_recv")
                    c.add(stage)
                    if stage < 3:
                        run_all(c.copies(stage + 1), "start")
            if total is not None and i < 4:
                run_all(total.copies(i), "wait_recv")
                total.add(i)
                if i < 3:
                    run_all(total.copies(i + 1), "start")

        def end():
            for c in chunks:
                for stage in range(4):
                    run_all(c.copies(stage), "wait_send")
            if total is not None:
                for stage in range(4):
                    run_all(total.copies(stage), "wait_send")

        last = max(count + 3 * depth, 4 if self.has_total else 0)
        return [begin] + [functools.partial(step, i) for i in range(last)] + [end]


def plan_kernel(plan, *refs):
    n_in, n_out = len(plan.in_specs), len(plan.out_specs)
    for step in plan.steps(refs[:n_in], refs[n_in : n_in + n_out], refs[n_in + n_out :]):
        step()


def run_plan(plan, collective_id, name):
    outs = pl.pallas_call(
        functools.partial(plan_kernel, plan),
        out_shape=plan.out_shape,
        in_specs=plan.in_specs,
        out_specs=plan.out_specs,
        scratch_shapes=plan.scratch,
        compiler_params=pltpu.CompilerParams(
            collective_id=collective_id, has_side_effects=True, vmem_limit_bytes=VMEM_LIMIT
        ),
        name=name,
    )(*plan.args)
    return plan.results(outs)


def exchange_kernel(dims, n_tensor, n, *refs):
    ins, outs = refs[:n], refs[n : 2 * n]
    send, recv, local = refs[2 * n :]
    place = Place(dims, n_tensor)

    def copies(i):
        for step in range(1, n_tensor):
            device, _ = place.peer(3, step)
            sems = (send.at[i, step - 1], recv.at[i, step - 1])
            yield remote(ins[i], outs[i].at[n_tensor - step], *sems, device)

    own = [pltpu.make_async_copy(ins[i], outs[i].at[0], local.at[i]) for i in range(n)]
    for copy in own:
        copy.start()
    place.barrier((3,))
    for i in range(n):
        for copy in copies(i):
            copy.start()
    for i in range(n):
        own[i].wait()
        for copy in copies(i):
            copy.wait()


def exchange_rows(arrays, dims, n_tensor, collective_id):
    n = len(arrays)
    outs = pl.pallas_call(
        functools.partial(exchange_kernel, dims, n_tensor, n),
        out_shape=[jax.ShapeDtypeStruct((n_tensor,) + a.shape, a.dtype) for a in arrays],
        in_specs=[VMEM] * n,
        out_specs=[ANY] * n,
        scratch_shapes=[
            pltpu.SemaphoreType.DMA((n, n_tensor - 1)),
            pltpu.SemaphoreType.DMA((n, n_tensor - 1)),
            pltpu.SemaphoreType.DMA((n,)),
        ],
        compiler_params=pltpu.CompilerParams(collective_id=collective_id, has_side_effects=True),
        name="exchange_rows",
    )(*arrays)
    return [o.reshape(-1, o.shape[-1]) for o in outs]


def return_kernel(dims, n_tensor, n, *refs):
    ins, outs, bufs = refs[:n], refs[n : 2 * n], refs[2 * n : 3 * n]
    send, recv = refs[3 * n :]
    place = Place(dims, n_tensor)
    rows = outs[0].shape[0]

    def copies(i):
        for step in range(1, n_tensor):
            device, _ = place.peer(3, step)
            sems = (send.at[i, step - 1], recv.at[i, step - 1])
            yield remote(ins[i].at[pl.ds(step * rows, rows), :], bufs[i].at[step - 1], *sems, device)

    place.barrier((3,))
    for i in range(n):
        for copy in copies(i):
            copy.start()
    for i in range(n):
        for copy in copies(i):
            copy.wait()
        for first in range(0, rows, 64):
            total = ins[i][first : first + 64, :].astype(jnp.float32)
            for step in range(1, n_tensor):
                total = total + bufs[i][step - 1, first : first + 64, :].astype(jnp.float32)
            outs[i][first : first + 64, :] = total.astype(outs[i].dtype)


def return_rows(arrays, dims, n_tensor, collective_id):
    n = len(arrays)
    rows, width = arrays[0].shape[0] // n_tensor, arrays[0].shape[1]
    return pl.pallas_call(
        functools.partial(return_kernel, dims, n_tensor, n),
        out_shape=[jax.ShapeDtypeStruct((rows, width), a.dtype) for a in arrays],
        in_specs=[VMEM] * n,
        out_specs=[VMEM] * n,
        scratch_shapes=[pltpu.VMEM((n_tensor - 1, rows, width), a.dtype) for a in arrays]
        + [pltpu.SemaphoreType.DMA((n, n_tensor - 1)), pltpu.SemaphoreType.DMA((n, n_tensor - 1))],
        compiler_params=pltpu.CompilerParams(collective_id=collective_id, has_side_effects=True),
        name="return_rows",
    )(*arrays)


def norm_forward(stream, gain_row, shift_row):
    centered = stream - jnp.mean(stream, axis=-1, keepdims=True)
    inv_std = lax.rsqrt(jnp.mean(centered * centered, axis=-1, keepdims=True) + EPSILON)
    normed = centered * inv_std
    return (normed * gain_row + shift_row, normed, inv_std)


def norm_backward(grad_result, normed, inv_std, gain_row):
    grad_normed = grad_result * gain_row
    return inv_std * (
        grad_normed
        - jnp.mean(grad_normed, axis=-1, keepdims=True)
        - normed * jnp.mean(grad_normed * normed, axis=-1, keepdims=True)
    )


def low(value):
    return value.astype(jnp.bfloat16)


def ffn_forward(entered, weight_in, weight_out_t):
    before = dot_nn(entered, weight_in)
    active = low(jax.nn.silu(before))
    return dot_nt(active, weight_out_t), (before, active)


def ffn_backward(entered, saved, grad_low, weight_in, weight_out_t):
    before, active = saved
    sigma = jax.nn.sigmoid(before)
    grad_active = dot_nn(grad_low, weight_out_t)
    grad_before = low(grad_active * sigma * (1.0 + before * (1.0 - sigma)))
    grad_in = low(dot_tn(entered, grad_before))
    grad_out_t = low(dot_tn(grad_low, active))
    return dot_nt(grad_before, weight_in), grad_in, grad_out_t


def taps_forward(signal, before, conv_taps):
    rows = signal.shape[0]
    padded = jnp.concatenate([before, signal], axis=0)
    skip = before.shape[0] - (KERNEL - 1)
    result = jnp.zeros_like(signal)
    for tap in range(KERNEL):
        result = result + conv_taps[tap] * padded[skip + tap : skip + tap + rows]
    return result


def taps_backward(grad, after, signal, before, conv_taps):
    rows = signal.shape[0]
    padded_signal = jnp.concatenate([before, signal], axis=0)
    padded_grad = jnp.concatenate([grad, after], axis=0)
    skip = before.shape[0] - (KERNEL - 1)
    grad_signal = jnp.zeros_like(signal)
    taps = []
    for tap in range(KERNEL):
        back = KERNEL - 1 - tap
        grad_signal = grad_signal + conv_taps[tap] * padded_grad[back : back + rows]
        taps.append(jnp.sum(grad * padded_signal[skip + tap : skip + tap + rows], axis=0))
    return grad_signal, jnp.stack(taps)


HALO = 32


def on_device(
    dims,
    n_tensor,
    stream_in,
    grad_out,
    clip_lengths,
    first_up,
    first_down,
    attn_proj,
    attn_out,
    rel_table,
    glu_weight,
    conv_taps,
    conv_out,
    second_up,
    second_down,
    norm_gains,
    norm_shifts,
):
    rank = lax.axis_index("tensor")
    rows, width = stream_in.shape
    keys = rows * n_tensor
    early = [first_up[None], first_down.T[None], attn_proj, attn_out.T[None]]
    late = [glu_weight, conv_out.T[None], second_up[None], second_down.T[None]]
    gathered = run_plan(GatherPlan(early, dims, n_tensor), 0, "gather_weights")
    (up_one,), (down_one,), proj, (out_attn,) = gathered

    def enter(stream, row):
        result, normed, inv_std = norm_forward(stream, norm_gains[row], norm_shifts[row])
        return low(result), (normed, inv_std)

    def norm_back(grad_result, saved, row):
        normed, inv_std = saved
        grad_input = norm_backward(grad_result, normed, inv_std, norm_gains[row])
        return grad_input, jnp.sum(grad_result * normed, axis=0), jnp.sum(grad_result, axis=0)

    def shift_rank(value, step):
        pairs = [(i, i + step) for i in range(n_tensor) if 0 <= i + step < n_tensor]
        return lax.ppermute(value, "tensor", pairs)

    stream = stream_in.astype(jnp.float32)
    squares = []

    entered_a, norm_a = enter(stream, 0)
    branch, ffn_a = ffn_forward(entered_a, up_one, down_one)
    squares.append(jnp.sum(branch * branch))
    stream = stream + 0.5 * branch

    entered_b, norm_b = enter(stream, 1)
    query, own_keys, own_vals = (low(dot_nn(entered_b, proj[i])) for i in range(3))
    key_rows, val_rows = exchange_rows([own_keys, own_vals], dims, n_tensor, 2)
    place = lax.rem(jnp.arange(keys, dtype=jnp.int32) + rank * rows, keys)
    mask = jnp.where(place < clip_lengths[0], 0.0, MASKED).astype(jnp.float32)[None]
    table = span_table(rel_table)
    attended, log_totals, gathered = attn_fwd(
        query, key_rows, val_rows, table, mask, GatherPlan(late, dims, n_tensor, *HOST_G), 4
    )
    glu, (out_conv,), (up_two,), (down_two,) = gathered
    branch = dot_nt(attended, out_attn)
    squares.append(jnp.sum(branch * branch))
    stream = stream + branch

    entered_c, norm_c = enter(stream, 2)
    glu_first = dot_nn(entered_c, glu[0])
    glu_second = dot_nn(entered_c, glu[1])
    sig_second = jax.nn.sigmoid(glu_second)
    gated = glu_first * sig_second
    gated_before = shift_rank(gated[rows - HALO :], 1)
    mixed = taps_forward(gated, gated_before, conv_taps)
    shaped, normed_mid, scale_mid = norm_forward(mixed, norm_gains[3], norm_shifts[3])
    conv_act = low(jax.nn.silu(shaped))
    branch = dot_nt(conv_act, out_conv)
    squares.append(jnp.sum(branch * branch))
    stream = stream + branch

    entered_d, norm_d = enter(stream, 4)
    branch, ffn_d = ffn_forward(entered_d, up_two, down_two)
    squares.append(jnp.sum(branch * branch))
    stream = stream + 0.5 * branch
    squares.append(jnp.sum(stream * stream))
    result, normed_e, scale_e = norm_forward(stream, norm_gains[5], norm_shifts[5])
    output = low(result)

    grad_stream, gain_e, shift_e = norm_back(grad_out.astype(jnp.float32), (normed_e, scale_e), 5)
    grad_low = low(0.5 * grad_stream)
    grad_entered, grad_up_two, grad_down_two = ffn_backward(entered_d, ffn_d, grad_low, up_two, down_two)
    grad_extra, gain_d, shift_d = norm_back(grad_entered, norm_d, 4)
    grad_stream = grad_stream + grad_extra

    grad_low = low(grad_stream)
    grad_conv_out = low(dot_tn(grad_low, conv_act))
    sigma = jax.nn.sigmoid(shaped)
    grad_shaped = dot_nn(grad_low, out_conv) * sigma * (1.0 + shaped * (1.0 - sigma))
    grad_mixed, gain_mid, shift_mid = norm_back(grad_shaped, (normed_mid, scale_mid), 3)
    grad_after = shift_rank(grad_mixed[:HALO], -1)
    grad_gated, taps_grad = taps_backward(grad_mixed, grad_after, gated, gated_before, conv_taps)
    grad_first = low(grad_gated * sig_second)
    grad_second = low(grad_gated * glu_first * sig_second * (1.0 - sig_second))
    grad_glu = [low(dot_tn(entered_c, g)) for g in (grad_first, grad_second)]
    grad_entered = dot_nt(grad_first, glu[0]) + dot_nt(grad_second, glu[1])
    grad_extra, gain_c, shift_c = norm_back(grad_entered, norm_c, 2)
    grad_stream = grad_stream + grad_extra

    grad_low = low(grad_stream)
    grad_attn_out = low(dot_tn(grad_low, attended))
    grad_attended = low(dot_nn(grad_low, out_attn))
    grads = [g[None] for g in (grad_down_two, grad_up_two, grad_conv_out, *grad_glu)]
    grad_query, grad_keys, grad_vals, grad_span, summed = attn_bwd(
        query, key_rows, val_rows, grad_attended, attended, log_totals, table, mask,
        ScatterPlan(grads, None, dims, n_tensor, *HOST_S), 5,
    )
    s_down_two, s_up_two, s_conv, s_glu0, s_glu1 = (s[0] for s in summed)
    grad_keys, grad_vals = return_rows([grad_keys, grad_vals], dims, n_tensor, 3)
    grad_parts = (grad_query, grad_keys, grad_vals)
    grad_proj = [low(dot_tn(entered_b, g)) for g in grad_parts]
    grad_entered = sum(dot_nt(g, proj[i]) for i, g in enumerate(grad_parts))
    grad_extra, gain_b, shift_b = norm_back(grad_entered, norm_b, 1)
    grad_stream = grad_stream + grad_extra

    grad_low = low(0.5 * grad_stream)
    grad_entered, grad_up_one, grad_down_one = ffn_backward(entered_a, ffn_a, grad_low, up_one, down_one)
    grad_extra, gain_a, shift_a = norm_back(grad_entered, norm_a, 0)
    grad_stream = grad_stream + grad_extra

    span_grad = fold_table(grad_span)
    span_rows = -(-span_grad.size // width)
    table_rows = jnp.pad(span_grad.reshape(-1), (0, span_rows * width - span_grad.size)).reshape(span_rows, width)
    square_row = jnp.pad(jnp.stack(squares), (0, width - len(squares)))[None]
    parts = [
        jnp.stack([gain_a, gain_b, gain_c, gain_mid, gain_d, gain_e]),
        jnp.stack([shift_a, shift_b, shift_c, shift_mid, shift_d, shift_e]),
        taps_grad,
        table_rows,
        square_row,
    ]
    vec = jnp.concatenate(parts, axis=0)
    vec = jnp.pad(vec, ((0, -vec.shape[0] % 8), (0, 0)))
    grads = [g[None] for g in (grad_attn_out, *grad_proj, grad_down_one, grad_up_one)]
    *summed, vec = run_plan(ScatterPlan(grads, vec, dims, n_tensor), 1, "scatter_grads")
    s_attn, s_q, s_k, s_v, s_down_one, s_up_one = (s[0] for s in summed)
    at = 0
    pieces = []
    for part in parts:
        pieces.append(vec[at : at + part.shape[0]])
        at += part.shape[0]
    gains_sum, shifts_sum, taps_sum, table_sum, square_sum = pieces
    table_sum = table_sum.reshape(-1)[: span_grad.size].reshape(span_grad.shape)
    count_all = float(lax.axis_size("dp") * keys * width)
    rms_values = jnp.sqrt(square_sum[0, : len(squares)] / count_all)
    return (
        output,
        grad_stream,
        s_up_one,
        s_down_one.T,
        jnp.stack([s_q, s_k, s_v]),
        s_attn.T,
        table_sum,
        jnp.stack([s_glu0, s_glu1]),
        taps_sum,
        s_conv.T,
        s_up_two,
        s_down_two.T,
        gains_sum,
        shifts_sum,
        rms_values,
    )


def solution(mesh):
    n_dp, n_tensor = mesh.shape["dp"], mesh.shape["tensor"]
    dims = FACTORS.get(n_dp, (n_dp, 1, 1))
    return jax.shard_map(
        functools.partial(on_device, dims, n_tensor),
        mesh=mesh,
        in_specs=(
            P(("dp", "tensor"), None),
            P(("dp", "tensor"), None),
            P("dp"),
            P("dp", "tensor"),
            P("tensor", "dp"),
            P(None, "dp", "tensor"),
            P("tensor", "dp"),
            P(),
            P(None, "dp", "tensor"),
            P(),
            P("tensor", "dp"),
            P("dp", "tensor"),
            P("tensor", "dp"),
            P(),
            P(),
        ),
        out_specs=(
            P(("dp", "tensor"), None),
            P(("dp", "tensor"), None),
            P("dp", "tensor"),
            P("tensor", "dp"),
            P(None, "dp", "tensor"),
            P("tensor", "dp"),
            P(),
            P(None, "dp", "tensor"),
            P(),
            P("tensor", "dp"),
            P("dp", "tensor"),
            P("tensor", "dp"),
            P(),
            P(),
            P(),
        ),
        check_vma=False,
    )
```

```python
import functools

import jax
import jax.numpy as jnp
from jax import lax
from jax.experimental import pallas as pl
from jax.experimental.pallas import tpu as pltpu
from jax.sharding import PartitionSpec as P

HEAD = 64
KERNEL = 31
LEFT = 64
RIGHT = 8
EPSILON = 1e-05
MASKED = -1e30
VMEM_LIMIT = 66_000_000
HOST_G = (512, 6, 5)
HOST_S = (256, 8, 4)
BLK = 128
SPAN = 512
NT = (((1,), (1,)), ((), ()))
TN = (((0,), (0,)), ((), ()))


def dot_nt(a, b):
    return lax.dot_general(a, b, NT, preferred_element_type=jnp.float32)


def dot_tn(a, b):
    return lax.dot_general(a, b, TN, preferred_element_type=jnp.float32)


def dot_nn(a, b):
    return jnp.dot(a, b, preferred_element_type=jnp.float32)


def rel_blocks(tin, b, own_blocks, key_blocks, rank):
    t_left, t_right = tin[:, 0:1], tin[:, SPAN - 1 : SPAN]
    band = pltpu.roll(tin, SPAN - BLK, 1, stride=1, stride_axis=0)
    out = []
    for kb in range(key_blocks):
        wraps = rank * own_blocks + kb >= key_blocks
        if kb in (b - 1, b) or (kb == b + 1 and kb < own_blocks):
            out.append(band[:, (kb - b + 1) * BLK : (kb - b + 2) * BLK])
        elif kb == b + 1:
            out.append(jnp.where(wraps, t_left, band[:, 2 * BLK : 3 * BLK]))
        elif b == 0 and kb == key_blocks - 1:
            out.append(jnp.where(wraps, band[:, :BLK], t_right))
        elif kb < b - 1:
            out.append(t_left)
        elif kb < own_blocks:
            out.append(t_right)
        else:
            out.append(jnp.where(wraps, t_left, t_right))
    return out


def halves(x):
    low = lax.broadcasted_iota(jnp.int32, x.shape, 1) < HEAD
    zero = jnp.zeros_like(x)
    return jnp.where(low, x, zero), jnp.where(low, zero, x)


def flip_rows(x):
    tiles = []
    back = 7 - lax.broadcasted_iota(jnp.int32, (8, BLK), 0)
    for first in range(x.shape[0] - 8, -1, -8):
        cols = [
            jnp.take_along_axis(x[first : first + 8, c : c + BLK], back, axis=0, mode="promise_in_bounds")
            for c in range(0, x.shape[1], BLK)
        ]
        tiles.append(jnp.concatenate(cols, axis=1) if len(cols) > 1 else cols[0])
    return jnp.concatenate(tiles, axis=0)


def split_refs(refs, sizes):
    out, at = [], 0
    for size in sizes:
        out.append(refs[at : at + size])
        at += size
    return out


def ticker(plan, ins, outs, scratch, ticks):
    if plan is None:
        return lambda block, blocks: None
    steps = plan.steps(ins, outs, scratch)

    def tick(block, blocks):
        for number, step in enumerate(steps):
            at = min(number * ticks // (len(steps) - 1), ticks - 1) if number < len(steps) - 1 else ticks
            if at < ticks and at % blocks == block:
                pl.when(pl.program_id(0) == at // blocks)(step)
            if at == ticks and block == blocks:
                pl.when(pl.program_id(0) == ticks // blocks - 1)(step)

    return tick


def attn_fwd_kernel(plan, *refs):
    n_in, n_out = (len(plan.in_specs), len(plan.out_specs)) if plan else (0, 0)
    own, plan_in, (o_ref, lse_ref), plan_out, plan_scratch = split_refs(refs, (5, n_in, 2, n_out, len(refs)))
    q_ref, k_ref, v_ref, tab_ref, mask_ref = own
    rank = lax.axis_index("tensor")
    rows, keys = q_ref.shape[0], k_ref.shape[0]
    own_blocks, key_blocks = rows // BLK, keys // BLK
    low = lax.broadcasted_iota(jnp.int32, (BLK, 2 * HEAD), 1) < HEAD
    tick = ticker(plan, plan_in, plan_out, plan_scratch, own_blocks * pl.num_programs(0))
    for b in range(own_blocks):
        tick(b, own_blocks)
        q_blk = q_ref[b * BLK : (b + 1) * BLK, :] * jnp.asarray(HEAD**-0.5, jnp.bfloat16)
        results = []
        for hh, q_one in enumerate(halves(q_blk)):
            tin = dot_nt(q_one, tab_ref[...])
            rel = rel_blocks(tin, b, own_blocks, key_blocks, rank)
            raw = dot_nt(q_one, k_ref[...])
            s = [
                raw[:, kb * BLK : (kb + 1) * BLK] + rel[kb] + mask_ref[:, kb * BLK : (kb + 1) * BLK]
                for kb in range(key_blocks)
            ]
            s = jnp.concatenate(s, axis=1)
            peak = jnp.max(s, axis=-1, keepdims=True)
            e = jnp.exp(s - peak)
            total = jnp.sum(e, axis=-1, keepdims=True)
            o = dot_nn(e.astype(jnp.bfloat16), v_ref[...])
            results.append(o / total)
            first = (hh * own_blocks + b) * BLK
            lse_ref[0, first : first + BLK, :] = peak + jnp.log(total)
        o_ref[b * BLK : (b + 1) * BLK, :] = jnp.where(low, results[0], results[1]).astype(jnp.bfloat16)
    tick(own_blocks, own_blocks)


def attn_fwd(q, k, v, tab2, mask, plan=None, collective_id=None):
    rows, width = q.shape
    keys = k.shape[0]
    pairs = width // (2 * HEAD)
    col = lambda n: pl.BlockSpec((n, 2 * HEAD), lambda p: (0, p))
    out_specs = [col(rows), pl.BlockSpec((1, 2 * rows, 1), lambda p: (p, 0, 0))]
    out_shape = [
        jax.ShapeDtypeStruct((rows, width), jnp.bfloat16),
        jax.ShapeDtypeStruct((pairs, 2 * rows, 1), jnp.float32),
    ]
    outs = pl.pallas_call(
        functools.partial(attn_fwd_kernel, plan),
        grid=(pairs,),
        in_specs=[
            col(rows),
            col(keys),
            col(keys),
            pl.BlockSpec((SPAN, 2 * HEAD), lambda p: (0, 0)),
            pl.BlockSpec((1, keys), lambda p: (0, 0)),
        ]
        + (plan.in_specs if plan else []),
        out_specs=out_specs + (plan.out_specs if plan else []),
        out_shape=out_shape + (plan.out_shape if plan else []),
        scratch_shapes=plan.scratch if plan else [],
        compiler_params=pltpu.CompilerParams(
            collective_id=collective_id, has_side_effects=plan is not None, vmem_limit_bytes=VMEM_LIMIT
        ),
        name="attn_fwd",
    )(q, k, v, tab2, mask, *(plan.args if plan else []))
    return outs[0], outs[1], plan.results(outs[2:]) if plan else []


def attn_bwd_kernel(plan, *refs):
    n_in, n_out = (len(plan.in_specs), len(plan.out_specs)) if plan else (0, 0)
    own, plan_in, own_out, plan_out, own_scratch, plan_scratch = split_refs(refs, (8, n_in, 4, n_out, 4, len(refs)))
    q_ref, k_ref, v_ref, do_ref, o_ref, lse_ref, tab_ref, mask_ref = own
    dq_ref, dk_ref, dv_ref, dtab_ref = own_out
    p_sc, ds_sc, q_sc, do_sc = own_scratch
    rank = lax.axis_index("tensor")
    rows, keys = q_ref.shape[0], k_ref.shape[0]
    own_blocks, key_blocks = rows // BLK, keys // BLK
    low = lax.broadcasted_iota(jnp.int32, (BLK, 2 * HEAD), 1) < HEAD
    lane = lax.broadcasted_iota(jnp.int32, (BLK, BLK), 1)
    scale = jnp.asarray(HEAD**-0.5, jnp.bfloat16)

    @pl.when(pl.program_id(0) == 0)
    def _():
        dtab_ref[...] = jnp.zeros_like(dtab_ref)

    tick = ticker(plan, plan_in, plan_out, plan_scratch, own_blocks * pl.num_programs(0))
    for b in range(own_blocks):
        tick(b, own_blocks)
        at = slice(b * BLK, (b + 1) * BLK)
        q_blk = q_ref[at, :] * scale
        do_blk = do_ref[at, :]
        prod = do_blk.astype(jnp.float32) * o_ref[at, :].astype(jnp.float32)
        q_back = halves(flip_rows(q_blk.astype(jnp.float32)).astype(jnp.bfloat16))
        results = []
        for hh, (q_one, do_one, pr_one) in enumerate(zip(halves(q_blk), halves(do_blk), halves(prod))):
            first = (hh * own_blocks + b) * BLK
            here = slice(first, first + BLK)
            inner = jnp.sum(pr_one, axis=-1, keepdims=True)
            lse = lse_ref[0, here, :]
            tin = dot_nt(q_one, tab_ref[...])
            rel = rel_blocks(tin - lse, b, own_blocks, key_blocks, rank)
            raw = dot_nt(q_one, k_ref[...])
            dp = dot_nt(do_one, v_ref[...])
            left = jnp.zeros((BLK, BLK), jnp.float32)
            right = jnp.zeros((BLK, BLK), jnp.float32)
            window = [None, None, None]
            for kb in range(key_blocks):
                ks = slice(kb * BLK, (kb + 1) * BLK)
                p = jnp.exp(raw[:, ks] + rel[kb] + mask_ref[:, ks])
                ds = (p * (dp[:, ks] - inner)).astype(jnp.bfloat16)
                p_sc[here, ks] = p.astype(jnp.bfloat16)
                ds_sc[here, ks] = ds
                ds = ds.astype(jnp.float32)
                wraps = rank * own_blocks + kb >= key_blocks
                zero = jnp.zeros_like(ds)
                if kb in (b - 1, b) or (kb == b + 1 and kb < own_blocks):
                    window[kb - b + 1] = ds
                elif kb == b + 1:
                    window[2] = jnp.where(wraps, zero, ds)
                    left = left + jnp.where(wraps, ds, zero)
                elif b == 0 and kb == key_blocks - 1:
                    window[0] = jnp.where(wraps, ds, zero)
                    right = right + jnp.where(wraps, zero, ds)
                elif kb < b - 1:
                    left = left + ds
                elif kb < own_blocks:
                    right = right + ds
                else:
                    left = left + jnp.where(wraps, ds, zero)
                    right = right + jnp.where(wraps, zero, ds)
            none = jnp.zeros((BLK, BLK), jnp.float32)
            window = jnp.concatenate([none if w is None else flip_rows(w) for w in window] + [none], axis=1)
            back = pltpu.roll(window, 1, 1, stride=1, stride_axis=0)
            s_left = flip_rows(jnp.broadcast_to(jnp.sum(left, axis=-1, keepdims=True), (BLK, BLK)))
            s_right = flip_rows(jnp.broadcast_to(jnp.sum(right, axis=-1, keepdims=True), (BLK, BLK)))
            u = jnp.concatenate(
                [
                    back[:, :BLK] + jnp.where(lane == 0, s_left, 0.0),
                    back[:, BLK : 3 * BLK],
                    back[:, 3 * BLK :] + jnp.where(lane == BLK - 1, s_right, 0.0),
                ],
                axis=1,
            ).astype(jnp.bfloat16)
            q_sc[here, :] = q_one
            do_sc[here, :] = do_one
            dtab_ref[...] += dot_tn(u, q_back[hh])
            results.append(dot_nn(ds_sc[here, :], k_ref[...]) + flip_rows(dot_nn(u, tab_ref[...])))
        dq_ref[at, :] = (jnp.where(low, results[0], results[1]) * HEAD**-0.5).astype(jnp.bfloat16)
    dk_ref[...] = dot_tn(ds_sc[...], q_sc[...]).astype(dk_ref.dtype)
    dv_ref[...] = dot_tn(p_sc[...], do_sc[...]).astype(dv_ref.dtype)
    tick(own_blocks, own_blocks)


def attn_bwd(q, k, v, do, o, lse, tab2, mask, plan=None, collective_id=None):
    rows, width = q.shape
    keys = k.shape[0]
    pairs = width // (2 * HEAD)
    col = lambda n: pl.BlockSpec((n, 2 * HEAD), lambda p: (0, p))
    table = pl.BlockSpec((SPAN, 2 * HEAD), lambda p: (0, 0))
    out_shape = [
        jax.ShapeDtypeStruct((rows, width), jnp.bfloat16),
        jax.ShapeDtypeStruct((keys, width), jnp.bfloat16),
        jax.ShapeDtypeStruct((keys, width), jnp.bfloat16),
        jax.ShapeDtypeStruct((SPAN, 2 * HEAD), jnp.float32),
    ]
    outs = pl.pallas_call(
        functools.partial(attn_bwd_kernel, plan),
        grid=(pairs,),
        in_specs=[
            col(rows),
            col(keys),
            col(keys),
            col(rows),
            col(rows),
            pl.BlockSpec((1, 2 * rows, 1), lambda p: (p, 0, 0)),
            table,
            pl.BlockSpec((1, keys), lambda p: (0, 0)),
        ]
        + (plan.in_specs if plan else []),
        out_specs=[col(rows), col(keys), col(keys), table] + (plan.out_specs if plan else []),
        out_shape=out_shape + (plan.out_shape if plan else []),
        scratch_shapes=[
            pltpu.VMEM((2 * rows, keys), jnp.bfloat16),
            pltpu.VMEM((2 * rows, keys), jnp.bfloat16),
            pltpu.VMEM((2 * rows, 2 * HEAD), jnp.bfloat16),
            pltpu.VMEM((2 * rows, 2 * HEAD), jnp.bfloat16),
        ]
        + (plan.scratch if plan else []),
        compiler_params=pltpu.CompilerParams(
            collective_id=collective_id, has_side_effects=plan is not None, vmem_limit_bytes=VMEM_LIMIT
        ),
        name="attn_bwd",
    )(q, k, v, do, o, lse, tab2, mask, *(plan.args if plan else []))
    return (*outs[:4], plan.results(outs[4:]) if plan else [])


def span_table(rel_table):
    rows = jnp.clip(jnp.arange(SPAN) - SPAN // 2, -LEFT, RIGHT) + LEFT
    table = jnp.take(rel_table, rows, axis=0)
    return jnp.concatenate([table, table], axis=1)


def fold_table(dtab):
    one = dtab[:, :HEAD] + dtab[:, HEAD:]
    rows = jnp.clip(jnp.arange(SPAN) - SPAN // 2, -LEFT, RIGHT) + LEFT
    pick = (rows[None, :] == jnp.arange(LEFT + RIGHT + 1)[:, None]).astype(jnp.float32)
    return jnp.dot(pick, one, precision=lax.Precision.HIGHEST)


MESH = pl.DeviceIdType.MESH
ANY = pl.BlockSpec(memory_space=pl.ANY)
VMEM = pl.BlockSpec(memory_space=pltpu.VMEM)
FACTORS = {16: (4, 2, 2), 32: (4, 2, 4)}


class Place:
    def __init__(self, dims, n_tensor):
        self.dims, self.n_tensor = dims, n_tensor
        n_a, n_b, n_c = dims
        d = lax.axis_index("dp")
        self.t = lax.axis_index("tensor")
        self.at = (lax.div(d, n_b * n_c), lax.rem(lax.div(d, n_c), n_b), lax.rem(d, n_c))

    def peer(self, axis, step):
        at, t = list(self.at), self.t
        if axis == 3:
            t = lax.rem(t + step, self.n_tensor)
            index = t
        else:
            at[axis] = index = lax.rem(at[axis] + step, self.dims[axis])
        n_a, n_b, n_c = self.dims
        return ((at[0] * n_b + at[1]) * n_c + at[2], t), index

    def size(self, axis):
        return self.n_tensor if axis == 3 else self.dims[axis]

    def barrier(self, axes=(0, 1, 2, 3)):
        sem = pltpu.get_barrier_semaphore()
        count = 0
        for axis in axes:
            for step in range(1, self.size(axis)):
                pl.semaphore_signal(sem, inc=1, device_id=self.peer(axis, step)[0], device_id_type=MESH)
                count += 1
        pl.semaphore_wait(sem, count)


def remote(src, dst, send_sem, recv_sem, device):
    return pltpu.make_async_remote_copy(
        src_ref=src, dst_ref=dst, send_sem=send_sem, recv_sem=recv_sem, device_id=device, device_id_type=MESH
    )


class Piece:
    def __init__(self, source, lead, first, width):
        self.source, self.lead, self.first, self.width = source, lead, first, width


def pieces_of(parts, chunk):
    return [
        Piece(source, lead, first, min(chunk, cols - first))
        for source, (n, cols) in enumerate(parts)
        for lead in range(n)
        for first in range(0, cols, chunk)
    ]


def run_all(copies, action):
    for copy in copies:
        getattr(copy, action)()


class Gather:
    NORMAL = ((0, 1, 2), (0, 2, 1))
    EARLY = ((2, 1, 0), (1, 2, 0))

    def __init__(self, place, piece, orders, shard, whole, send, recv, local):
        self.place, self.piece, self.orders = place, piece, orders
        self.shard, self.whole = shard, whole
        self.send, self.recv, self.local = send, recv, local
        self.half = shard.shape[1] // 2

    @staticmethod
    def slots(dims, n_tensor):
        return 2 * (sum(d - 1 for d in dims) + 2 * (n_tensor - 1))

    def slot(self, color, stage, step):
        place, order = self.place, self.orders[color]
        sizes = [place.dims[x] - 1 for x in order] + [place.n_tensor - 1] * 2
        return color * sum(sizes) + sum(sizes[:stage]) + step - 1

    def columns(self, t):
        piece = self.piece
        return pl.ds(pl.multiple_of(t * self.shard.shape[2] + piece.first, 128), piece.width)

    def region(self, color, index, t):
        rows = pl.ds(color * self.half, self.half)
        return self.whole.at[(self.piece.lead,) + tuple(index) + (rows, self.columns(t))]

    def source(self, rows):
        piece = self.piece
        return self.shard.at[piece.lead, rows, pl.ds(piece.first, piece.width)]

    def index(self, color, stage, moved=None):
        order, out = self.orders[color], list(self.place.at)
        for axis in order[:stage]:
            out[axis] = slice(None)
        if moved is not None:
            out[order[stage]] = moved
        return out

    def own(self):
        there = self.whole.at[(self.piece.lead,) + self.place.at + (slice(None), self.columns(self.place.t))]
        return pltpu.make_async_copy(self.source(slice(None)), there, self.local)

    def copies(self, stage, arriving=False):
        place, t = self.place, self.place.t
        for color, order in enumerate(self.orders):
            in_one = place.dims[order[2]] > 2
            if stage == 3 and in_one:
                continue
            axis = order[stage] if stage < 3 else 3
            for step in range(1, place.size(axis)):
                device, _ = place.peer(axis, step)
                _, origin = place.peer(axis, place.size(axis) - step)
                slot = self.slot(color, stage, step)
                if stage < 3:
                    index, there, then = self.index(color, stage), self.index(color, stage, origin), t
                else:
                    if in_one:
                        index = self.index(color, 3)
                    elif stage == 3:
                        index = self.index(color, 2)
                    else:
                        index = self.index(color, 2, place.peer(order[2], 1)[1])
                    there, then = index, origin
                mine, theirs = self.region(color, index, t), self.region(color, there, then)
                origin_ref = self.source(pl.ds(color * self.half, self.half)) if stage == 0 else mine
                sems = (self.send.at[slot], self.recv.at[slot], device)
                yield remote(theirs, theirs, *sems) if arriving else remote(origin_ref, mine, *sems)

    def start(self, stage):
        run_all(self.copies(stage), "start")

    def arrived(self, stage):
        run_all(self.copies(stage, arriving=True), "wait_recv")

    def sent(self, stage):
        run_all(self.copies(stage), "wait_send")


class GatherPlan:
    def __init__(self, shards, dims, n_tensor, chunk=1024, every=6, depth=3):
        self.dims, self.n_tensor, self.depth = dims, n_tensor, depth
        self.args = list(shards)
        self.pieces = pieces_of([(s.shape[0], s.shape[2]) for s in shards], chunk)
        self.orders = [Gather.EARLY if i % every == 0 else Gather.NORMAL for i in range(len(self.pieces))]
        count, slots = len(self.pieces), Gather.slots(dims, n_tensor)
        self.in_specs = [VMEM] * len(shards)
        self.out_specs = [ANY] * len(shards)
        self.out_shape = [
            jax.ShapeDtypeStruct((s.shape[0], *dims, s.shape[1], n_tensor * s.shape[2]), s.dtype) for s in shards
        ]
        self.scratch = [
            pltpu.SemaphoreType.DMA((count, slots)),
            pltpu.SemaphoreType.DMA((count, slots)),
            pltpu.SemaphoreType.DMA((count,)),
        ]

    def results(self, outs):
        return [o.reshape(o.shape[0], -1, o.shape[-1]) for o in outs]

    def steps(self, shards, wholes, scratch):
        send, recv, local = scratch
        place = Place(self.dims, self.n_tensor)
        gathers = [
            Gather(place, p, orders, shards[p.source], wholes[p.source], send.at[i], recv.at[i], local.at[i])
            for i, (p, orders) in enumerate(zip(self.pieces, self.orders))
        ]
        count, depth = len(gathers), self.depth

        def begin():
            for g in gathers:
                g.own().start()
            place.barrier()
            for g in gathers:
                g.start(0)
            for g in gathers:
                g.own().wait()

        def step(i):
            if i < count:
                gathers[i].arrived(0)
                gathers[i].start(1)
            at = i - depth
            if 0 <= at < count:
                gathers[at].arrived(1)
                gathers[at].start(2)
                gathers[at].start(3)
            at = i - 2 * depth
            if 0 <= at < count:
                gathers[at].arrived(2)
                gathers[at].start(4)

        def end():
            for g in gathers:
                g.arrived(3)
                g.arrived(4)
                for stage in range(5):
                    g.sent(stage)

        return [begin] + [functools.partial(step, i) for i in range(count + 2 * depth)] + [end]


class Scatter:
    NORMAL = ((2, 1, 0), (1, 2, 0))
    EARLY = ((0, 1, 2), (0, 2, 1))

    def __init__(self, place, piece, orders, left_op, slabs, out, held, near, sent, bufs, sems):
        self.place, self.piece, self.orders = place, piece, orders
        self.left_op, self.slabs, self.out = left_op, slabs, out
        self.held, self.near, self.sent, self.bufs = held, near, sent, bufs
        self.send, self.recv = sems
        self.half = held.shape[3] // 2

    @staticmethod
    def slots(dims, n_tensor):
        return n_tensor - 1 + 2 * sum(d - 1 for d in dims)

    @staticmethod
    def left(order, stage):
        return [x for x in (0, 1, 2) if x not in order[:stage]]

    def product(self, t, target):
        n_a, n_b, n_c = self.place.dims
        rows = self.held.shape[3]
        block = n_b * n_c * rows

        def body(a, _):
            lhs = self.left_op[pl.ds(pl.multiple_of(a * block, block), block), :]
            value = dot_nn(lhs, self.slabs[t]).astype(jnp.bfloat16)
            target[a] = value.reshape(n_b, n_c, rows, value.shape[-1])
            return 0

        lax.fori_loop(0, n_a, body, 0)

    def compute(self):
        for step, copy in enumerate(self.copies(0)):
            self.product(self.place.peer(3, step + 1)[1], self.sent.at[step])
            copy.start()
        self.product(self.place.t, self.held)

    def copies(self, stage):
        place = self.place
        if stage == 0:
            for step in range(1, place.n_tensor):
                sems = (self.send.at[step - 1], self.recv.at[step - 1], place.peer(3, step)[0])
                yield remote(self.sent.at[step - 1], self.near.at[step - 1], *sems)
            return
        base = place.n_tensor - 1
        for color, order in enumerate(self.orders):
            axis = order[stage - 1]
            for step in range(1, place.size(axis)):
                device, there = place.peer(axis, step)
                index = [slice(None)] * 3
                for done in order[: stage - 1]:
                    index[done] = place.at[done]
                index[axis] = there
                slot = base + color * sum(d - 1 for d in place.dims)
                slot += sum(place.size(x) - 1 for x in order[: stage - 1]) + step - 1
                origin = self.held.at[tuple(index) + (pl.ds(color * self.half, self.half),)]
                sems = (self.send.at[slot], self.recv.at[slot], device)
                yield remote(origin, self.bufs[stage - 1][color].at[step - 1], *sems)

    def add_tensor(self):
        n_a, n_b, n_c = self.place.dims

        def body(i, _):
            at = (lax.div(i, n_b * n_c), lax.rem(lax.div(i, n_c), n_b), lax.rem(i, n_c))
            total = self.held[at].astype(jnp.float32)
            for step in range(1, self.place.n_tensor):
                total = total + self.near[(step - 1,) + at].astype(jnp.float32)
            self.held[at] = total.astype(jnp.bfloat16)
            return 0

        lax.fori_loop(0, n_a * n_b * n_c, body, 0)

    def add(self, stage):
        place, piece = self.place, self.piece
        for color, order in enumerate(self.orders):
            rows = slice(color * self.half, (color + 1) * self.half)
            left = self.left(order, stage)
            buf = self.bufs[stage - 1][color]

            def total_at(where):
                at = list(place.at)
                for x, w in zip(left, where):
                    at[x] = w
                at = tuple(at) + (rows,)
                total = self.held[at].astype(jnp.float32)
                for step in range(1, place.size(order[stage - 1])):
                    total = total + buf[(step - 1,) + where].astype(jnp.float32)
                return at, total

            def body(i, _):
                if len(left) == 2:
                    size = place.dims[left[1]]
                    at, total = total_at((lax.div(i, size), lax.rem(i, size)))
                else:
                    at, total = total_at((i,))
                self.held[at] = total.astype(jnp.bfloat16)
                return 0

            if left:
                count = 1
                for x in left:
                    count *= place.dims[x]
                lax.fori_loop(0, count, body, 0)
            else:
                cols = slice(piece.first, piece.first + piece.width)
                self.out[rows, cols] = total_at(())[1]


class Total:
    AXES = (3, 2, 1, 0)

    def __init__(self, place, value, out, boxes, send, recv):
        self.place, self.value, self.out, self.boxes, self.send, self.recv = place, value, out, boxes, send, recv

    @staticmethod
    def slots(dims, n_tensor):
        return sum(dims) + n_tensor - 4

    def copies(self, stage):
        place, axis = self.place, self.AXES[stage]
        base = sum(place.size(x) - 1 for x in self.AXES[:stage])
        for step in range(1, place.size(axis)):
            device, _ = place.peer(axis, step)
            sems = (self.send.at[base + step - 1], self.recv.at[base + step - 1], device)
            yield remote(self.value.at[stage], self.boxes[stage].at[step - 1], *sems)

    def add(self, stage):
        place, axis = self.place, self.AXES[stage]
        size = place.size(axis)
        mine = place.t if axis == 3 else place.at[axis]
        own = self.value[stage]
        if size == 2:
            total = own + self.boxes[stage][0]
        else:
            total = jnp.zeros_like(own)
            for index in range(size):
                step = lax.rem(mine - index + size, size)
                term = self.boxes[stage][jnp.maximum(step - 1, 0)]
                total = total + jnp.where(step == 0, own, term)
        if stage == 3:
            self.out[...] = total
        else:
            self.value[stage + 1] = total


class ScatterPlan:
    def __init__(self, terms, vec, dims, n_tensor, chunk=256, every=8, depth=4):
        self.dims, self.n_tensor, self.has_total, self.depth = dims, n_tensor, vec is not None, depth
        n_a, n_b, n_c = dims
        tokens, width = terms[0][0].shape
        rows = width // (n_a * n_b * n_c)
        parts = [(1, right.shape[1] // n_tensor) for _, right in terms]
        chunk = min(chunk, *(cols for _, cols in parts))
        self.pieces = pieces_of(parts, chunk)
        self.part_cols = [cols for _, cols in parts]
        count, slots = len(self.pieces), Scatter.slots(dims, n_tensor)
        kinds = [0 if i % every else 1 for i in range(count)]
        self.places = [(k, kinds[:i].count(k)) for i, k in enumerate(kinds)]
        lefts = []
        self.left_at = []
        for left, _ in terms:
            known = [i for i, other in enumerate(lefts) if other is left]
            if not known:
                lefts.append(left)
            self.left_at.append(known[0] if known else len(lefts) - 1)
        self.n_left = len(lefts)
        self.args = lefts + [right for _, right in terms]
        self.in_specs = [VMEM] * len(lefts) + [ANY] * len(terms)
        self.out_shape = [jax.ShapeDtypeStruct((rows, cols), jnp.float32) for _, cols in parts]
        self.out_specs = [VMEM] * len(terms)
        bf, half = jnp.bfloat16, rows // 2
        self.scratch = [
            pltpu.VMEM((count, n_a, n_b, n_c, rows, chunk), bf),
            pltpu.VMEM((count, n_tensor - 1, n_a, n_b, n_c, rows, chunk), bf),
            pltpu.VMEM((self.SENDS, n_tensor - 1, n_a, n_b, n_c, rows, chunk), bf),
            pltpu.VMEM((2, n_tensor, tokens, chunk), bf),
            pltpu.VMEM((len(lefts), width, tokens), bf),
            pltpu.SemaphoreType.DMA((count, slots)),
            pltpu.SemaphoreType.DMA((count, slots)),
            pltpu.SemaphoreType.DMA((2, n_tensor)),
        ]
        for kind, orders in enumerate((Scatter.NORMAL, Scatter.EARLY)):
            for stage in (1, 2, 3):
                for order in orders:
                    left = [dims[x] for x in Scatter.left(order, stage)]
                    shape = (max(kinds.count(kind), 1), dims[order[stage - 1]] - 1, *left, half, chunk)
                    self.scratch.append(pltpu.VMEM(shape, bf))
        if self.has_total:
            self.args.append(vec)
            self.in_specs.append(VMEM)
            self.out_shape.append(jax.ShapeDtypeStruct(vec.shape, vec.dtype))
            self.out_specs.append(VMEM)
            self.scratch.append(pltpu.VMEM((4,) + vec.shape, vec.dtype))
            self.scratch += [pltpu.VMEM((k - 1,) + vec.shape, vec.dtype) for k in (n_tensor, n_c, n_b, n_a)]
            self.scratch += [pltpu.SemaphoreType.DMA((Total.slots(dims, n_tensor),))] * 2

    SENDS = 3

    def results(self, outs):
        return list(outs)

    def steps(self, ins, outs, scratch):
        place = Place(self.dims, self.n_tensor)
        held, near, sent, slabs, turned, send, recv, local = scratch[:8]
        chunks = []
        for i, (piece, (kind, at)) in enumerate(zip(self.pieces, self.places)):
            orders = (Scatter.NORMAL, Scatter.EARLY)[kind]
            boxes = scratch[8 + 6 * kind : 14 + 6 * kind]
            bufs = [[boxes[2 * stage + color].at[at] for color in (0, 1)] for stage in range(3)]
            chunks.append(
                Scatter(
                    place, piece, orders, turned.at[self.left_at[piece.source]], slabs.at[i % 2], outs[piece.source],
                    held.at[i], near.at[i], sent.at[i % self.SENDS], bufs, (send.at[i], recv.at[i]),
                )
            )
        count, depth = len(chunks), self.depth
        total = None
        if self.has_total:
            value, *rest = scratch[20:]
            total = Total(place, value, outs[-1], rest[:4], rest[4], rest[5])

        def loads(i):
            piece = self.pieces[i]
            right = ins[self.n_left + piece.source]
            for t in range(self.n_tensor):
                cols = pl.ds(t * self.part_cols[piece.source] + piece.first, piece.width)
                yield pltpu.make_async_copy(right.at[:, cols], slabs.at[i % 2, t], local.at[i % 2, t])

        def turn(number):
            block = 256

            def body(a, _):
                cols = pl.ds(pl.multiple_of(a * block, block), block)
                turned[number, cols, :] = ins[number][:, cols].T
                return 0

            lax.fori_loop(0, turned.shape[1] // block, body, 0)

        firsts = [next(i for i, p in enumerate(self.pieces) if self.left_at[p.source] == n) for n in range(self.n_left)]

        def begin():
            run_all(loads(0), "start")
            if total is not None:
                value[0] = ins[-1][...]
            place.barrier()
            if total is not None:
                run_all(total.copies(0), "start")

        def step(i):
            if i < count:
                run_all(loads(i), "wait")
                if i + 1 < count:
                    run_all(loads(i + 1), "start")
                if i >= self.SENDS:
                    run_all(chunks[i - self.SENDS].copies(0), "wait_send")
                for number, first in enumerate(firsts):
                    if first == i:
                        turn(number)
                chunks[i].compute()
            if 0 <= i - 1 < count:
                c = chunks[i - 1]
                run_all(c.copies(0), "wait_recv")
                c.add_tensor()
                run_all(c.copies(1), "start")
            for stage in (1, 2, 3):
                at = i - 1 - depth * stage
                if 0 <= at < count:
                    run_all(chunks[at].copies(stage), "wait_recv")
                    chunks[at].add(stage)
                    if stage < 3:
                        run_all(chunks[at].copies(stage + 1), "start")
            if total is not None and i < 4:
                run_all(total.copies(i), "wait_recv")
                total.add(i)
                if i < 3:
                    run_all(total.copies(i + 1), "start")

        def end():
            for i, c in enumerate(chunks):
                for stage in range(0 if i >= count - self.SENDS else 1, 4):
                    run_all(c.copies(stage), "wait_send")
            if total is not None:
                for stage in range(4):
                    run_all(total.copies(stage), "wait_send")

        last = max(count + 1 + 3 * depth, 4 if self.has_total else 0)
        return [begin] + [functools.partial(step, i) for i in range(last)] + [end]


def plan_kernel(plan, *refs):
    n_in, n_out = len(plan.in_specs), len(plan.out_specs)
    for step in plan.steps(refs[:n_in], refs[n_in : n_in + n_out], refs[n_in + n_out :]):
        step()


def run_plan(plan, collective_id, name):
    outs = pl.pallas_call(
        functools.partial(plan_kernel, plan),
        out_shape=plan.out_shape,
        in_specs=plan.in_specs,
        out_specs=plan.out_specs,
        scratch_shapes=plan.scratch,
        compiler_params=pltpu.CompilerParams(
            collective_id=collective_id, has_side_effects=True, vmem_limit_bytes=VMEM_LIMIT
        ),
        name=name,
    )(*plan.args)
    return plan.results(outs)


def exchange_kernel(dims, n_tensor, n, *refs):
    ins, outs = refs[:n], refs[n : 2 * n]
    send, recv, local = refs[2 * n :]
    place = Place(dims, n_tensor)

    def copies(i):
        for step in range(1, n_tensor):
            device, _ = place.peer(3, step)
            sems = (send.at[i, step - 1], recv.at[i, step - 1])
            yield remote(ins[i], outs[i].at[n_tensor - step], *sems, device)

    own = [pltpu.make_async_copy(ins[i], outs[i].at[0], local.at[i]) for i in range(n)]
    for copy in own:
        copy.start()
    place.barrier((3,))
    for i in range(n):
        for copy in copies(i):
            copy.start()
    for i in range(n):
        own[i].wait()
        for copy in copies(i):
            copy.wait()


def exchange_rows(arrays, dims, n_tensor, collective_id):
    n = len(arrays)
    outs = pl.pallas_call(
        functools.partial(exchange_kernel, dims, n_tensor, n),
        out_shape=[jax.ShapeDtypeStruct((n_tensor,) + a.shape, a.dtype) for a in arrays],
        in_specs=[VMEM] * n,
        out_specs=[ANY] * n,
        scratch_shapes=[
            pltpu.SemaphoreType.DMA((n, n_tensor - 1)),
            pltpu.SemaphoreType.DMA((n, n_tensor - 1)),
            pltpu.SemaphoreType.DMA((n,)),
        ],
        compiler_params=pltpu.CompilerParams(collective_id=collective_id, has_side_effects=True),
        name="exchange_rows",
    )(*arrays)
    return [o.reshape(-1, o.shape[-1]) for o in outs]


def return_kernel(dims, n_tensor, n, *refs):
    ins, outs, bufs = refs[:n], refs[n : 2 * n], refs[2 * n : 3 * n]
    send, recv = refs[3 * n :]
    place = Place(dims, n_tensor)
    rows = outs[0].shape[0]

    def copies(i):
        for step in range(1, n_tensor):
            device, _ = place.peer(3, step)
            sems = (send.at[i, step - 1], recv.at[i, step - 1])
            yield remote(ins[i].at[pl.ds(step * rows, rows), :], bufs[i].at[step - 1], *sems, device)

    place.barrier((3,))
    for i in range(n):
        for copy in copies(i):
            copy.start()
    for i in range(n):
        for copy in copies(i):
            copy.wait()
        for first in range(0, rows, 64):
            total = ins[i][first : first + 64, :].astype(jnp.float32)
            for step in range(1, n_tensor):
                total = total + bufs[i][step - 1, first : first + 64, :].astype(jnp.float32)
            outs[i][first : first + 64, :] = total.astype(outs[i].dtype)


def return_rows(arrays, dims, n_tensor, collective_id):
    n = len(arrays)
    rows, width = arrays[0].shape[0] // n_tensor, arrays[0].shape[1]
    return pl.pallas_call(
        functools.partial(return_kernel, dims, n_tensor, n),
        out_shape=[jax.ShapeDtypeStruct((rows, width), a.dtype) for a in arrays],
        in_specs=[VMEM] * n,
        out_specs=[VMEM] * n,
        scratch_shapes=[pltpu.VMEM((n_tensor - 1, rows, width), a.dtype) for a in arrays]
        + [pltpu.SemaphoreType.DMA((n, n_tensor - 1)), pltpu.SemaphoreType.DMA((n, n_tensor - 1))],
        compiler_params=pltpu.CompilerParams(collective_id=collective_id, has_side_effects=True),
        name="return_rows",
    )(*arrays)


def norm_forward(stream, gain_row, shift_row):
    centered = stream - jnp.mean(stream, axis=-1, keepdims=True)
    inv_std = lax.rsqrt(jnp.mean(centered * centered, axis=-1, keepdims=True) + EPSILON)
    normed = centered * inv_std
    return (normed * gain_row + shift_row, normed, inv_std)


def norm_backward(grad_result, normed, inv_std, gain_row):
    grad_normed = grad_result * gain_row
    return inv_std * (
        grad_normed
        - jnp.mean(grad_normed, axis=-1, keepdims=True)
        - normed * jnp.mean(grad_normed * normed, axis=-1, keepdims=True)
    )


def low(value):
    return value.astype(jnp.bfloat16)


def ffn_forward(entered, weight_in, weight_out_t):
    before = dot_nn(entered, weight_in)
    active = low(jax.nn.silu(before))
    return dot_nt(active, weight_out_t), (before, active)


def ffn_backward(entered, saved, grad_low, weight_in, weight_out_t):
    before, active = saved
    sigma = jax.nn.sigmoid(before)
    grad_active = dot_nn(grad_low, weight_out_t)
    grad_before = low(grad_active * sigma * (1.0 + before * (1.0 - sigma)))
    return dot_nt(grad_before, weight_in), [(grad_low, active), (entered, grad_before)]


def taps_forward(signal, before, conv_taps):
    rows = signal.shape[0]
    padded = jnp.concatenate([before, signal], axis=0)
    skip = before.shape[0] - (KERNEL - 1)
    result = jnp.zeros_like(signal)
    for tap in range(KERNEL):
        result = result + conv_taps[tap] * padded[skip + tap : skip + tap + rows]
    return result


def taps_backward(grad, after, signal, before, conv_taps):
    rows = signal.shape[0]
    padded_signal = jnp.concatenate([before, signal], axis=0)
    padded_grad = jnp.concatenate([grad, after], axis=0)
    skip = before.shape[0] - (KERNEL - 1)
    grad_signal = jnp.zeros_like(signal)
    taps = []
    for tap in range(KERNEL):
        back = KERNEL - 1 - tap
        grad_signal = grad_signal + conv_taps[tap] * padded_grad[back : back + rows]
        taps.append(jnp.sum(grad * padded_signal[skip + tap : skip + tap + rows], axis=0))
    return grad_signal, jnp.stack(taps)


HALO = 32


def on_device(
    dims,
    n_tensor,
    stream_in,
    grad_out,
    clip_lengths,
    first_up,
    first_down,
    attn_proj,
    attn_out,
    rel_table,
    glu_weight,
    conv_taps,
    conv_out,
    second_up,
    second_down,
    norm_gains,
    norm_shifts,
):
    rank = lax.axis_index("tensor")
    rows, width = stream_in.shape
    keys = rows * n_tensor
    early = [first_up[None], first_down.T[None], attn_proj, attn_out.T[None]]
    late = [glu_weight, conv_out.T[None], second_up[None], second_down.T[None]]
    gathered = run_plan(GatherPlan(early, dims, n_tensor), 0, "gather_weights")
    (up_one,), (down_one,), proj, (out_attn,) = gathered

    def enter(stream, row):
        result, normed, inv_std = norm_forward(stream, norm_gains[row], norm_shifts[row])
        return low(result), (normed, inv_std)

    def norm_back(grad_result, saved, row):
        normed, inv_std = saved
        grad_input = norm_backward(grad_result, normed, inv_std, norm_gains[row])
        return grad_input, jnp.sum(grad_result * normed, axis=0), jnp.sum(grad_result, axis=0)

    def shift_rank(value, step):
        pairs = [(i, i + step) for i in range(n_tensor) if 0 <= i + step < n_tensor]
        return lax.ppermute(value, "tensor", pairs)

    stream = stream_in.astype(jnp.float32)
    squares = []

    entered_a, norm_a = enter(stream, 0)
    branch, ffn_a = ffn_forward(entered_a, up_one, down_one)
    squares.append(jnp.sum(branch * branch))
    stream = stream + 0.5 * branch

    entered_b, norm_b = enter(stream, 1)
    query, own_keys, own_vals = (low(dot_nn(entered_b, proj[i])) for i in range(3))
    key_rows, val_rows = exchange_rows([own_keys, own_vals], dims, n_tensor, 2)
    place = lax.rem(jnp.arange(keys, dtype=jnp.int32) + rank * rows, keys)
    mask = jnp.where(place < clip_lengths[0], 0.0, MASKED).astype(jnp.float32)[None]
    table = span_table(rel_table)
    attended, log_totals, gathered = attn_fwd(
        query, key_rows, val_rows, table, mask, GatherPlan(late, dims, n_tensor, *HOST_G), 4
    )
    glu, (out_conv,), (up_two,), (down_two,) = gathered
    branch = dot_nt(attended, out_attn)
    squares.append(jnp.sum(branch * branch))
    stream = stream + branch

    entered_c, norm_c = enter(stream, 2)
    glu_first = dot_nn(entered_c, glu[0])
    glu_second = dot_nn(entered_c, glu[1])
    sig_second = jax.nn.sigmoid(glu_second)
    gated = glu_first * sig_second
    gated_before = shift_rank(gated[rows - HALO :], 1)
    mixed = taps_forward(gated, gated_before, conv_taps)
    shaped, normed_mid, scale_mid = norm_forward(mixed, norm_gains[3], norm_shifts[3])
    conv_act = low(jax.nn.silu(shaped))
    branch = dot_nt(conv_act, out_conv)
    squares.append(jnp.sum(branch * branch))
    stream = stream + branch

    entered_d, norm_d = enter(stream, 4)
    branch, ffn_d = ffn_forward(entered_d, up_two, down_two)
    squares.append(jnp.sum(branch * branch))
    stream = stream + 0.5 * branch
    squares.append(jnp.sum(stream * stream))
    result, normed_e, scale_e = norm_forward(stream, norm_gains[5], norm_shifts[5])
    output = low(result)

    grad_stream, gain_e, shift_e = norm_back(grad_out.astype(jnp.float32), (normed_e, scale_e), 5)
    grad_low = low(0.5 * grad_stream)
    grad_entered, terms_two = ffn_backward(entered_d, ffn_d, grad_low, up_two, down_two)
    grad_extra, gain_d, shift_d = norm_back(grad_entered, norm_d, 4)
    grad_stream = grad_stream + grad_extra

    grad_low = low(grad_stream)
    terms_mid = [(grad_low, conv_act)]
    sigma = jax.nn.sigmoid(shaped)
    grad_shaped = dot_nn(grad_low, out_conv) * sigma * (1.0 + shaped * (1.0 - sigma))
    grad_mixed, gain_mid, shift_mid = norm_back(grad_shaped, (normed_mid, scale_mid), 3)
    grad_after = shift_rank(grad_mixed[:HALO], -1)
    grad_gated, taps_grad = taps_backward(grad_mixed, grad_after, gated, gated_before, conv_taps)
    grad_first = low(grad_gated * sig_second)
    grad_second = low(grad_gated * glu_first * sig_second * (1.0 - sig_second))
    terms_mid += [(entered_c, g) for g in (grad_first, grad_second)]
    grad_entered = dot_nt(grad_first, glu[0]) + dot_nt(grad_second, glu[1])
    grad_extra, gain_c, shift_c = norm_back(grad_entered, norm_c, 2)
    grad_stream = grad_stream + grad_extra

    grad_low = low(grad_stream)
    terms_attn = [(grad_low, attended)]
    grad_attended = low(dot_nn(grad_low, out_attn))
    grad_query, grad_keys, grad_vals, grad_span, summed = attn_bwd(
        query, key_rows, val_rows, grad_attended, attended, log_totals, table, mask,
        ScatterPlan(terms_two + terms_mid, None, dims, n_tensor, *HOST_S), 5,
    )
    s_down_two, s_up_two, s_conv, s_glu0, s_glu1 = summed
    grad_keys, grad_vals = return_rows([grad_keys, grad_vals], dims, n_tensor, 3)
    grad_parts = (grad_query, grad_keys, grad_vals)
    terms_attn += [(entered_b, g) for g in grad_parts]
    grad_entered = sum(dot_nt(g, proj[i]) for i, g in enumerate(grad_parts))
    grad_extra, gain_b, shift_b = norm_back(grad_entered, norm_b, 1)
    grad_stream = grad_stream + grad_extra

    grad_low = low(0.5 * grad_stream)
    grad_entered, terms_one = ffn_backward(entered_a, ffn_a, grad_low, up_one, down_one)
    grad_extra, gain_a, shift_a = norm_back(grad_entered, norm_a, 0)
    grad_stream = grad_stream + grad_extra

    span_grad = fold_table(grad_span)
    span_rows = -(-span_grad.size // width)
    table_rows = jnp.pad(span_grad.reshape(-1), (0, span_rows * width - span_grad.size)).reshape(span_rows, width)
    square_row = jnp.pad(jnp.stack(squares), (0, width - len(squares)))[None]
    parts = [
        jnp.stack([gain_a, gain_b, gain_c, gain_mid, gain_d, gain_e]),
        jnp.stack([shift_a, shift_b, shift_c, shift_mid, shift_d, shift_e]),
        taps_grad,
        table_rows,
        square_row,
    ]
    vec = jnp.concatenate(parts, axis=0)
    vec = jnp.pad(vec, ((0, -vec.shape[0] % 8), (0, 0)))
    *summed, vec = run_plan(ScatterPlan(terms_attn + terms_one, vec, dims, n_tensor), 1, "scatter_grads")
    s_attn, s_q, s_k, s_v, s_down_one, s_up_one = summed
    at = 0
    pieces = []
    for part in parts:
        pieces.append(vec[at : at + part.shape[0]])
        at += part.shape[0]
    gains_sum, shifts_sum, taps_sum, table_sum, square_sum = pieces
    table_sum = table_sum.reshape(-1)[: span_grad.size].reshape(span_grad.shape)
    count_all = float(lax.axis_size("dp") * keys * width)
    rms_values = jnp.sqrt(square_sum[0, : len(squares)] / count_all)
    return (
        output,
        grad_stream,
        s_up_one,
        s_down_one.T,
        jnp.stack([s_q, s_k, s_v]),
        s_attn.T,
        table_sum,
        jnp.stack([s_glu0, s_glu1]),
        taps_sum,
        s_conv.T,
        s_up_two,
        s_down_two.T,
        gains_sum,
        shifts_sum,
        rms_values,
    )


def solution(mesh):
    n_dp, n_tensor = mesh.shape["dp"], mesh.shape["tensor"]
    dims = FACTORS.get(n_dp, (n_dp, 1, 1))
    return jax.shard_map(
        functools.partial(on_device, dims, n_tensor),
        mesh=mesh,
        in_specs=(
            P(("dp", "tensor"), None),
            P(("dp", "tensor"), None),
            P("dp"),
            P("dp", "tensor"),
            P("tensor", "dp"),
            P(None, "dp", "tensor"),
            P("tensor", "dp"),
            P(),
            P(None, "dp", "tensor"),
            P(),
            P("tensor", "dp"),
            P("dp", "tensor"),
            P("tensor", "dp"),
            P(),
            P(),
        ),
        out_specs=(
            P(("dp", "tensor"), None),
            P(("dp", "tensor"), None),
            P("dp", "tensor"),
            P("tensor", "dp"),
            P(None, "dp", "tensor"),
            P("tensor", "dp"),
            P(),
            P(None, "dp", "tensor"),
            P(),
            P("tensor", "dp"),
            P("dp", "tensor"),
            P("tensor", "dp"),
            P(),
            P(),
            P(),
        ),
        check_vma=False,
    )
```

```python
import functools

import jax
import jax.numpy as jnp
from jax import lax
from jax.experimental import pallas as pl
from jax.experimental.pallas import tpu as pltpu
from jax.sharding import PartitionSpec as P

HEAD = 64
KERNEL = 31
LEFT = 64
RIGHT = 8
EPSILON = 1e-05
MASKED = -1e30
VMEM_LIMIT = 66_000_000
HOST_G = (512, 6, 5)
HOST_S = (256, 8, 4)
BLK = 128
SPAN = 512
NT = (((1,), (1,)), ((), ()))
TN = (((0,), (0,)), ((), ()))


def dot_nt(a, b):
    return lax.dot_general(a, b, NT, preferred_element_type=jnp.float32)


def dot_tn(a, b):
    return lax.dot_general(a, b, TN, preferred_element_type=jnp.float32)


def dot_nn(a, b):
    return jnp.dot(a, b, preferred_element_type=jnp.float32)


def rel_blocks(tin, b, own_blocks, key_blocks, rank):
    t_left, t_right = tin[:, 0:1], tin[:, SPAN - 1 : SPAN]
    band = pltpu.roll(tin, SPAN - BLK, 1, stride=1, stride_axis=0)
    out = []
    for kb in range(key_blocks):
        wraps = rank * own_blocks + kb >= key_blocks
        if kb in (b - 1, b) or (kb == b + 1 and kb < own_blocks):
            out.append(band[:, (kb - b + 1) * BLK : (kb - b + 2) * BLK])
        elif kb == b + 1:
            out.append(jnp.where(wraps, t_left, band[:, 2 * BLK : 3 * BLK]))
        elif b == 0 and kb == key_blocks - 1:
            out.append(jnp.where(wraps, band[:, :BLK], t_right))
        elif kb < b - 1:
            out.append(t_left)
        elif kb < own_blocks:
            out.append(t_right)
        else:
            out.append(jnp.where(wraps, t_left, t_right))
    return out


def halves(x):
    low = lax.broadcasted_iota(jnp.int32, x.shape, 1) < HEAD
    zero = jnp.zeros_like(x)
    return jnp.where(low, x, zero), jnp.where(low, zero, x)


def flip_rows(x):
    tiles = []
    back = 7 - lax.broadcasted_iota(jnp.int32, (8, BLK), 0)
    for first in range(x.shape[0] - 8, -1, -8):
        cols = [
            jnp.take_along_axis(x[first : first + 8, c : c + BLK], back, axis=0, mode="promise_in_bounds")
            for c in range(0, x.shape[1], BLK)
        ]
        tiles.append(jnp.concatenate(cols, axis=1) if len(cols) > 1 else cols[0])
    return jnp.concatenate(tiles, axis=0)


def split_refs(refs, sizes):
    out, at = [], 0
    for size in sizes:
        out.append(refs[at : at + size])
        at += size
    return out


def ticker(plan, ins, outs, scratch, ticks):
    if plan is None:
        return lambda block, blocks: None
    steps = plan.steps(ins, outs, scratch)

    def tick(block, blocks):
        for number, step in enumerate(steps):
            at = min(number * ticks // (len(steps) - 1), ticks - 1) if number < len(steps) - 1 else ticks
            if at < ticks and at % blocks == block:
                pl.when(pl.program_id(0) == at // blocks)(step)
            if at == ticks and block == blocks:
                pl.when(pl.program_id(0) == ticks // blocks - 1)(step)

    return tick


def attn_fwd_kernel(plan, *refs):
    n_in, n_out = (len(plan.in_specs), len(plan.out_specs)) if plan else (0, 0)
    own, plan_in, (o_ref, lse_ref), plan_out, plan_scratch = split_refs(refs, (5, n_in, 2, n_out, len(refs)))
    q_ref, k_ref, v_ref, tab_ref, mask_ref = own
    rank = lax.axis_index("tensor")
    rows, keys = q_ref.shape[0], k_ref.shape[0]
    own_blocks, key_blocks = rows // BLK, keys // BLK
    low = lax.broadcasted_iota(jnp.int32, (BLK, 2 * HEAD), 1) < HEAD
    tick = ticker(plan, plan_in, plan_out, plan_scratch, own_blocks * pl.num_programs(0))
    for b in range(own_blocks):
        tick(b, own_blocks)
        q_blk = q_ref[b * BLK : (b + 1) * BLK, :] * jnp.asarray(HEAD**-0.5, jnp.bfloat16)
        results = []
        for hh, q_one in enumerate(halves(q_blk)):
            tin = dot_nt(q_one, tab_ref[...])
            rel = rel_blocks(tin, b, own_blocks, key_blocks, rank)
            raw = dot_nt(q_one, k_ref[...])
            s = [
                raw[:, kb * BLK : (kb + 1) * BLK] + rel[kb] + mask_ref[:, kb * BLK : (kb + 1) * BLK]
                for kb in range(key_blocks)
            ]
            s = jnp.concatenate(s, axis=1)
            peak = jnp.max(s, axis=-1, keepdims=True)
            e = jnp.exp(s - peak)
            total = jnp.sum(e, axis=-1, keepdims=True)
            o = dot_nn(e.astype(jnp.bfloat16), v_ref[...])
            results.append(o / total)
            first = (hh * own_blocks + b) * BLK
            lse_ref[0, first : first + BLK, :] = peak + jnp.log(total)
        o_ref[b * BLK : (b + 1) * BLK, :] = jnp.where(low, results[0], results[1]).astype(jnp.bfloat16)
    tick(own_blocks, own_blocks)


def attn_fwd(q, k, v, tab2, mask, plan=None, collective_id=None):
    rows, width = q.shape
    keys = k.shape[0]
    pairs = width // (2 * HEAD)
    col = lambda n: pl.BlockSpec((n, 2 * HEAD), lambda p: (0, p))
    out_specs = [col(rows), pl.BlockSpec((1, 2 * rows, 1), lambda p: (p, 0, 0))]
    out_shape = [
        jax.ShapeDtypeStruct((rows, width), jnp.bfloat16),
        jax.ShapeDtypeStruct((pairs, 2 * rows, 1), jnp.float32),
    ]
    outs = pl.pallas_call(
        functools.partial(attn_fwd_kernel, plan),
        grid=(pairs,),
        in_specs=[
            col(rows),
            col(keys),
            col(keys),
            pl.BlockSpec((SPAN, 2 * HEAD), lambda p: (0, 0)),
            pl.BlockSpec((1, keys), lambda p: (0, 0)),
        ]
        + (plan.in_specs if plan else []),
        out_specs=out_specs + (plan.out_specs if plan else []),
        out_shape=out_shape + (plan.out_shape if plan else []),
        scratch_shapes=plan.scratch if plan else [],
        compiler_params=pltpu.CompilerParams(
            collective_id=collective_id, has_side_effects=plan is not None, vmem_limit_bytes=VMEM_LIMIT
        ),
        name="attn_fwd",
    )(q, k, v, tab2, mask, *(plan.args if plan else []))
    return outs[0], outs[1], plan.results(outs[2:]) if plan else []


def attn_bwd_kernel(plan, *refs):
    n_in, n_out = (len(plan.in_specs), len(plan.out_specs)) if plan else (0, 0)
    own, plan_in, own_out, plan_out, own_scratch, plan_scratch = split_refs(refs, (8, n_in, 4, n_out, 4, len(refs)))
    q_ref, k_ref, v_ref, do_ref, o_ref, lse_ref, tab_ref, mask_ref = own
    dq_ref, dk_ref, dv_ref, dtab_ref = own_out
    p_sc, ds_sc, q_sc, do_sc = own_scratch
    rank = lax.axis_index("tensor")
    rows, keys = q_ref.shape[0], k_ref.shape[0]
    own_blocks, key_blocks = rows // BLK, keys // BLK
    low = lax.broadcasted_iota(jnp.int32, (BLK, 2 * HEAD), 1) < HEAD
    lane = lax.broadcasted_iota(jnp.int32, (BLK, BLK), 1)
    scale = jnp.asarray(HEAD**-0.5, jnp.bfloat16)

    @pl.when(pl.program_id(0) == 0)
    def _():
        dtab_ref[...] = jnp.zeros_like(dtab_ref)

    tick = ticker(plan, plan_in, plan_out, plan_scratch, own_blocks * pl.num_programs(0))
    for b in range(own_blocks):
        tick(b, own_blocks)
        at = slice(b * BLK, (b + 1) * BLK)
        q_blk = q_ref[at, :] * scale
        do_blk = do_ref[at, :]
        prod = do_blk.astype(jnp.float32) * o_ref[at, :].astype(jnp.float32)
        q_back = halves(flip_rows(q_blk.astype(jnp.float32)).astype(jnp.bfloat16))
        results = []
        for hh, (q_one, do_one, pr_one) in enumerate(zip(halves(q_blk), halves(do_blk), halves(prod))):
            first = (hh * own_blocks + b) * BLK
            here = slice(first, first + BLK)
            inner = jnp.sum(pr_one, axis=-1, keepdims=True)
            lse = lse_ref[0, here, :]
            tin = dot_nt(q_one, tab_ref[...])
            rel = rel_blocks(tin - lse, b, own_blocks, key_blocks, rank)
            raw = dot_nt(q_one, k_ref[...])
            dp = dot_nt(do_one, v_ref[...])
            left = jnp.zeros((BLK, BLK), jnp.float32)
            right = jnp.zeros((BLK, BLK), jnp.float32)
            window = [None, None, None]
            for kb in range(key_blocks):
                ks = slice(kb * BLK, (kb + 1) * BLK)
                p = jnp.exp(raw[:, ks] + rel[kb] + mask_ref[:, ks])
                ds = (p * (dp[:, ks] - inner)).astype(jnp.bfloat16)
                p_sc[here, ks] = p.astype(jnp.bfloat16)
                ds_sc[here, ks] = ds
                ds = ds.astype(jnp.float32)
                wraps = rank * own_blocks + kb >= key_blocks
                zero = jnp.zeros_like(ds)
                if kb in (b - 1, b) or (kb == b + 1 and kb < own_blocks):
                    window[kb - b + 1] = ds
                elif kb == b + 1:
                    window[2] = jnp.where(wraps, zero, ds)
                    left = left + jnp.where(wraps, ds, zero)
                elif b == 0 and kb == key_blocks - 1:
                    window[0] = jnp.where(wraps, ds, zero)
                    right = right + jnp.where(wraps, zero, ds)
                elif kb < b - 1:
                    left = left + ds
                elif kb < own_blocks:
                    right = right + ds
                else:
                    left = left + jnp.where(wraps, ds, zero)
                    right = right + jnp.where(wraps, zero, ds)
            none = jnp.zeros((BLK, BLK), jnp.float32)
            window = jnp.concatenate([none if w is None else flip_rows(w) for w in window] + [none], axis=1)
            back = pltpu.roll(window, 1, 1, stride=1, stride_axis=0)
            s_left = flip_rows(jnp.broadcast_to(jnp.sum(left, axis=-1, keepdims=True), (BLK, BLK)))
            s_right = flip_rows(jnp.broadcast_to(jnp.sum(right, axis=-1, keepdims=True), (BLK, BLK)))
            u = jnp.concatenate(
                [
                    back[:, :BLK] + jnp.where(lane == 0, s_left, 0.0),
                    back[:, BLK : 3 * BLK],
                    back[:, 3 * BLK :] + jnp.where(lane == BLK - 1, s_right, 0.0),
                ],
                axis=1,
            ).astype(jnp.bfloat16)
            q_sc[here, :] = q_one
            do_sc[here, :] = do_one
            dtab_ref[...] += dot_tn(u, q_back[hh])
            results.append(dot_nn(ds_sc[here, :], k_ref[...]) + flip_rows(dot_nn(u, tab_ref[...])))
        dq_ref[at, :] = (jnp.where(low, results[0], results[1]) * HEAD**-0.5).astype(jnp.bfloat16)
    dk_ref[...] = dot_tn(ds_sc[...], q_sc[...]).astype(dk_ref.dtype)
    dv_ref[...] = dot_tn(p_sc[...], do_sc[...]).astype(dv_ref.dtype)
    tick(own_blocks, own_blocks)


def attn_bwd(q, k, v, do, o, lse, tab2, mask, plan=None, collective_id=None):
    rows, width = q.shape
    keys = k.shape[0]
    pairs = width // (2 * HEAD)
    col = lambda n: pl.BlockSpec((n, 2 * HEAD), lambda p: (0, p))
    table = pl.BlockSpec((SPAN, 2 * HEAD), lambda p: (0, 0))
    out_shape = [
        jax.ShapeDtypeStruct((rows, width), jnp.bfloat16),
        jax.ShapeDtypeStruct((keys, width), jnp.bfloat16),
        jax.ShapeDtypeStruct((keys, width), jnp.bfloat16),
        jax.ShapeDtypeStruct((SPAN, 2 * HEAD), jnp.float32),
    ]
    outs = pl.pallas_call(
        functools.partial(attn_bwd_kernel, plan),
        grid=(pairs,),
        in_specs=[
            col(rows),
            col(keys),
            col(keys),
            col(rows),
            col(rows),
            pl.BlockSpec((1, 2 * rows, 1), lambda p: (p, 0, 0)),
            table,
            pl.BlockSpec((1, keys), lambda p: (0, 0)),
        ]
        + (plan.in_specs if plan else []),
        out_specs=[col(rows), col(keys), col(keys), table] + (plan.out_specs if plan else []),
        out_shape=out_shape + (plan.out_shape if plan else []),
        scratch_shapes=[
            pltpu.VMEM((2 * rows, keys), jnp.bfloat16),
            pltpu.VMEM((2 * rows, keys), jnp.bfloat16),
            pltpu.VMEM((2 * rows, 2 * HEAD), jnp.bfloat16),
            pltpu.VMEM((2 * rows, 2 * HEAD), jnp.bfloat16),
        ]
        + (plan.scratch if plan else []),
        compiler_params=pltpu.CompilerParams(
            collective_id=collective_id, has_side_effects=plan is not None, vmem_limit_bytes=VMEM_LIMIT
        ),
        name="attn_bwd",
    )(q, k, v, do, o, lse, tab2, mask, *(plan.args if plan else []))
    return (*outs[:4], plan.results(outs[4:]) if plan else [])


def span_table(rel_table):
    rows = jnp.clip(jnp.arange(SPAN) - SPAN // 2, -LEFT, RIGHT) + LEFT
    table = jnp.take(rel_table, rows, axis=0)
    return jnp.concatenate([table, table], axis=1)


def fold_table(dtab):
    one = dtab[:, :HEAD] + dtab[:, HEAD:]
    rows = jnp.clip(jnp.arange(SPAN) - SPAN // 2, -LEFT, RIGHT) + LEFT
    pick = (rows[None, :] == jnp.arange(LEFT + RIGHT + 1)[:, None]).astype(jnp.float32)
    return jnp.dot(pick, one, precision=lax.Precision.HIGHEST)


MESH = pl.DeviceIdType.MESH
ANY = pl.BlockSpec(memory_space=pl.ANY)
VMEM = pl.BlockSpec(memory_space=pltpu.VMEM)
FACTORS = {16: (4, 2, 2), 32: (4, 2, 4)}


class Place:
    def __init__(self, dims, n_tensor):
        self.dims, self.n_tensor = dims, n_tensor
        n_a, n_b, n_c = dims
        d = lax.axis_index("dp")
        self.t = lax.axis_index("tensor")
        self.at = (lax.div(d, n_b * n_c), lax.rem(lax.div(d, n_c), n_b), lax.rem(d, n_c))

    def peer(self, axis, step):
        at, t = list(self.at), self.t
        if axis == 3:
            t = lax.rem(t + step, self.n_tensor)
            index = t
        else:
            at[axis] = index = lax.rem(at[axis] + step, self.dims[axis])
        n_a, n_b, n_c = self.dims
        return ((at[0] * n_b + at[1]) * n_c + at[2], t), index

    def size(self, axis):
        return self.n_tensor if axis == 3 else self.dims[axis]

    def barrier(self, axes=(0, 1, 2, 3)):
        sem = pltpu.get_barrier_semaphore()
        count = 0
        for axis in axes:
            for step in range(1, self.size(axis)):
                pl.semaphore_signal(sem, inc=1, device_id=self.peer(axis, step)[0], device_id_type=MESH)
                count += 1
        pl.semaphore_wait(sem, count)


def remote(src, dst, send_sem, recv_sem, device):
    return pltpu.make_async_remote_copy(
        src_ref=src, dst_ref=dst, send_sem=send_sem, recv_sem=recv_sem, device_id=device, device_id_type=MESH
    )


class Piece:
    def __init__(self, source, lead, first, width):
        self.source, self.lead, self.first, self.width = source, lead, first, width


def pieces_of(parts, chunk):
    return [
        Piece(source, lead, first, min(chunk, cols - first))
        for source, (n, cols) in enumerate(parts)
        for lead in range(n)
        for first in range(0, cols, chunk)
    ]


def run_all(copies, action):
    for copy in copies:
        getattr(copy, action)()


class Gather:
    NORMAL = ((0, 1, 2), (0, 2, 1))
    EARLY = ((2, 1, 0), (1, 2, 0))

    def __init__(self, place, piece, orders, shard, whole, send, recv, local):
        self.place, self.piece, self.orders = place, piece, orders
        self.shard, self.whole = shard, whole
        self.send, self.recv, self.local = send, recv, local
        self.half = shard.shape[1] // 2

    @staticmethod
    def slots(dims, n_tensor):
        return 2 * (sum(d - 1 for d in dims) + 2 * (n_tensor - 1))

    def slot(self, color, stage, step):
        place, order = self.place, self.orders[color]
        sizes = [place.dims[x] - 1 for x in order] + [place.n_tensor - 1] * 2
        return color * sum(sizes) + sum(sizes[:stage]) + step - 1

    def columns(self, t):
        piece = self.piece
        return pl.ds(pl.multiple_of(t * self.shard.shape[2] + piece.first, 128), piece.width)

    def region(self, color, index, t):
        rows = pl.ds(color * self.half, self.half)
        return self.whole.at[(self.piece.lead,) + tuple(index) + (rows, self.columns(t))]

    def source(self, rows):
        piece = self.piece
        return self.shard.at[piece.lead, rows, pl.ds(piece.first, piece.width)]

    def index(self, color, stage, moved=None):
        order, out = self.orders[color], list(self.place.at)
        for axis in order[:stage]:
            out[axis] = slice(None)
        if moved is not None:
            out[order[stage]] = moved
        return out

    def own(self):
        there = self.whole.at[(self.piece.lead,) + self.place.at + (slice(None), self.columns(self.place.t))]
        return pltpu.make_async_copy(self.source(slice(None)), there, self.local)

    def copies(self, stage, arriving=False):
        place, t = self.place, self.place.t
        for color, order in enumerate(self.orders):
            in_one = place.dims[order[2]] > 2
            if stage == 3 and in_one:
                continue
            axis = order[stage] if stage < 3 else 3
            for step in range(1, place.size(axis)):
                device, _ = place.peer(axis, step)
                _, origin = place.peer(axis, place.size(axis) - step)
                slot = self.slot(color, stage, step)
                if stage < 3:
                    index, there, then = self.index(color, stage), self.index(color, stage, origin), t
                else:
                    if in_one:
                        index = self.index(color, 3)
                    elif stage == 3:
                        index = self.index(color, 2)
                    else:
                        index = self.index(color, 2, place.peer(order[2], 1)[1])
                    there, then = index, origin
                mine, theirs = self.region(color, index, t), self.region(color, there, then)
                origin_ref = self.source(pl.ds(color * self.half, self.half)) if stage == 0 else mine
                sems = (self.send.at[slot], self.recv.at[slot], device)
                yield remote(theirs, theirs, *sems) if arriving else remote(origin_ref, mine, *sems)

    def start(self, stage):
        run_all(self.copies(stage), "start")

    def arrived(self, stage):
        run_all(self.copies(stage, arriving=True), "wait_recv")

    def sent(self, stage):
        run_all(self.copies(stage), "wait_send")


class GatherPlan:
    def __init__(self, shards, dims, n_tensor, chunk=1024, every=6, depth=3):
        self.dims, self.n_tensor, self.depth = dims, n_tensor, depth
        self.args = list(shards)
        self.pieces = pieces_of([(s.shape[0], s.shape[2]) for s in shards], chunk)
        self.orders = [Gather.EARLY if i % every == 0 else Gather.NORMAL for i in range(len(self.pieces))]
        count, slots = len(self.pieces), Gather.slots(dims, n_tensor)
        self.in_specs = [VMEM] * len(shards)
        self.out_specs = [ANY] * len(shards)
        self.out_shape = [
            jax.ShapeDtypeStruct((s.shape[0], *dims, s.shape[1], n_tensor * s.shape[2]), s.dtype) for s in shards
        ]
        self.scratch = [
            pltpu.SemaphoreType.DMA((count, slots)),
            pltpu.SemaphoreType.DMA((count, slots)),
            pltpu.SemaphoreType.DMA((count,)),
        ]

    def results(self, outs):
        return [o.reshape(o.shape[0], -1, o.shape[-1]) for o in outs]

    def steps(self, shards, wholes, scratch):
        send, recv, local = scratch
        place = Place(self.dims, self.n_tensor)
        gathers = [
            Gather(place, p, orders, shards[p.source], wholes[p.source], send.at[i], recv.at[i], local.at[i])
            for i, (p, orders) in enumerate(zip(self.pieces, self.orders))
        ]
        return self.steps_of(place, gathers)

    def steps_of(self, place, gathers, read=()):
        count, depth = len(gathers), self.depth

        def begin():
            for g in gathers:
                g.own().start()
            place.barrier()
            for g in gathers:
                g.start(0)
            for g in gathers:
                g.own().wait()

        def step(i):
            if i < count:
                gathers[i].arrived(0)
                gathers[i].start(1)
            at = i - depth
            if 0 <= at < count:
                gathers[at].arrived(1)
                gathers[at].start(2)
                gathers[at].start(3)
            at = i - 2 * depth
            if 0 <= at < count:
                gathers[at].arrived(2)
                gathers[at].start(4)

        def end():
            for i, g in enumerate(gathers):
                if i not in read:
                    g.arrived(3)
                    g.arrived(4)
                for stage in range(5):
                    g.sent(stage)

        return [begin] + [functools.partial(step, i) for i in range(count + 2 * depth)] + [end]


class FeedPlan(GatherPlan):
    TILE = 512

    def __init__(self, shards, entered, dims, n_tensor):
        super().__init__(shards, dims, n_tensor)
        tokens, width = entered.shape
        cols = shards[0].shape[2]
        hidden = cols * n_tensor
        fed = sorted((p for p in self.pieces if p.source < 2), key=lambda p: (p.first, p.source))
        self.pieces = fed + [p for p in self.pieces if p.source >= 2]
        self.pairs = len(fed) // 2
        self.tile = tile = min(self.TILE, fed[0].width)
        self.args = self.args + [entered]
        self.in_specs = self.in_specs + [VMEM]
        self.out_specs = self.out_specs + [ANY, ANY, VMEM]
        self.out_shape = self.out_shape + [
            jax.ShapeDtypeStruct((tokens, hidden), jnp.float32),
            jax.ShapeDtypeStruct((tokens, hidden), jnp.bfloat16),
            jax.ShapeDtypeStruct((tokens, width), jnp.float32),
        ]
        rows = shards[0].shape[1]
        self.scratch = self.scratch + [
            pltpu.VMEM((2, 2, *dims, rows, tile), jnp.bfloat16),
            pltpu.VMEM((2, tokens, tile), jnp.float32),
            pltpu.VMEM((2, tokens, tile), jnp.bfloat16),
            pltpu.SemaphoreType.DMA((2, 2)),
            pltpu.SemaphoreType.DMA((2, 2)),
        ]

    def results(self, outs):
        return super().results(outs[:-3]) + list(outs[-3:])

    def steps(self, ins, outs, scratch):
        send, recv, local, weights, pre_st, act_st, load_sem, store_sem = scratch
        place = Place(self.dims, self.n_tensor)
        shards, entered = ins[:-1], ins[-1]
        wholes, (before, active, branch) = outs[:-3], outs[-3:]
        gathers = [
            Gather(place, p, orders, shards[p.source], wholes[p.source], send.at[i], recv.at[i], local.at[i])
            for i, (p, orders) in enumerate(zip(self.pieces, self.orders))
        ]
        steps = self.steps_of(place, gathers, range(2 * self.pairs))
        tile, tokens, width = self.tile, entered.shape[0], entered.shape[1]
        tiles = [
            (pair, t * shards[0].shape[2] + self.pieces[2 * pair].first + sub * tile)
            for pair in range(self.pairs)
            for t in range(self.n_tensor)
            for sub in range(self.pieces[2 * pair].width // tile)
        ]

        def loads(number):
            cols = pl.ds(tiles[number][1], tile)
            for k in (0, 1):
                origin = wholes[k].at[0, :, :, :, :, cols]
                yield pltpu.make_async_copy(origin, weights.at[number % 2, k], load_sem.at[number % 2, k])

        def stores(number):
            cols, slot = pl.ds(tiles[number][1], tile), number % 2
            yield pltpu.make_async_copy(pre_st.at[slot], before.at[:, cols], store_sem.at[slot, 0])
            yield pltpu.make_async_copy(act_st.at[slot], active.at[:, cols], store_sem.at[slot, 1])

        def feed(number):
            slot, pair = number % 2, tiles[number][0]
            if number == 0 or tiles[number - 1][0] != pair:
                for g in gathers[2 * pair : 2 * pair + 2]:
                    g.arrived(3)
                    g.arrived(4)
                run_all(loads(number), "start")
            run_all(loads(number), "wait")
            if number + 1 < len(tiles) and tiles[number + 1][0] == pair:
                run_all(loads(number + 1), "start")
            if number >= 2:
                run_all(stores(number - 2), "wait")
            up = weights[slot, 0].reshape(width, tile)
            pre = dot_nn(entered[...], up)
            pre_st[slot] = pre
            act = low(jax.nn.silu(pre))
            act_st[slot] = act
            run_all(stores(number), "start")
            added = dot_nt(act, weights[slot, 1].reshape(width, tile))
            branch[...] = added if number == 0 else branch[...] + added
            if number == len(tiles) - 1:
                for last in range(max(number - 1, 0), number + 1):
                    run_all(stores(last), "wait")

        first = [2 * pair + 2 + 2 * self.depth + 1 for pair in range(self.pairs)]
        out, at = [], 0
        for number, step in enumerate(steps[:-1]):
            out.append(step)
            rest = len(steps) - 2 - number
            room = -(-(len(tiles) - at) // max(rest + 1, 1)) if number > first[0] else 0
            while room and at < len(tiles) and number > first[tiles[at][0]]:
                out.append(functools.partial(feed, at))
                at, room = at + 1, room - 1
        out += [functools.partial(feed, k) for k in range(at, len(tiles))]
        return out + steps[-1:]


class Scatter:
    NORMAL = ((2, 1, 0), (1, 2, 0))
    EARLY = ((0, 1, 2), (0, 2, 1))

    def __init__(self, place, piece, orders, left_op, slabs, out, held, near, sent, bufs, sems):
        self.place, self.piece, self.orders = place, piece, orders
        self.left_op, self.slabs, self.out = left_op, slabs, out
        self.held, self.near, self.sent, self.bufs = held, near, sent, bufs
        self.send, self.recv = sems
        self.half = held.shape[3] // 2

    @staticmethod
    def slots(dims, n_tensor):
        return n_tensor - 1 + 2 * sum(d - 1 for d in dims)

    @staticmethod
    def left(order, stage):
        return [x for x in (0, 1, 2) if x not in order[:stage]]

    def product(self, t, target):
        n_a, n_b, n_c = self.place.dims
        rows = self.held.shape[3]
        block = n_b * n_c * rows

        def body(a, _):
            lhs = self.left_op[pl.ds(pl.multiple_of(a * block, block), block), :]
            value = dot_nn(lhs, self.slabs[t]).astype(jnp.bfloat16)
            target[a] = value.reshape(n_b, n_c, rows, value.shape[-1])
            return 0

        lax.fori_loop(0, n_a, body, 0)

    def compute(self):
        for step, copy in enumerate(self.copies(0)):
            self.product(self.place.peer(3, step + 1)[1], self.sent.at[step])
            copy.start()
        self.product(self.place.t, self.held)

    def copies(self, stage):
        place = self.place
        if stage == 0:
            for step in range(1, place.n_tensor):
                sems = (self.send.at[step - 1], self.recv.at[step - 1], place.peer(3, step)[0])
                yield remote(self.sent.at[step - 1], self.near.at[step - 1], *sems)
            return
        base = place.n_tensor - 1
        for color, order in enumerate(self.orders):
            axis = order[stage - 1]
            for step in range(1, place.size(axis)):
                device, there = place.peer(axis, step)
                index = [slice(None)] * 3
                for done in order[: stage - 1]:
                    index[done] = place.at[done]
                index[axis] = there
                slot = base + color * sum(d - 1 for d in place.dims)
                slot += sum(place.size(x) - 1 for x in order[: stage - 1]) + step - 1
                origin = self.held.at[tuple(index) + (pl.ds(color * self.half, self.half),)]
                sems = (self.send.at[slot], self.recv.at[slot], device)
                yield remote(origin, self.bufs[stage - 1][color].at[step - 1], *sems)

    def add_tensor(self):
        n_a, n_b, n_c = self.place.dims

        def body(i, _):
            at = (lax.div(i, n_b * n_c), lax.rem(lax.div(i, n_c), n_b), lax.rem(i, n_c))
            total = self.held[at].astype(jnp.float32)
            for step in range(1, self.place.n_tensor):
                total = total + self.near[(step - 1,) + at].astype(jnp.float32)
            self.held[at] = total.astype(jnp.bfloat16)
            return 0

        lax.fori_loop(0, n_a * n_b * n_c, body, 0)

    def add(self, stage):
        place, piece = self.place, self.piece
        for color, order in enumerate(self.orders):
            rows = slice(color * self.half, (color + 1) * self.half)
            left = self.left(order, stage)
            buf = self.bufs[stage - 1][color]

            def total_at(where):
                at = list(place.at)
                for x, w in zip(left, where):
                    at[x] = w
                at = tuple(at) + (rows,)
                total = self.held[at].astype(jnp.float32)
                for step in range(1, place.size(order[stage - 1])):
                    total = total + buf[(step - 1,) + where].astype(jnp.float32)
                return at, total

            def body(i, _):
                if len(left) == 2:
                    size = place.dims[left[1]]
                    at, total = total_at((lax.div(i, size), lax.rem(i, size)))
                else:
                    at, total = total_at((i,))
                self.held[at] = total.astype(jnp.bfloat16)
                return 0

            if left:
                count = 1
                for x in left:
                    count *= place.dims[x]
                lax.fori_loop(0, count, body, 0)
            else:
                cols = slice(piece.first, piece.first + piece.width)
                self.out[rows, cols] = total_at(())[1]


class Total:
    AXES = (3, 2, 1, 0)

    def __init__(self, place, value, out, boxes, send, recv):
        self.place, self.value, self.out, self.boxes, self.send, self.recv = place, value, out, boxes, send, recv

    @staticmethod
    def slots(dims, n_tensor):
        return sum(dims) + n_tensor - 4

    def copies(self, stage):
        place, axis = self.place, self.AXES[stage]
        base = sum(place.size(x) - 1 for x in self.AXES[:stage])
        for step in range(1, place.size(axis)):
            device, _ = place.peer(axis, step)
            sems = (self.send.at[base + step - 1], self.recv.at[base + step - 1], device)
            yield remote(self.value.at[stage], self.boxes[stage].at[step - 1], *sems)

    def add(self, stage):
        place, axis = self.place, self.AXES[stage]
        size = place.size(axis)
        mine = place.t if axis == 3 else place.at[axis]
        own = self.value[stage]
        if size == 2:
            total = own + self.boxes[stage][0]
        else:
            total = jnp.zeros_like(own)
            for index in range(size):
                step = lax.rem(mine - index + size, size)
                term = self.boxes[stage][jnp.maximum(step - 1, 0)]
                total = total + jnp.where(step == 0, own, term)
        if stage == 3:
            self.out[...] = total
        else:
            self.value[stage + 1] = total


class ScatterPlan:
    def __init__(self, terms, vec, dims, n_tensor, chunk=256, every=8, depth=4):
        self.dims, self.n_tensor, self.has_total, self.depth = dims, n_tensor, vec is not None, depth
        n_a, n_b, n_c = dims
        tokens, width = terms[0][0].shape
        rows = width // (n_a * n_b * n_c)
        parts = [(1, right.shape[1] // n_tensor) for _, right in terms]
        chunk = min(chunk, *(cols for _, cols in parts))
        self.pieces = pieces_of(parts, chunk)
        self.part_cols = [cols for _, cols in parts]
        count, slots = len(self.pieces), Scatter.slots(dims, n_tensor)
        kinds = [0 if i % every else 1 for i in range(count)]
        self.places = [(k, kinds[:i].count(k)) for i, k in enumerate(kinds)]
        lefts = []
        self.left_at = []
        for left, _ in terms:
            known = [i for i, other in enumerate(lefts) if other is left]
            if not known:
                lefts.append(left)
            self.left_at.append(known[0] if known else len(lefts) - 1)
        self.n_left = len(lefts)
        self.args = lefts + [right for _, right in terms]
        self.in_specs = [VMEM] * len(lefts) + [ANY] * len(terms)
        self.out_shape = [jax.ShapeDtypeStruct((rows, cols), jnp.float32) for _, cols in parts]
        self.out_specs = [VMEM] * len(terms)
        bf, half = jnp.bfloat16, rows // 2
        self.scratch = [
            pltpu.VMEM((count, n_a, n_b, n_c, rows, chunk), bf),
            pltpu.VMEM((count, n_tensor - 1, n_a, n_b, n_c, rows, chunk), bf),
            pltpu.VMEM((self.SENDS, n_tensor - 1, n_a, n_b, n_c, rows, chunk), bf),
            pltpu.VMEM((2, n_tensor, tokens, chunk), bf),
            pltpu.VMEM((len(lefts), width, tokens), bf),
            pltpu.SemaphoreType.DMA((count, slots)),
            pltpu.SemaphoreType.DMA((count, slots)),
            pltpu.SemaphoreType.DMA((2, n_tensor)),
        ]
        for kind, orders in enumerate((Scatter.NORMAL, Scatter.EARLY)):
            for stage in (1, 2, 3):
                for order in orders:
                    left = [dims[x] for x in Scatter.left(order, stage)]
                    shape = (max(kinds.count(kind), 1), dims[order[stage - 1]] - 1, *left, half, chunk)
                    self.scratch.append(pltpu.VMEM(shape, bf))
        if self.has_total:
            self.args.append(vec)
            self.in_specs.append(VMEM)
            self.out_shape.append(jax.ShapeDtypeStruct(vec.shape, vec.dtype))
            self.out_specs.append(VMEM)
            self.scratch.append(pltpu.VMEM((4,) + vec.shape, vec.dtype))
            self.scratch += [pltpu.VMEM((k - 1,) + vec.shape, vec.dtype) for k in (n_tensor, n_c, n_b, n_a)]
            self.scratch += [pltpu.SemaphoreType.DMA((Total.slots(dims, n_tensor),))] * 2

    SENDS = 3

    def results(self, outs):
        return list(outs)

    def steps(self, ins, outs, scratch):
        place = Place(self.dims, self.n_tensor)
        held, near, sent, slabs, turned, send, recv, local = scratch[:8]
        chunks = []
        for i, (piece, (kind, at)) in enumerate(zip(self.pieces, self.places)):
            orders = (Scatter.NORMAL, Scatter.EARLY)[kind]
            boxes = scratch[8 + 6 * kind : 14 + 6 * kind]
            bufs = [[boxes[2 * stage + color].at[at] for color in (0, 1)] for stage in range(3)]
            chunks.append(
                Scatter(
                    place, piece, orders, turned.at[self.left_at[piece.source]], slabs.at[i % 2], outs[piece.source],
                    held.at[i], near.at[i], sent.at[i % self.SENDS], bufs, (send.at[i], recv.at[i]),
                )
            )
        count, depth = len(chunks), self.depth
        total = None
        if self.has_total:
            value, *rest = scratch[20:]
            total = Total(place, value, outs[-1], rest[:4], rest[4], rest[5])

        def loads(i):
            piece = self.pieces[i]
            right = ins[self.n_left + piece.source]
            for t in range(self.n_tensor):
                cols = pl.ds(t * self.part_cols[piece.source] + piece.first, piece.width)
                yield pltpu.make_async_copy(right.at[:, cols], slabs.at[i % 2, t], local.at[i % 2, t])

        def turn(number):
            block = 256

            def body(a, _):
                cols = pl.ds(pl.multiple_of(a * block, block), block)
                turned[number, cols, :] = ins[number][:, cols].T
                return 0

            lax.fori_loop(0, turned.shape[1] // block, body, 0)

        firsts = [next(i for i, p in enumerate(self.pieces) if self.left_at[p.source] == n) for n in range(self.n_left)]

        def begin():
            run_all(loads(0), "start")
            if total is not None:
                value[0] = ins[-1][...]
            place.barrier()
            if total is not None:
                run_all(total.copies(0), "start")

        def step(i):
            if i < count:
                run_all(loads(i), "wait")
                if i + 1 < count:
                    run_all(loads(i + 1), "start")
                if i >= self.SENDS:
                    run_all(chunks[i - self.SENDS].copies(0), "wait_send")
                for number, first in enumerate(firsts):
                    if first == i:
                        turn(number)
                chunks[i].compute()
            if 0 <= i - 1 < count:
                c = chunks[i - 1]
                run_all(c.copies(0), "wait_recv")
                c.add_tensor()
                run_all(c.copies(1), "start")
            for stage in (1, 2, 3):
                at = i - 1 - depth * stage
                if 0 <= at < count:
                    run_all(chunks[at].copies(stage), "wait_recv")
                    chunks[at].add(stage)
                    if stage < 3:
                        run_all(chunks[at].copies(stage + 1), "start")
            if total is not None and i < 4:
                run_all(total.copies(i), "wait_recv")
                total.add(i)
                if i < 3:
                    run_all(total.copies(i + 1), "start")

        def end():
            for i, c in enumerate(chunks):
                for stage in range(0 if i >= count - self.SENDS else 1, 4):
                    run_all(c.copies(stage), "wait_send")
            if total is not None:
                for stage in range(4):
                    run_all(total.copies(stage), "wait_send")

        last = max(count + 1 + 3 * depth, 4 if self.has_total else 0)
        return [begin] + [functools.partial(step, i) for i in range(last)] + [end]


def plan_kernel(plan, *refs):
    n_in, n_out = len(plan.in_specs), len(plan.out_specs)
    for step in plan.steps(refs[:n_in], refs[n_in : n_in + n_out], refs[n_in + n_out :]):
        step()


def run_plan(plan, collective_id, name):
    outs = pl.pallas_call(
        functools.partial(plan_kernel, plan),
        out_shape=plan.out_shape,
        in_specs=plan.in_specs,
        out_specs=plan.out_specs,
        scratch_shapes=plan.scratch,
        compiler_params=pltpu.CompilerParams(
            collective_id=collective_id, has_side_effects=True, vmem_limit_bytes=VMEM_LIMIT
        ),
        name=name,
    )(*plan.args)
    return plan.results(outs)


def exchange_kernel(dims, n_tensor, n, *refs):
    ins, outs = refs[:n], refs[n : 2 * n]
    send, recv, local = refs[2 * n :]
    place = Place(dims, n_tensor)

    def copies(i):
        for step in range(1, n_tensor):
            device, _ = place.peer(3, step)
            sems = (send.at[i, step - 1], recv.at[i, step - 1])
            yield remote(ins[i], outs[i].at[n_tensor - step], *sems, device)

    own = [pltpu.make_async_copy(ins[i], outs[i].at[0], local.at[i]) for i in range(n)]
    for copy in own:
        copy.start()
    place.barrier((3,))
    for i in range(n):
        for copy in copies(i):
            copy.start()
    for i in range(n):
        own[i].wait()
        for copy in copies(i):
            copy.wait()


def exchange_rows(arrays, dims, n_tensor, collective_id):
    n = len(arrays)
    outs = pl.pallas_call(
        functools.partial(exchange_kernel, dims, n_tensor, n),
        out_shape=[jax.ShapeDtypeStruct((n_tensor,) + a.shape, a.dtype) for a in arrays],
        in_specs=[VMEM] * n,
        out_specs=[ANY] * n,
        scratch_shapes=[
            pltpu.SemaphoreType.DMA((n, n_tensor - 1)),
            pltpu.SemaphoreType.DMA((n, n_tensor - 1)),
            pltpu.SemaphoreType.DMA((n,)),
        ],
        compiler_params=pltpu.CompilerParams(collective_id=collective_id, has_side_effects=True),
        name="exchange_rows",
    )(*arrays)
    return [o.reshape(-1, o.shape[-1]) for o in outs]


def return_kernel(dims, n_tensor, n, *refs):
    ins, outs, bufs = refs[:n], refs[n : 2 * n], refs[2 * n : 3 * n]
    send, recv = refs[3 * n :]
    place = Place(dims, n_tensor)
    rows = outs[0].shape[0]

    def copies(i):
        for step in range(1, n_tensor):
            device, _ = place.peer(3, step)
            sems = (send.at[i, step - 1], recv.at[i, step - 1])
            yield remote(ins[i].at[pl.ds(step * rows, rows), :], bufs[i].at[step - 1], *sems, device)

    place.barrier((3,))
    for i in range(n):
        for copy in copies(i):
            copy.start()
    for i in range(n):
        for copy in copies(i):
            copy.wait()
        for first in range(0, rows, 64):
            total = ins[i][first : first + 64, :].astype(jnp.float32)
            for step in range(1, n_tensor):
                total = total + bufs[i][step - 1, first : first + 64, :].astype(jnp.float32)
            outs[i][first : first + 64, :] = total.astype(outs[i].dtype)


def return_rows(arrays, dims, n_tensor, collective_id):
    n = len(arrays)
    rows, width = arrays[0].shape[0] // n_tensor, arrays[0].shape[1]
    return pl.pallas_call(
        functools.partial(return_kernel, dims, n_tensor, n),
        out_shape=[jax.ShapeDtypeStruct((rows, width), a.dtype) for a in arrays],
        in_specs=[VMEM] * n,
        out_specs=[VMEM] * n,
        scratch_shapes=[pltpu.VMEM((n_tensor - 1, rows, width), a.dtype) for a in arrays]
        + [pltpu.SemaphoreType.DMA((n, n_tensor - 1)), pltpu.SemaphoreType.DMA((n, n_tensor - 1))],
        compiler_params=pltpu.CompilerParams(collective_id=collective_id, has_side_effects=True),
        name="return_rows",
    )(*arrays)


def norm_forward(stream, gain_row, shift_row):
    centered = stream - jnp.mean(stream, axis=-1, keepdims=True)
    inv_std = lax.rsqrt(jnp.mean(centered * centered, axis=-1, keepdims=True) + EPSILON)
    normed = centered * inv_std
    return (normed * gain_row + shift_row, normed, inv_std)


def norm_backward(grad_result, normed, inv_std, gain_row):
    grad_normed = grad_result * gain_row
    return inv_std * (
        grad_normed
        - jnp.mean(grad_normed, axis=-1, keepdims=True)
        - normed * jnp.mean(grad_normed * normed, axis=-1, keepdims=True)
    )


def low(value):
    return value.astype(jnp.bfloat16)


def ffn_forward(entered, weight_in, weight_out_t):
    before = dot_nn(entered, weight_in)
    active = low(jax.nn.silu(before))
    return dot_nt(active, weight_out_t), (before, active)


def ffn_backward(entered, saved, grad_low, weight_in, weight_out_t):
    before, active = saved
    sigma = jax.nn.sigmoid(before)
    grad_active = dot_nn(grad_low, weight_out_t)
    grad_before = low(grad_active * sigma * (1.0 + before * (1.0 - sigma)))
    return dot_nt(grad_before, weight_in), [(grad_low, active), (entered, grad_before)]


def taps_forward(signal, before, conv_taps):
    rows = signal.shape[0]
    padded = jnp.concatenate([before, signal], axis=0)
    skip = before.shape[0] - (KERNEL - 1)
    result = jnp.zeros_like(signal)
    for tap in range(KERNEL):
        result = result + conv_taps[tap] * padded[skip + tap : skip + tap + rows]
    return result


def taps_backward(grad, after, signal, before, conv_taps):
    rows = signal.shape[0]
    padded_signal = jnp.concatenate([before, signal], axis=0)
    padded_grad = jnp.concatenate([grad, after], axis=0)
    skip = before.shape[0] - (KERNEL - 1)
    grad_signal = jnp.zeros_like(signal)
    taps = []
    for tap in range(KERNEL):
        back = KERNEL - 1 - tap
        grad_signal = grad_signal + conv_taps[tap] * padded_grad[back : back + rows]
        taps.append(jnp.sum(grad * padded_signal[skip + tap : skip + tap + rows], axis=0))
    return grad_signal, jnp.stack(taps)


HALO = 32


def on_device(
    dims,
    n_tensor,
    stream_in,
    grad_out,
    clip_lengths,
    first_up,
    first_down,
    attn_proj,
    attn_out,
    rel_table,
    glu_weight,
    conv_taps,
    conv_out,
    second_up,
    second_down,
    norm_gains,
    norm_shifts,
):
    rank = lax.axis_index("tensor")
    rows, width = stream_in.shape
    keys = rows * n_tensor
    early = [first_up[None], first_down.T[None], attn_proj, attn_out.T[None]]
    late = [glu_weight, conv_out.T[None], second_up[None], second_down.T[None]]
    def enter(stream, row):
        result, normed, inv_std = norm_forward(stream, norm_gains[row], norm_shifts[row])
        return low(result), (normed, inv_std)

    def norm_back(grad_result, saved, row):
        normed, inv_std = saved
        grad_input = norm_backward(grad_result, normed, inv_std, norm_gains[row])
        return grad_input, jnp.sum(grad_result * normed, axis=0), jnp.sum(grad_result, axis=0)

    def shift_rank(value, step):
        pairs = [(i, i + step) for i in range(n_tensor) if 0 <= i + step < n_tensor]
        return lax.ppermute(value, "tensor", pairs)

    stream = stream_in.astype(jnp.float32)
    entered_a, norm_a = enter(stream, 0)
    gathered = run_plan(FeedPlan(early, entered_a, dims, n_tensor), 0, "gather_weights")
    (up_one,), (down_one,), proj, (out_attn,), before_a, active_a, branch = gathered
    squares = []
    ffn_a = (before_a, active_a)
    squares.append(jnp.sum(branch * branch))
    stream = stream + 0.5 * branch

    entered_b, norm_b = enter(stream, 1)
    query, own_keys, own_vals = (low(dot_nn(entered_b, proj[i])) for i in range(3))
    key_rows, val_rows = exchange_rows([own_keys, own_vals], dims, n_tensor, 2)
    place = lax.rem(jnp.arange(keys, dtype=jnp.int32) + rank * rows, keys)
    mask = jnp.where(place < clip_lengths[0], 0.0, MASKED).astype(jnp.float32)[None]
    table = span_table(rel_table)
    attended, log_totals, gathered = attn_fwd(
        query, key_rows, val_rows, table, mask, GatherPlan(late, dims, n_tensor, *HOST_G), 4
    )
    glu, (out_conv,), (up_two,), (down_two,) = gathered
    branch = dot_nt(attended, out_attn)
    squares.append(jnp.sum(branch * branch))
    stream = stream + branch

    entered_c, norm_c = enter(stream, 2)
    glu_first = dot_nn(entered_c, glu[0])
    glu_second = dot_nn(entered_c, glu[1])
    sig_second = jax.nn.sigmoid(glu_second)
    gated = glu_first * sig_second
    gated_before = shift_rank(gated[rows - HALO :], 1)
    mixed = taps_forward(gated, gated_before, conv_taps)
    shaped, normed_mid, scale_mid = norm_forward(mixed, norm_gains[3], norm_shifts[3])
    conv_act = low(jax.nn.silu(shaped))
    branch = dot_nt(conv_act, out_conv)
    squares.append(jnp.sum(branch * branch))
    stream = stream + branch

    entered_d, norm_d = enter(stream, 4)
    branch, ffn_d = ffn_forward(entered_d, up_two, down_two)
    squares.append(jnp.sum(branch * branch))
    stream = stream + 0.5 * branch
    squares.append(jnp.sum(stream * stream))
    result, normed_e, scale_e = norm_forward(stream, norm_gains[5], norm_shifts[5])
    output = low(result)

    grad_stream, gain_e, shift_e = norm_back(grad_out.astype(jnp.float32), (normed_e, scale_e), 5)
    grad_low = low(0.5 * grad_stream)
    grad_entered, terms_two = ffn_backward(entered_d, ffn_d, grad_low, up_two, down_two)
    grad_extra, gain_d, shift_d = norm_back(grad_entered, norm_d, 4)
    grad_stream = grad_stream + grad_extra

    grad_low = low(grad_stream)
    terms_mid = [(grad_low, conv_act)]
    sigma = jax.nn.sigmoid(shaped)
    grad_shaped = dot_nn(grad_low, out_conv) * sigma * (1.0 + shaped * (1.0 - sigma))
    grad_mixed, gain_mid, shift_mid = norm_back(grad_shaped, (normed_mid, scale_mid), 3)
    grad_after = shift_rank(grad_mixed[:HALO], -1)
    grad_gated, taps_grad = taps_backward(grad_mixed, grad_after, gated, gated_before, conv_taps)
    grad_first = low(grad_gated * sig_second)
    grad_second = low(grad_gated * glu_first * sig_second * (1.0 - sig_second))
    terms_mid += [(entered_c, g) for g in (grad_first, grad_second)]
    grad_entered = dot_nt(grad_first, glu[0]) + dot_nt(grad_second, glu[1])
    grad_extra, gain_c, shift_c = norm_back(grad_entered, norm_c, 2)
    grad_stream = grad_stream + grad_extra

    grad_low = low(grad_stream)
    terms_attn = [(grad_low, attended)]
    grad_attended = low(dot_nn(grad_low, out_attn))
    grad_query, grad_keys, grad_vals, grad_span, summed = attn_bwd(
        query, key_rows, val_rows, grad_attended, attended, log_totals, table, mask,
        ScatterPlan(terms_two + terms_mid, None, dims, n_tensor, *HOST_S), 5,
    )
    s_down_two, s_up_two, s_conv, s_glu0, s_glu1 = summed
    grad_keys, grad_vals = return_rows([grad_keys, grad_vals], dims, n_tensor, 3)
    grad_parts = (grad_query, grad_keys, grad_vals)
    terms_attn += [(entered_b, g) for g in grad_parts]
    grad_entered = sum(dot_nt(g, proj[i]) for i, g in enumerate(grad_parts))
    grad_extra, gain_b, shift_b = norm_back(grad_entered, norm_b, 1)
    grad_stream = grad_stream + grad_extra

    grad_low = low(0.5 * grad_stream)
    grad_entered, terms_one = ffn_backward(entered_a, ffn_a, grad_low, up_one, down_one)
    grad_extra, gain_a, shift_a = norm_back(grad_entered, norm_a, 0)
    grad_stream = grad_stream + grad_extra

    span_grad = fold_table(grad_span)
    span_rows = -(-span_grad.size // width)
    table_rows = jnp.pad(span_grad.reshape(-1), (0, span_rows * width - span_grad.size)).reshape(span_rows, width)
    square_row = jnp.pad(jnp.stack(squares), (0, width - len(squares)))[None]
    parts = [
        jnp.stack([gain_a, gain_b, gain_c, gain_mid, gain_d, gain_e]),
        jnp.stack([shift_a, shift_b, shift_c, shift_mid, shift_d, shift_e]),
        taps_grad,
        table_rows,
        square_row,
    ]
    vec = jnp.concatenate(parts, axis=0)
    vec = jnp.pad(vec, ((0, -vec.shape[0] % 8), (0, 0)))
    *summed, vec = run_plan(ScatterPlan(terms_attn + terms_one, vec, dims, n_tensor), 1, "scatter_grads")
    s_attn, s_q, s_k, s_v, s_down_one, s_up_one = summed
    at = 0
    pieces = []
    for part in parts:
        pieces.append(vec[at : at + part.shape[0]])
        at += part.shape[0]
    gains_sum, shifts_sum, taps_sum, table_sum, square_sum = pieces
    table_sum = table_sum.reshape(-1)[: span_grad.size].reshape(span_grad.shape)
    count_all = float(lax.axis_size("dp") * keys * width)
    rms_values = jnp.sqrt(square_sum[0, : len(squares)] / count_all)
    return (
        output,
        grad_stream,
        s_up_one,
        s_down_one.T,
        jnp.stack([s_q, s_k, s_v]),
        s_attn.T,
        table_sum,
        jnp.stack([s_glu0, s_glu1]),
        taps_sum,
        s_conv.T,
        s_up_two,
        s_down_two.T,
        gains_sum,
        shifts_sum,
        rms_values,
    )


def solution(mesh):
    n_dp, n_tensor = mesh.shape["dp"], mesh.shape["tensor"]
    dims = FACTORS.get(n_dp, (n_dp, 1, 1))
    return jax.shard_map(
        functools.partial(on_device, dims, n_tensor),
        mesh=mesh,
        in_specs=(
            P(("dp", "tensor"), None),
            P(("dp", "tensor"), None),
            P("dp"),
            P("dp", "tensor"),
            P("tensor", "dp"),
            P(None, "dp", "tensor"),
            P("tensor", "dp"),
            P(),
            P(None, "dp", "tensor"),
            P(),
            P("tensor", "dp"),
            P("dp", "tensor"),
            P("tensor", "dp"),
            P(),
            P(),
        ),
        out_specs=(
            P(("dp", "tensor"), None),
            P(("dp", "tensor"), None),
            P("dp", "tensor"),
            P("tensor", "dp"),
            P(None, "dp", "tensor"),
            P("tensor", "dp"),
            P(),
            P(None, "dp", "tensor"),
            P(),
            P("tensor", "dp"),
            P("dp", "tensor"),
            P("tensor", "dp"),
            P(),
            P(),
            P(),
        ),
        check_vma=False,
    )
```

```python
import functools

import jax
import jax.numpy as jnp
from jax import lax
from jax.experimental import pallas as pl
from jax.experimental.pallas import tpu as pltpu
from jax.sharding import PartitionSpec as P

HEAD = 64
KERNEL = 31
LEFT = 64
RIGHT = 8
EPSILON = 1e-05
MASKED = -1e30
VMEM_LIMIT = 66_000_000
HOST_G = (512, 6, 5)
HOST_S = (256, 8, 4)
BLK = 128
SPAN = 512
NT = (((1,), (1,)), ((), ()))
TN = (((0,), (0,)), ((), ()))


def dot_nt(a, b):
    return lax.dot_general(a, b, NT, preferred_element_type=jnp.float32)


def dot_tn(a, b):
    return lax.dot_general(a, b, TN, preferred_element_type=jnp.float32)


def dot_nn(a, b):
    return jnp.dot(a, b, preferred_element_type=jnp.float32)


def rel_blocks(tin, b, own_blocks, key_blocks, rank):
    t_left, t_right = tin[:, 0:1], tin[:, SPAN - 1 : SPAN]
    band = pltpu.roll(tin, SPAN - BLK, 1, stride=1, stride_axis=0)
    out = []
    for kb in range(key_blocks):
        wraps = rank * own_blocks + kb >= key_blocks
        if kb in (b - 1, b) or (kb == b + 1 and kb < own_blocks):
            out.append(band[:, (kb - b + 1) * BLK : (kb - b + 2) * BLK])
        elif kb == b + 1:
            out.append(jnp.where(wraps, t_left, band[:, 2 * BLK : 3 * BLK]))
        elif b == 0 and kb == key_blocks - 1:
            out.append(jnp.where(wraps, band[:, :BLK], t_right))
        elif kb < b - 1:
            out.append(t_left)
        elif kb < own_blocks:
            out.append(t_right)
        else:
            out.append(jnp.where(wraps, t_left, t_right))
    return out


def halves(x):
    low = lax.broadcasted_iota(jnp.int32, x.shape, 1) < HEAD
    zero = jnp.zeros_like(x)
    return jnp.where(low, x, zero), jnp.where(low, zero, x)


def flip_rows(x):
    tiles = []
    back = 7 - lax.broadcasted_iota(jnp.int32, (8, BLK), 0)
    for first in range(x.shape[0] - 8, -1, -8):
        cols = [
            jnp.take_along_axis(x[first : first + 8, c : c + BLK], back, axis=0, mode="promise_in_bounds")
            for c in range(0, x.shape[1], BLK)
        ]
        tiles.append(jnp.concatenate(cols, axis=1) if len(cols) > 1 else cols[0])
    return jnp.concatenate(tiles, axis=0)


def split_refs(refs, sizes):
    out, at = [], 0
    for size in sizes:
        out.append(refs[at : at + size])
        at += size
    return out


def ticker(plan, ins, outs, scratch, ticks):
    if plan is None:
        return lambda block, blocks: None
    steps = plan.steps(ins, outs, scratch)

    def tick(block, blocks):
        for number, step in enumerate(steps):
            at = min(number * ticks // (len(steps) - 1), ticks - 1) if number < len(steps) - 1 else ticks
            if at < ticks and at % blocks == block:
                pl.when(pl.program_id(0) == at // blocks)(step)
            if at == ticks and block == blocks:
                pl.when(pl.program_id(0) == ticks // blocks - 1)(step)

    return tick


def attn_fwd_kernel(plan, *refs):
    n_in, n_out = (len(plan.in_specs), len(plan.out_specs)) if plan else (0, 0)
    own, plan_in, (o_ref, lse_ref), plan_out, plan_scratch = split_refs(refs, (5, n_in, 2, n_out, len(refs)))
    q_ref, k_ref, v_ref, tab_ref, mask_ref = own
    rank = lax.axis_index("tensor")
    rows, keys = q_ref.shape[0], k_ref.shape[0]
    own_blocks, key_blocks = rows // BLK, keys // BLK
    low = lax.broadcasted_iota(jnp.int32, (BLK, 2 * HEAD), 1) < HEAD
    tick = ticker(plan, plan_in, plan_out, plan_scratch, own_blocks * pl.num_programs(0))
    for b in range(own_blocks):
        tick(b, own_blocks)
        q_blk = q_ref[b * BLK : (b + 1) * BLK, :] * jnp.asarray(HEAD**-0.5, jnp.bfloat16)
        results = []
        for hh, q_one in enumerate(halves(q_blk)):
            tin = dot_nt(q_one, tab_ref[...])
            rel = rel_blocks(tin, b, own_blocks, key_blocks, rank)
            raw = dot_nt(q_one, k_ref[...])
            s = [
                raw[:, kb * BLK : (kb + 1) * BLK] + rel[kb] + mask_ref[:, kb * BLK : (kb + 1) * BLK]
                for kb in range(key_blocks)
            ]
            s = jnp.concatenate(s, axis=1)
            peak = jnp.max(s, axis=-1, keepdims=True)
            e = jnp.exp(s - peak)
            total = jnp.sum(e, axis=-1, keepdims=True)
            o = dot_nn(e.astype(jnp.bfloat16), v_ref[...])
            results.append(o / total)
            first = (hh * own_blocks + b) * BLK
            lse_ref[0, first : first + BLK, :] = peak + jnp.log(total)
        o_ref[b * BLK : (b + 1) * BLK, :] = jnp.where(low, results[0], results[1]).astype(jnp.bfloat16)
    tick(own_blocks, own_blocks)


def attn_fwd(q, k, v, tab2, mask, plan=None, collective_id=None):
    rows, width = q.shape
    keys = k.shape[0]
    pairs = width // (2 * HEAD)
    col = lambda n: pl.BlockSpec((n, 2 * HEAD), lambda p: (0, p))
    out_specs = [col(rows), pl.BlockSpec((1, 2 * rows, 1), lambda p: (p, 0, 0))]
    out_shape = [
        jax.ShapeDtypeStruct((rows, width), jnp.bfloat16),
        jax.ShapeDtypeStruct((pairs, 2 * rows, 1), jnp.float32),
    ]
    outs = pl.pallas_call(
        functools.partial(attn_fwd_kernel, plan),
        grid=(pairs,),
        in_specs=[
            col(rows),
            col(keys),
            col(keys),
            pl.BlockSpec((SPAN, 2 * HEAD), lambda p: (0, 0)),
            pl.BlockSpec((1, keys), lambda p: (0, 0)),
        ]
        + (plan.in_specs if plan else []),
        out_specs=out_specs + (plan.out_specs if plan else []),
        out_shape=out_shape + (plan.out_shape if plan else []),
        scratch_shapes=plan.scratch if plan else [],
        compiler_params=pltpu.CompilerParams(
            collective_id=collective_id, has_side_effects=plan is not None, vmem_limit_bytes=VMEM_LIMIT
        ),
        name="attn_fwd",
    )(q, k, v, tab2, mask, *(plan.args if plan else []))
    return outs[0], outs[1], plan.results(outs[2:]) if plan else []


def attn_bwd_kernel(plan, *refs):
    n_in, n_out = (len(plan.in_specs), len(plan.out_specs)) if plan else (0, 0)
    own, plan_in, own_out, plan_out, own_scratch, plan_scratch = split_refs(refs, (8, n_in, 4, n_out, 4, len(refs)))
    q_ref, k_ref, v_ref, do_ref, o_ref, lse_ref, tab_ref, mask_ref = own
    dq_ref, dk_ref, dv_ref, dtab_ref = own_out
    p_sc, ds_sc, q_sc, do_sc = own_scratch
    rank = lax.axis_index("tensor")
    rows, keys = q_ref.shape[0], k_ref.shape[0]
    own_blocks, key_blocks = rows // BLK, keys // BLK
    low = lax.broadcasted_iota(jnp.int32, (BLK, 2 * HEAD), 1) < HEAD
    lane = lax.broadcasted_iota(jnp.int32, (BLK, BLK), 1)
    scale = jnp.asarray(HEAD**-0.5, jnp.bfloat16)

    @pl.when(pl.program_id(0) == 0)
    def _():
        dtab_ref[...] = jnp.zeros_like(dtab_ref)

    tick = ticker(plan, plan_in, plan_out, plan_scratch, own_blocks * pl.num_programs(0))
    for b in range(own_blocks):
        tick(b, own_blocks)
        at = slice(b * BLK, (b + 1) * BLK)
        q_blk = q_ref[at, :] * scale
        do_blk = do_ref[at, :]
        prod = do_blk.astype(jnp.float32) * o_ref[at, :].astype(jnp.float32)
        q_back = halves(flip_rows(q_blk.astype(jnp.float32)).astype(jnp.bfloat16))
        results = []
        for hh, (q_one, do_one, pr_one) in enumerate(zip(halves(q_blk), halves(do_blk), halves(prod))):
            first = (hh * own_blocks + b) * BLK
            here = slice(first, first + BLK)
            inner = jnp.sum(pr_one, axis=-1, keepdims=True)
            lse = lse_ref[0, here, :]
            tin = dot_nt(q_one, tab_ref[...])
            rel = rel_blocks(tin - lse, b, own_blocks, key_blocks, rank)
            raw = dot_nt(q_one, k_ref[...])
            dp = dot_nt(do_one, v_ref[...])
            left = jnp.zeros((BLK, BLK), jnp.float32)
            right = jnp.zeros((BLK, BLK), jnp.float32)
            window = [None, None, None]
            for kb in range(key_blocks):
                ks = slice(kb * BLK, (kb + 1) * BLK)
                p = jnp.exp(raw[:, ks] + rel[kb] + mask_ref[:, ks])
                ds = (p * (dp[:, ks] - inner)).astype(jnp.bfloat16)
                p_sc[here, ks] = p.astype(jnp.bfloat16)
                ds_sc[here, ks] = ds
                ds = ds.astype(jnp.float32)
                wraps = rank * own_blocks + kb >= key_blocks
                zero = jnp.zeros_like(ds)
                if kb in (b - 1, b) or (kb == b + 1 and kb < own_blocks):
                    window[kb - b + 1] = ds
                elif kb == b + 1:
                    window[2] = jnp.where(wraps, zero, ds)
                    left = left + jnp.where(wraps, ds, zero)
                elif b == 0 and kb == key_blocks - 1:
                    window[0] = jnp.where(wraps, ds, zero)
                    right = right + jnp.where(wraps, zero, ds)
                elif kb < b - 1:
                    left = left + ds
                elif kb < own_blocks:
                    right = right + ds
                else:
                    left = left + jnp.where(wraps, ds, zero)
                    right = right + jnp.where(wraps, zero, ds)
            none = jnp.zeros((BLK, BLK), jnp.float32)
            window = jnp.concatenate([none if w is None else flip_rows(w) for w in window] + [none], axis=1)
            back = pltpu.roll(window, 1, 1, stride=1, stride_axis=0)
            s_left = flip_rows(jnp.broadcast_to(jnp.sum(left, axis=-1, keepdims=True), (BLK, BLK)))
            s_right = flip_rows(jnp.broadcast_to(jnp.sum(right, axis=-1, keepdims=True), (BLK, BLK)))
            u = jnp.concatenate(
                [
                    back[:, :BLK] + jnp.where(lane == 0, s_left, 0.0),
                    back[:, BLK : 3 * BLK],
                    back[:, 3 * BLK :] + jnp.where(lane == BLK - 1, s_right, 0.0),
                ],
                axis=1,
            ).astype(jnp.bfloat16)
            q_sc[here, :] = q_one
            do_sc[here, :] = do_one
            dtab_ref[...] += dot_tn(u, q_back[hh])
            results.append(dot_nn(ds_sc[here, :], k_ref[...]) + flip_rows(dot_nn(u, tab_ref[...])))
        dq_ref[at, :] = (jnp.where(low, results[0], results[1]) * HEAD**-0.5).astype(jnp.bfloat16)
    dk_ref[...] = dot_tn(ds_sc[...], q_sc[...]).astype(dk_ref.dtype)
    dv_ref[...] = dot_tn(p_sc[...], do_sc[...]).astype(dv_ref.dtype)
    tick(own_blocks, own_blocks)


def attn_bwd(q, k, v, do, o, lse, tab2, mask, plan=None, collective_id=None):
    rows, width = q.shape
    keys = k.shape[0]
    pairs = width // (2 * HEAD)
    col = lambda n: pl.BlockSpec((n, 2 * HEAD), lambda p: (0, p))
    table = pl.BlockSpec((SPAN, 2 * HEAD), lambda p: (0, 0))
    out_shape = [
        jax.ShapeDtypeStruct((rows, width), jnp.bfloat16),
        jax.ShapeDtypeStruct((keys, width), jnp.bfloat16),
        jax.ShapeDtypeStruct((keys, width), jnp.bfloat16),
        jax.ShapeDtypeStruct((SPAN, 2 * HEAD), jnp.float32),
    ]
    outs = pl.pallas_call(
        functools.partial(attn_bwd_kernel, plan),
        grid=(pairs,),
        in_specs=[
            col(rows),
            col(keys),
            col(keys),
            col(rows),
            col(rows),
            pl.BlockSpec((1, 2 * rows, 1), lambda p: (p, 0, 0)),
            table,
            pl.BlockSpec((1, keys), lambda p: (0, 0)),
        ]
        + (plan.in_specs if plan else []),
        out_specs=[col(rows), col(keys), col(keys), table] + (plan.out_specs if plan else []),
        out_shape=out_shape + (plan.out_shape if plan else []),
        scratch_shapes=[
            pltpu.VMEM((2 * rows, keys), jnp.bfloat16),
            pltpu.VMEM((2 * rows, keys), jnp.bfloat16),
            pltpu.VMEM((2 * rows, 2 * HEAD), jnp.bfloat16),
            pltpu.VMEM((2 * rows, 2 * HEAD), jnp.bfloat16),
        ]
        + (plan.scratch if plan else []),
        compiler_params=pltpu.CompilerParams(
            collective_id=collective_id, has_side_effects=plan is not None, vmem_limit_bytes=VMEM_LIMIT
        ),
        name="attn_bwd",
    )(q, k, v, do, o, lse, tab2, mask, *(plan.args if plan else []))
    return (*outs[:4], plan.results(outs[4:]) if plan else [])


def span_table(rel_table):
    rows = jnp.clip(jnp.arange(SPAN) - SPAN // 2, -LEFT, RIGHT) + LEFT
    table = jnp.take(rel_table, rows, axis=0)
    return jnp.concatenate([table, table], axis=1)


def fold_table(dtab):
    one = dtab[:, :HEAD] + dtab[:, HEAD:]
    rows = jnp.clip(jnp.arange(SPAN) - SPAN // 2, -LEFT, RIGHT) + LEFT
    pick = (rows[None, :] == jnp.arange(LEFT + RIGHT + 1)[:, None]).astype(jnp.float32)
    return jnp.dot(pick, one, precision=lax.Precision.HIGHEST)


MESH = pl.DeviceIdType.MESH
ANY = pl.BlockSpec(memory_space=pl.ANY)
VMEM = pl.BlockSpec(memory_space=pltpu.VMEM)
FACTORS = {16: (4, 2, 2), 32: (4, 2, 4)}


class Place:
    def __init__(self, dims, n_tensor):
        self.dims, self.n_tensor = dims, n_tensor
        n_a, n_b, n_c = dims
        d = lax.axis_index("dp")
        self.t = lax.axis_index("tensor")
        self.at = (lax.div(d, n_b * n_c), lax.rem(lax.div(d, n_c), n_b), lax.rem(d, n_c))

    def peer(self, axis, step):
        at, t = list(self.at), self.t
        if axis == 3:
            t = lax.rem(t + step, self.n_tensor)
            index = t
        else:
            at[axis] = index = lax.rem(at[axis] + step, self.dims[axis])
        n_a, n_b, n_c = self.dims
        return ((at[0] * n_b + at[1]) * n_c + at[2], t), index

    def size(self, axis):
        return self.n_tensor if axis == 3 else self.dims[axis]

    def barrier(self, axes=(0, 1, 2, 3)):
        sem = pltpu.get_barrier_semaphore()
        count = 0
        for axis in axes:
            for step in range(1, self.size(axis)):
                pl.semaphore_signal(sem, inc=1, device_id=self.peer(axis, step)[0], device_id_type=MESH)
                count += 1
        pl.semaphore_wait(sem, count)


def remote(src, dst, send_sem, recv_sem, device):
    return pltpu.make_async_remote_copy(
        src_ref=src, dst_ref=dst, send_sem=send_sem, recv_sem=recv_sem, device_id=device, device_id_type=MESH
    )


class Piece:
    def __init__(self, source, lead, first, width):
        self.source, self.lead, self.first, self.width = source, lead, first, width


def pieces_of(parts, chunk):
    return [
        Piece(source, lead, first, min(chunk, cols - first))
        for source, (n, cols) in enumerate(parts)
        for lead in range(n)
        for first in range(0, cols, chunk)
    ]


def run_all(copies, action):
    for copy in copies:
        getattr(copy, action)()


class Gather:
    NORMAL = ((0, 1, 2), (0, 2, 1))
    EARLY = ((2, 1, 0), (1, 2, 0))

    def __init__(self, place, piece, orders, shard, whole, send, recv, local):
        self.place, self.piece, self.orders = place, piece, orders
        self.shard, self.whole = shard, whole
        self.send, self.recv, self.local = send, recv, local
        self.half = shard.shape[1] // 2

    @staticmethod
    def slots(dims, n_tensor):
        return 2 * (sum(d - 1 for d in dims) + 2 * (n_tensor - 1))

    def slot(self, color, stage, step):
        place, order = self.place, self.orders[color]
        sizes = [place.dims[x] - 1 for x in order] + [place.n_tensor - 1] * 2
        return color * sum(sizes) + sum(sizes[:stage]) + step - 1

    def columns(self, t):
        piece = self.piece
        return pl.ds(pl.multiple_of(t * self.shard.shape[2] + piece.first, 128), piece.width)

    def region(self, color, index, t):
        rows = pl.ds(color * self.half, self.half)
        return self.whole.at[(self.piece.lead,) + tuple(index) + (rows, self.columns(t))]

    def source(self, rows):
        piece = self.piece
        return self.shard.at[piece.lead, rows, pl.ds(piece.first, piece.width)]

    def index(self, color, stage, moved=None):
        order, out = self.orders[color], list(self.place.at)
        for axis in order[:stage]:
            out[axis] = slice(None)
        if moved is not None:
            out[order[stage]] = moved
        return out

    def own(self):
        there = self.whole.at[(self.piece.lead,) + self.place.at + (slice(None), self.columns(self.place.t))]
        return pltpu.make_async_copy(self.source(slice(None)), there, self.local)

    def copies(self, stage, arriving=False):
        place, t = self.place, self.place.t
        for color, order in enumerate(self.orders):
            in_one = place.dims[order[2]] > 2
            if stage == 3 and in_one:
                continue
            axis = order[stage] if stage < 3 else 3
            for step in range(1, place.size(axis)):
                device, _ = place.peer(axis, step)
                _, origin = place.peer(axis, place.size(axis) - step)
                slot = self.slot(color, stage, step)
                if stage < 3:
                    index, there, then = self.index(color, stage), self.index(color, stage, origin), t
                else:
                    if in_one:
                        index = self.index(color, 3)
                    elif stage == 3:
                        index = self.index(color, 2)
                    else:
                        index = self.index(color, 2, place.peer(order[2], 1)[1])
                    there, then = index, origin
                mine, theirs = self.region(color, index, t), self.region(color, there, then)
                origin_ref = self.source(pl.ds(color * self.half, self.half)) if stage == 0 else mine
                sems = (self.send.at[slot], self.recv.at[slot], device)
                yield remote(theirs, theirs, *sems) if arriving else remote(origin_ref, mine, *sems)

    def start(self, stage):
        run_all(self.copies(stage), "start")

    def arrived(self, stage):
        run_all(self.copies(stage, arriving=True), "wait_recv")

    def sent(self, stage):
        run_all(self.copies(stage), "wait_send")


class GatherPlan:
    def __init__(self, shards, dims, n_tensor, chunk=1024, every=6, depth=3):
        self.dims, self.n_tensor, self.depth = dims, n_tensor, depth
        self.args = list(shards)
        self.pieces = pieces_of([(s.shape[0], s.shape[2]) for s in shards], chunk)
        self.orders = [Gather.EARLY if i % every == 0 else Gather.NORMAL for i in range(len(self.pieces))]
        count, slots = len(self.pieces), Gather.slots(dims, n_tensor)
        self.in_specs = [VMEM] * len(shards)
        self.out_specs = [ANY] * len(shards)
        self.out_shape = [
            jax.ShapeDtypeStruct((s.shape[0], *dims, s.shape[1], n_tensor * s.shape[2]), s.dtype) for s in shards
        ]
        self.scratch = [
            pltpu.SemaphoreType.DMA((count, slots)),
            pltpu.SemaphoreType.DMA((count, slots)),
            pltpu.SemaphoreType.DMA((count,)),
        ]

    def results(self, outs):
        return [o.reshape(o.shape[0], -1, o.shape[-1]) for o in outs]

    def steps(self, shards, wholes, scratch):
        send, recv, local = scratch
        place = Place(self.dims, self.n_tensor)
        gathers = [
            Gather(place, p, orders, shards[p.source], wholes[p.source], send.at[i], recv.at[i], local.at[i])
            for i, (p, orders) in enumerate(zip(self.pieces, self.orders))
        ]
        return self.steps_of(place, gathers)

    def steps_of(self, place, gathers, read=()):
        count, depth = len(gathers), self.depth

        def begin():
            for g in gathers:
                g.own().start()
            place.barrier()
            for g in gathers:
                g.start(0)
            for g in gathers:
                g.own().wait()

        def step(i):
            if i < count:
                gathers[i].arrived(0)
                gathers[i].start(1)
            at = i - depth
            if 0 <= at < count:
                gathers[at].arrived(1)
                gathers[at].start(2)
                gathers[at].start(3)
            at = i - 2 * depth
            if 0 <= at < count:
                gathers[at].arrived(2)
                gathers[at].start(4)

        def end():
            for i, g in enumerate(gathers):
                if i not in read:
                    g.arrived(3)
                    g.arrived(4)
                for stage in range(5):
                    g.sent(stage)

        return [begin] + [functools.partial(step, i) for i in range(count + 2 * depth)] + [end]


class FeedPlan(GatherPlan):
    TILE = 512

    def __init__(self, shards, entered, dims, n_tensor):
        super().__init__(shards, dims, n_tensor)
        tokens, width = entered.shape
        cols = shards[0].shape[2]
        hidden = cols * n_tensor
        fed = sorted((p for p in self.pieces if p.source < 2), key=lambda p: (p.first, p.source))
        self.pieces = fed + [p for p in self.pieces if p.source >= 2]
        self.pairs = len(fed) // 2
        self.tile = tile = min(self.TILE, fed[0].width)
        self.args = self.args + [entered]
        self.in_specs = self.in_specs + [VMEM]
        self.out_specs = self.out_specs + [ANY, ANY, VMEM]
        self.out_shape = self.out_shape + [
            jax.ShapeDtypeStruct((tokens, hidden), jnp.float32),
            jax.ShapeDtypeStruct((tokens, hidden), jnp.bfloat16),
            jax.ShapeDtypeStruct((tokens, width), jnp.float32),
        ]
        rows = shards[0].shape[1]
        self.scratch = self.scratch + [
            pltpu.VMEM((2, 2, *dims, rows, tile), jnp.bfloat16),
            pltpu.VMEM((2, tokens, tile), jnp.float32),
            pltpu.VMEM((2, tokens, tile), jnp.bfloat16),
            pltpu.SemaphoreType.DMA((2, 2)),
            pltpu.SemaphoreType.DMA((2, 2)),
        ]

    def results(self, outs):
        return super().results(outs[:-3]) + list(outs[-3:])

    def steps(self, ins, outs, scratch):
        send, recv, local, weights, pre_st, act_st, load_sem, store_sem = scratch
        place = Place(self.dims, self.n_tensor)
        shards, entered = ins[:-1], ins[-1]
        wholes, (before, active, branch) = outs[:-3], outs[-3:]
        gathers = [
            Gather(place, p, orders, shards[p.source], wholes[p.source], send.at[i], recv.at[i], local.at[i])
            for i, (p, orders) in enumerate(zip(self.pieces, self.orders))
        ]
        steps = self.steps_of(place, gathers, range(2 * self.pairs))
        tile, tokens, width = self.tile, entered.shape[0], entered.shape[1]
        tiles = [
            (pair, t * shards[0].shape[2] + self.pieces[2 * pair].first + sub * tile)
            for pair in range(self.pairs)
            for t in range(self.n_tensor)
            for sub in range(self.pieces[2 * pair].width // tile)
        ]

        def loads(number):
            cols = pl.ds(tiles[number][1], tile)
            for k in (0, 1):
                origin = wholes[k].at[0, :, :, :, :, cols]
                yield pltpu.make_async_copy(origin, weights.at[number % 2, k], load_sem.at[number % 2, k])

        def stores(number):
            cols, slot = pl.ds(tiles[number][1], tile), number % 2
            yield pltpu.make_async_copy(pre_st.at[slot], before.at[:, cols], store_sem.at[slot, 0])
            yield pltpu.make_async_copy(act_st.at[slot], active.at[:, cols], store_sem.at[slot, 1])

        def feed(number):
            slot, pair = number % 2, tiles[number][0]
            if number == 0 or tiles[number - 1][0] != pair:
                for g in gathers[2 * pair : 2 * pair + 2]:
                    g.arrived(3)
                    g.arrived(4)
                run_all(loads(number), "start")
            run_all(loads(number), "wait")
            if number + 1 < len(tiles) and tiles[number + 1][0] == pair:
                run_all(loads(number + 1), "start")
            if number >= 2:
                run_all(stores(number - 2), "wait")
            up = weights[slot, 0].reshape(width, tile)
            pre = dot_nn(entered[...], up)
            pre_st[slot] = pre
            act = low(jax.nn.silu(pre))
            act_st[slot] = act
            run_all(stores(number), "start")
            added = dot_nt(act, weights[slot, 1].reshape(width, tile))
            branch[...] = added if number == 0 else branch[...] + added
            if number == len(tiles) - 1:
                for last in range(max(number - 1, 0), number + 1):
                    run_all(stores(last), "wait")

        first = [2 * pair + 2 + 2 * self.depth + 1 for pair in range(self.pairs)]
        out, at = [], 0
        for number, step in enumerate(steps[:-1]):
            out.append(step)
            rest = len(steps) - 2 - number
            room = -(-(len(tiles) - at) // max(rest + 1, 1)) if number > first[0] else 0
            while room and at < len(tiles) and number > first[tiles[at][0]]:
                out.append(functools.partial(feed, at))
                at, room = at + 1, room - 1
        out += [functools.partial(feed, k) for k in range(at, len(tiles))]
        return out + steps[-1:]


class Scatter:
    NORMAL = ((2, 1, 0), (1, 2, 0))
    EARLY = ((0, 1, 2), (0, 2, 1))

    def __init__(self, place, piece, orders, left_op, slabs, out, held, near, sent, bufs, sems):
        self.place, self.piece, self.orders = place, piece, orders
        self.left_op, self.slabs, self.out = left_op, slabs, out
        self.held, self.near, self.sent, self.bufs = held, near, sent, bufs
        self.send, self.recv = sems
        self.half = held.shape[3] // 2

    @staticmethod
    def slots(dims, n_tensor):
        return n_tensor - 1 + 2 * sum(d - 1 for d in dims)

    @staticmethod
    def left(order, stage):
        return [x for x in (0, 1, 2) if x not in order[:stage]]

    def product(self, t, target):
        n_a, n_b, n_c = self.place.dims
        rows = self.held.shape[3]
        block = n_b * n_c * rows

        def body(a, _):
            lhs = self.left_op[pl.ds(pl.multiple_of(a * block, block), block), :]
            value = dot_nn(lhs, self.slabs[t]).astype(jnp.bfloat16)
            target[a] = value.reshape(n_b, n_c, rows, value.shape[-1])
            return 0

        lax.fori_loop(0, n_a, body, 0)

    def compute(self):
        for step, copy in enumerate(self.copies(0)):
            self.product(self.place.peer(3, step + 1)[1], self.sent.at[step])
            copy.start()
        self.product(self.place.t, self.held)

    def copies(self, stage):
        place = self.place
        if stage == 0:
            for step in range(1, place.n_tensor):
                sems = (self.send.at[step - 1], self.recv.at[step - 1], place.peer(3, step)[0])
                yield remote(self.sent.at[step - 1], self.near.at[step - 1], *sems)
            return
        base = place.n_tensor - 1
        for color, order in enumerate(self.orders):
            axis = order[stage - 1]
            for step in range(1, place.size(axis)):
                device, there = place.peer(axis, step)
                index = [slice(None)] * 3
                for done in order[: stage - 1]:
                    index[done] = place.at[done]
                index[axis] = there
                slot = base + color * sum(d - 1 for d in place.dims)
                slot += sum(place.size(x) - 1 for x in order[: stage - 1]) + step - 1
                origin = self.held.at[tuple(index) + (pl.ds(color * self.half, self.half),)]
                sems = (self.send.at[slot], self.recv.at[slot], device)
                yield remote(origin, self.bufs[stage - 1][color].at[step - 1], *sems)

    def add_tensor(self):
        def body(a, _):
            total = self.held[a].astype(jnp.float32)
            for step in range(1, self.place.n_tensor):
                total = total + self.near[step - 1, a].astype(jnp.float32)
            self.held[a] = total.astype(jnp.bfloat16)
            return 0

        lax.fori_loop(0, self.place.dims[0], body, 0)

    def add(self, stage):
        place, piece = self.place, self.piece
        for color, order in enumerate(self.orders):
            rows = slice(color * self.half, (color + 1) * self.half)
            left = self.left(order, stage)
            buf = self.bufs[stage - 1][color]

            def total_at(where):
                at = list(place.at)
                for x, w in zip(left, where):
                    at[x] = w
                at = tuple(at) + (rows,)
                total = self.held[at].astype(jnp.float32)
                for step in range(1, place.size(order[stage - 1])):
                    total = total + buf[(step - 1,) + where].astype(jnp.float32)
                return at, total

            def body(i, _):
                at, total = total_at((i, slice(None)))
                self.held[at] = total.astype(jnp.bfloat16)
                return 0

            if len(left) == 2:
                lax.fori_loop(0, place.dims[left[0]], body, 0)
            elif left:
                at, total = total_at((slice(None),))
                self.held[at] = total.astype(jnp.bfloat16)
            else:
                cols = slice(piece.first, piece.first + piece.width)
                self.out[rows, cols] = total_at(())[1]


class Total:
    AXES = (3, 2, 1, 0)

    def __init__(self, place, value, out, boxes, send, recv):
        self.place, self.value, self.out, self.boxes, self.send, self.recv = place, value, out, boxes, send, recv

    @staticmethod
    def slots(dims, n_tensor):
        return sum(dims) + n_tensor - 4

    def copies(self, stage):
        place, axis = self.place, self.AXES[stage]
        base = sum(place.size(x) - 1 for x in self.AXES[:stage])
        for step in range(1, place.size(axis)):
            device, _ = place.peer(axis, step)
            sems = (self.send.at[base + step - 1], self.recv.at[base + step - 1], device)
            yield remote(self.value.at[stage], self.boxes[stage].at[step - 1], *sems)

    def add(self, stage):
        place, axis = self.place, self.AXES[stage]
        size = place.size(axis)
        mine = place.t if axis == 3 else place.at[axis]
        own = self.value[stage]
        if size == 2:
            total = own + self.boxes[stage][0]
        else:
            total = jnp.zeros_like(own)
            for index in range(size):
                step = lax.rem(mine - index + size, size)
                term = self.boxes[stage][jnp.maximum(step - 1, 0)]
                total = total + jnp.where(step == 0, own, term)
        if stage == 3:
            self.out[...] = total
        else:
            self.value[stage + 1] = total


class ScatterPlan:
    def __init__(self, terms, vec, dims, n_tensor, chunk=256, every=8, depth=4):
        self.dims, self.n_tensor, self.has_total, self.depth = dims, n_tensor, vec is not None, depth
        n_a, n_b, n_c = dims
        tokens, width = terms[0][0].shape
        rows = width // (n_a * n_b * n_c)
        parts = [(1, right.shape[1] // n_tensor) for _, right in terms]
        chunk = min(chunk, *(cols for _, cols in parts))
        self.pieces = pieces_of(parts, chunk)
        self.part_cols = [cols for _, cols in parts]
        count, slots = len(self.pieces), Scatter.slots(dims, n_tensor)
        kinds = [0 if i % every else 1 for i in range(count)]
        self.places = [(k, kinds[:i].count(k)) for i, k in enumerate(kinds)]
        lefts = []
        self.left_at = []
        for left, _ in terms:
            known = [i for i, other in enumerate(lefts) if other is left]
            if not known:
                lefts.append(left)
            self.left_at.append(known[0] if known else len(lefts) - 1)
        self.n_left = len(lefts)
        self.args = lefts + [right for _, right in terms]
        self.in_specs = [VMEM] * len(lefts) + [ANY] * len(terms)
        self.out_shape = [jax.ShapeDtypeStruct((rows, cols), jnp.float32) for _, cols in parts]
        self.out_specs = [VMEM] * len(terms)
        bf, half = jnp.bfloat16, rows // 2
        self.scratch = [
            pltpu.VMEM((count, n_a, n_b, n_c, rows, chunk), bf),
            pltpu.VMEM((count, n_tensor - 1, n_a, n_b, n_c, rows, chunk), bf),
            pltpu.VMEM((self.SENDS, n_tensor - 1, n_a, n_b, n_c, rows, chunk), bf),
            pltpu.VMEM((2, n_tensor, tokens, chunk), bf),
            pltpu.VMEM((len(lefts), width, tokens), bf),
            pltpu.SemaphoreType.DMA((count, slots)),
            pltpu.SemaphoreType.DMA((count, slots)),
            pltpu.SemaphoreType.DMA((2, n_tensor)),
        ]
        for kind, orders in enumerate((Scatter.NORMAL, Scatter.EARLY)):
            for stage in (1, 2, 3):
                for order in orders:
                    left = [dims[x] for x in Scatter.left(order, stage)]
                    shape = (max(kinds.count(kind), 1), dims[order[stage - 1]] - 1, *left, half, chunk)
                    self.scratch.append(pltpu.VMEM(shape, bf))
        if self.has_total:
            self.args.append(vec)
            self.in_specs.append(VMEM)
            self.out_shape.append(jax.ShapeDtypeStruct(vec.shape, vec.dtype))
            self.out_specs.append(VMEM)
            self.scratch.append(pltpu.VMEM((4,) + vec.shape, vec.dtype))
            self.scratch += [pltpu.VMEM((k - 1,) + vec.shape, vec.dtype) for k in (n_tensor, n_c, n_b, n_a)]
            self.scratch += [pltpu.SemaphoreType.DMA((Total.slots(dims, n_tensor),))] * 2

    SENDS = 3

    def results(self, outs):
        return list(outs)

    def steps(self, ins, outs, scratch):
        place = Place(self.dims, self.n_tensor)
        held, near, sent, slabs, turned, send, recv, local = scratch[:8]
        chunks = []
        for i, (piece, (kind, at)) in enumerate(zip(self.pieces, self.places)):
            orders = (Scatter.NORMAL, Scatter.EARLY)[kind]
            boxes = scratch[8 + 6 * kind : 14 + 6 * kind]
            bufs = [[boxes[2 * stage + color].at[at] for color in (0, 1)] for stage in range(3)]
            chunks.append(
                Scatter(
                    place, piece, orders, turned.at[self.left_at[piece.source]], slabs.at[i % 2], outs[piece.source],
                    held.at[i], near.at[i], sent.at[i % self.SENDS], bufs, (send.at[i], recv.at[i]),
                )
            )
        count, depth = len(chunks), self.depth
        total = None
        if self.has_total:
            value, *rest = scratch[20:]
            total = Total(place, value, outs[-1], rest[:4], rest[4], rest[5])

        def loads(i):
            piece = self.pieces[i]
            right = ins[self.n_left + piece.source]
            for t in range(self.n_tensor):
                cols = pl.ds(t * self.part_cols[piece.source] + piece.first, piece.width)
                yield pltpu.make_async_copy(right.at[:, cols], slabs.at[i % 2, t], local.at[i % 2, t])

        def turn(number):
            block = 256

            def body(a, _):
                cols = pl.ds(pl.multiple_of(a * block, block), block)
                turned[number, cols, :] = ins[number][:, cols].T
                return 0

            lax.fori_loop(0, turned.shape[1] // block, body, 0)

        firsts = [next(i for i, p in enumerate(self.pieces) if self.left_at[p.source] == n) for n in range(self.n_left)]

        def begin():
            run_all(loads(0), "start")
            if total is not None:
                value[0] = ins[-1][...]
            place.barrier()
            if total is not None:
                run_all(total.copies(0), "start")

        def step(i):
            if i < count:
                run_all(loads(i), "wait")
                if i + 1 < count:
                    run_all(loads(i + 1), "start")
                if i >= self.SENDS:
                    run_all(chunks[i - self.SENDS].copies(0), "wait_send")
                for number, first in enumerate(firsts):
                    if first == i:
                        turn(number)
                chunks[i].compute()
            if 0 <= i - 1 < count:
                c = chunks[i - 1]
                run_all(c.copies(0), "wait_recv")
                c.add_tensor()
                run_all(c.copies(1), "start")
            for stage in (1, 2, 3):
                at = i - 1 - depth * stage
                if 0 <= at < count:
                    run_all(chunks[at].copies(stage), "wait_recv")
                    chunks[at].add(stage)
                    if stage < 3:
                        run_all(chunks[at].copies(stage + 1), "start")
            if total is not None and i < 4:
                run_all(total.copies(i), "wait_recv")
                total.add(i)
                if i < 3:
                    run_all(total.copies(i + 1), "start")

        def end():
            for i, c in enumerate(chunks):
                for stage in range(0 if i >= count - self.SENDS else 1, 4):
                    run_all(c.copies(stage), "wait_send")
            if total is not None:
                for stage in range(4):
                    run_all(total.copies(stage), "wait_send")

        last = max(count + 1 + 3 * depth, 4 if self.has_total else 0)
        return [begin] + [functools.partial(step, i) for i in range(last)] + [end]


def plan_kernel(plan, *refs):
    n_in, n_out = len(plan.in_specs), len(plan.out_specs)
    for step in plan.steps(refs[:n_in], refs[n_in : n_in + n_out], refs[n_in + n_out :]):
        step()


def run_plan(plan, collective_id, name):
    outs = pl.pallas_call(
        functools.partial(plan_kernel, plan),
        out_shape=plan.out_shape,
        in_specs=plan.in_specs,
        out_specs=plan.out_specs,
        scratch_shapes=plan.scratch,
        compiler_params=pltpu.CompilerParams(
            collective_id=collective_id, has_side_effects=True, vmem_limit_bytes=VMEM_LIMIT
        ),
        name=name,
    )(*plan.args)
    return plan.results(outs)


def exchange_kernel(dims, n_tensor, n, *refs):
    ins, outs = refs[:n], refs[n : 2 * n]
    send, recv, local = refs[2 * n :]
    place = Place(dims, n_tensor)

    def copies(i):
        for step in range(1, n_tensor):
            device, _ = place.peer(3, step)
            sems = (send.at[i, step - 1], recv.at[i, step - 1])
            yield remote(ins[i], outs[i].at[n_tensor - step], *sems, device)

    own = [pltpu.make_async_copy(ins[i], outs[i].at[0], local.at[i]) for i in range(n)]
    for copy in own:
        copy.start()
    place.barrier((3,))
    for i in range(n):
        for copy in copies(i):
            copy.start()
    for i in range(n):
        own[i].wait()
        for copy in copies(i):
            copy.wait()


def exchange_rows(arrays, dims, n_tensor, collective_id):
    n = len(arrays)
    outs = pl.pallas_call(
        functools.partial(exchange_kernel, dims, n_tensor, n),
        out_shape=[jax.ShapeDtypeStruct((n_tensor,) + a.shape, a.dtype) for a in arrays],
        in_specs=[VMEM] * n,
        out_specs=[ANY] * n,
        scratch_shapes=[
            pltpu.SemaphoreType.DMA((n, n_tensor - 1)),
            pltpu.SemaphoreType.DMA((n, n_tensor - 1)),
            pltpu.SemaphoreType.DMA((n,)),
        ],
        compiler_params=pltpu.CompilerParams(collective_id=collective_id, has_side_effects=True),
        name="exchange_rows",
    )(*arrays)
    return [o.reshape(-1, o.shape[-1]) for o in outs]


def return_kernel(dims, n_tensor, n, *refs):
    ins, outs, bufs = refs[:n], refs[n : 2 * n], refs[2 * n : 3 * n]
    send, recv = refs[3 * n :]
    place = Place(dims, n_tensor)
    rows = outs[0].shape[0]

    def copies(i):
        for step in range(1, n_tensor):
            device, _ = place.peer(3, step)
            sems = (send.at[i, step - 1], recv.at[i, step - 1])
            yield remote(ins[i].at[pl.ds(step * rows, rows), :], bufs[i].at[step - 1], *sems, device)

    place.barrier((3,))
    for i in range(n):
        for copy in copies(i):
            copy.start()
    for i in range(n):
        for copy in copies(i):
            copy.wait()
        for first in range(0, rows, 64):
            total = ins[i][first : first + 64, :].astype(jnp.float32)
            for step in range(1, n_tensor):
                total = total + bufs[i][step - 1, first : first + 64, :].astype(jnp.float32)
            outs[i][first : first + 64, :] = total.astype(outs[i].dtype)


def return_rows(arrays, dims, n_tensor, collective_id):
    n = len(arrays)
    rows, width = arrays[0].shape[0] // n_tensor, arrays[0].shape[1]
    return pl.pallas_call(
        functools.partial(return_kernel, dims, n_tensor, n),
        out_shape=[jax.ShapeDtypeStruct((rows, width), a.dtype) for a in arrays],
        in_specs=[VMEM] * n,
        out_specs=[VMEM] * n,
        scratch_shapes=[pltpu.VMEM((n_tensor - 1, rows, width), a.dtype) for a in arrays]
        + [pltpu.SemaphoreType.DMA((n, n_tensor - 1)), pltpu.SemaphoreType.DMA((n, n_tensor - 1))],
        compiler_params=pltpu.CompilerParams(collective_id=collective_id, has_side_effects=True),
        name="return_rows",
    )(*arrays)


def norm_forward(stream, gain_row, shift_row):
    centered = stream - jnp.mean(stream, axis=-1, keepdims=True)
    inv_std = lax.rsqrt(jnp.mean(centered * centered, axis=-1, keepdims=True) + EPSILON)
    normed = centered * inv_std
    return (normed * gain_row + shift_row, normed, inv_std)


def norm_backward(grad_result, normed, inv_std, gain_row):
    grad_normed = grad_result * gain_row
    return inv_std * (
        grad_normed
        - jnp.mean(grad_normed, axis=-1, keepdims=True)
        - normed * jnp.mean(grad_normed * normed, axis=-1, keepdims=True)
    )


def low(value):
    return value.astype(jnp.bfloat16)


def ffn_forward(entered, weight_in, weight_out_t):
    before = dot_nn(entered, weight_in)
    active = low(jax.nn.silu(before))
    return dot_nt(active, weight_out_t), (before, active)


def ffn_backward(entered, saved, grad_low, weight_in, weight_out_t):
    before, active = saved
    sigma = jax.nn.sigmoid(before)
    grad_active = dot_nn(grad_low, weight_out_t)
    grad_before = low(grad_active * sigma * (1.0 + before * (1.0 - sigma)))
    return dot_nt(grad_before, weight_in), [(grad_low, active), (entered, grad_before)]


def taps_forward(signal, before, conv_taps):
    rows = signal.shape[0]
    padded = jnp.concatenate([before, signal], axis=0)
    skip = before.shape[0] - (KERNEL - 1)
    result = jnp.zeros_like(signal)
    for tap in range(KERNEL):
        result = result + conv_taps[tap] * padded[skip + tap : skip + tap + rows]
    return result


def taps_backward(grad, after, signal, before, conv_taps):
    rows = signal.shape[0]
    padded_signal = jnp.concatenate([before, signal], axis=0)
    padded_grad = jnp.concatenate([grad, after], axis=0)
    skip = before.shape[0] - (KERNEL - 1)
    grad_signal = jnp.zeros_like(signal)
    taps = []
    for tap in range(KERNEL):
        back = KERNEL - 1 - tap
        grad_signal = grad_signal + conv_taps[tap] * padded_grad[back : back + rows]
        taps.append(jnp.sum(grad * padded_signal[skip + tap : skip + tap + rows], axis=0))
    return grad_signal, jnp.stack(taps)


HALO = 32


def on_device(
    dims,
    n_tensor,
    stream_in,
    grad_out,
    clip_lengths,
    first_up,
    first_down,
    attn_proj,
    attn_out,
    rel_table,
    glu_weight,
    conv_taps,
    conv_out,
    second_up,
    second_down,
    norm_gains,
    norm_shifts,
):
    rank = lax.axis_index("tensor")
    rows, width = stream_in.shape
    keys = rows * n_tensor
    early = [first_up[None], first_down.T[None], attn_proj, attn_out.T[None]]
    late = [glu_weight, conv_out.T[None], second_up[None], second_down.T[None]]
    def enter(stream, row):
        result, normed, inv_std = norm_forward(stream, norm_gains[row], norm_shifts[row])
        return low(result), (normed, inv_std)

    def norm_back(grad_result, saved, row):
        normed, inv_std = saved
        grad_input = norm_backward(grad_result, normed, inv_std, norm_gains[row])
        return grad_input, jnp.sum(grad_result * normed, axis=0), jnp.sum(grad_result, axis=0)

    def shift_rank(value, step):
        pairs = [(i, i + step) for i in range(n_tensor) if 0 <= i + step < n_tensor]
        return lax.ppermute(value, "tensor", pairs)

    stream = stream_in.astype(jnp.float32)
    entered_a, norm_a = enter(stream, 0)
    gathered = run_plan(FeedPlan(early, entered_a, dims, n_tensor), 0, "gather_weights")
    (up_one,), (down_one,), proj, (out_attn,), before_a, active_a, branch = gathered
    squares = []
    ffn_a = (before_a, active_a)
    squares.append(jnp.sum(branch * branch))
    stream = stream + 0.5 * branch

    entered_b, norm_b = enter(stream, 1)
    query, own_keys, own_vals = (low(dot_nn(entered_b, proj[i])) for i in range(3))
    key_rows, val_rows = exchange_rows([own_keys, own_vals], dims, n_tensor, 2)
    place = lax.rem(jnp.arange(keys, dtype=jnp.int32) + rank * rows, keys)
    mask = jnp.where(place < clip_lengths[0], 0.0, MASKED).astype(jnp.float32)[None]
    table = span_table(rel_table)
    attended, log_totals, gathered = attn_fwd(
        query, key_rows, val_rows, table, mask, GatherPlan(late, dims, n_tensor, *HOST_G), 4
    )
    glu, (out_conv,), (up_two,), (down_two,) = gathered
    branch = dot_nt(attended, out_attn)
    squares.append(jnp.sum(branch * branch))
    stream = stream + branch

    entered_c, norm_c = enter(stream, 2)
    glu_first = dot_nn(entered_c, glu[0])
    glu_second = dot_nn(entered_c, glu[1])
    sig_second = jax.nn.sigmoid(glu_second)
    gated = glu_first * sig_second
    gated_before = shift_rank(gated[rows - HALO :], 1)
    mixed = taps_forward(gated, gated_before, conv_taps)
    shaped, normed_mid, scale_mid = norm_forward(mixed, norm_gains[3], norm_shifts[3])
    conv_act = low(jax.nn.silu(shaped))
    branch = dot_nt(conv_act, out_conv)
    squares.append(jnp.sum(branch * branch))
    stream = stream + branch

    entered_d, norm_d = enter(stream, 4)
    branch, ffn_d = ffn_forward(entered_d, up_two, down_two)
    squares.append(jnp.sum(branch * branch))
    stream = stream + 0.5 * branch
    squares.append(jnp.sum(stream * stream))
    result, normed_e, scale_e = norm_forward(stream, norm_gains[5], norm_shifts[5])
    output = low(result)

    grad_stream, gain_e, shift_e = norm_back(grad_out.astype(jnp.float32), (normed_e, scale_e), 5)
    grad_low = low(0.5 * grad_stream)
    grad_entered, terms_two = ffn_backward(entered_d, ffn_d, grad_low, up_two, down_two)
    grad_extra, gain_d, shift_d = norm_back(grad_entered, norm_d, 4)
    grad_stream = grad_stream + grad_extra

    grad_low = low(grad_stream)
    terms_mid = [(grad_low, conv_act)]
    sigma = jax.nn.sigmoid(shaped)
    grad_shaped = dot_nn(grad_low, out_conv) * sigma * (1.0 + shaped * (1.0 - sigma))
    grad_mixed, gain_mid, shift_mid = norm_back(grad_shaped, (normed_mid, scale_mid), 3)
    grad_after = shift_rank(grad_mixed[:HALO], -1)
    grad_gated, taps_grad = taps_backward(grad_mixed, grad_after, gated, gated_before, conv_taps)
    grad_first = low(grad_gated * sig_second)
    grad_second = low(grad_gated * glu_first * sig_second * (1.0 - sig_second))
    terms_mid += [(entered_c, g) for g in (grad_first, grad_second)]
    grad_entered = dot_nt(grad_first, glu[0]) + dot_nt(grad_second, glu[1])
    grad_extra, gain_c, shift_c = norm_back(grad_entered, norm_c, 2)
    grad_stream = grad_stream + grad_extra

    grad_low = low(grad_stream)
    terms_attn = [(grad_low, attended)]
    grad_attended = low(dot_nn(grad_low, out_attn))
    grad_query, grad_keys, grad_vals, grad_span, summed = attn_bwd(
        query, key_rows, val_rows, grad_attended, attended, log_totals, table, mask,
        ScatterPlan(terms_two + terms_mid, None, dims, n_tensor, *HOST_S), 5,
    )
    s_down_two, s_up_two, s_conv, s_glu0, s_glu1 = summed
    grad_keys, grad_vals = return_rows([grad_keys, grad_vals], dims, n_tensor, 3)
    grad_parts = (grad_query, grad_keys, grad_vals)
    terms_attn += [(entered_b, g) for g in grad_parts]
    grad_entered = sum(dot_nt(g, proj[i]) for i, g in enumerate(grad_parts))
    grad_extra, gain_b, shift_b = norm_back(grad_entered, norm_b, 1)
    grad_stream = grad_stream + grad_extra

    grad_low = low(0.5 * grad_stream)
    grad_entered, terms_one = ffn_backward(entered_a, ffn_a, grad_low, up_one, down_one)
    grad_extra, gain_a, shift_a = norm_back(grad_entered, norm_a, 0)
    grad_stream = grad_stream + grad_extra

    span_grad = fold_table(grad_span)
    span_rows = -(-span_grad.size // width)
    table_rows = jnp.pad(span_grad.reshape(-1), (0, span_rows * width - span_grad.size)).reshape(span_rows, width)
    square_row = jnp.pad(jnp.stack(squares), (0, width - len(squares)))[None]
    parts = [
        jnp.stack([gain_a, gain_b, gain_c, gain_mid, gain_d, gain_e]),
        jnp.stack([shift_a, shift_b, shift_c, shift_mid, shift_d, shift_e]),
        taps_grad,
        table_rows,
        square_row,
    ]
    vec = jnp.concatenate(parts, axis=0)
    vec = jnp.pad(vec, ((0, -vec.shape[0] % 8), (0, 0)))
    *summed, vec = run_plan(ScatterPlan(terms_attn + terms_one, vec, dims, n_tensor), 1, "scatter_grads")
    s_attn, s_q, s_k, s_v, s_down_one, s_up_one = summed
    at = 0
    pieces = []
    for part in parts:
        pieces.append(vec[at : at + part.shape[0]])
        at += part.shape[0]
    gains_sum, shifts_sum, taps_sum, table_sum, square_sum = pieces
    table_sum = table_sum.reshape(-1)[: span_grad.size].reshape(span_grad.shape)
    count_all = float(lax.axis_size("dp") * keys * width)
    rms_values = jnp.sqrt(square_sum[0, : len(squares)] / count_all)
    return (
        output,
        grad_stream,
        s_up_one,
        s_down_one.T,
        jnp.stack([s_q, s_k, s_v]),
        s_attn.T,
        table_sum,
        jnp.stack([s_glu0, s_glu1]),
        taps_sum,
        s_conv.T,
        s_up_two,
        s_down_two.T,
        gains_sum,
        shifts_sum,
        rms_values,
    )


def solution(mesh):
    n_dp, n_tensor = mesh.shape["dp"], mesh.shape["tensor"]
    dims = FACTORS.get(n_dp, (n_dp, 1, 1))
    return jax.shard_map(
        functools.partial(on_device, dims, n_tensor),
        mesh=mesh,
        in_specs=(
            P(("dp", "tensor"), None),
            P(("dp", "tensor"), None),
            P("dp"),
            P("dp", "tensor"),
            P("tensor", "dp"),
            P(None, "dp", "tensor"),
            P("tensor", "dp"),
            P(),
            P(None, "dp", "tensor"),
            P(),
            P("tensor", "dp"),
            P("dp", "tensor"),
            P("tensor", "dp"),
            P(),
            P(),
        ),
        out_specs=(
            P(("dp", "tensor"), None),
            P(("dp", "tensor"), None),
            P("dp", "tensor"),
            P("tensor", "dp"),
            P(None, "dp", "tensor"),
            P("tensor", "dp"),
            P(),
            P(None, "dp", "tensor"),
            P(),
            P("tensor", "dp"),
            P("dp", "tensor"),
            P("tensor", "dp"),
            P(),
            P(),
            P(),
        ),
        check_vma=False,
    )
```
